32 devices in a mesh: dp: 4 (over z), mp: 8 (over y, x, core).
Axes of the slice: x: 2, y: 2, z: 4, core: 2. Of those that a mesh axis runs over, the one named last changes fastest.
Arguments:
- tokens: bfloat16 [8, 2048, 2048], P('dp', None, 'mp'), may hold values from -6 to 6
- doc_lengths: int32 [8, 6], P('dp'), may hold values from 1 to 1024, 2048 in all within a row
- out_grad: bfloat16 [8, 2048, 2048], P('dp', None, 'mp'), may hold values from -6 to 6
- attn_gain: float32 [2048], P('mp'), may hold values from 0.25 to 1.75
- ffn_gain: float32 [2048], P('mp'), may hold values from 0.25 to 1.75
- query_base: bfloat16 [2048, 2048], P('mp'), may hold values from -0.125 to 0.125
- query_lower: float32 [2048, 16], P('mp'), may hold values from -0.125 to 0.125
- query_upper: float32 [16, 2048], replicated, may hold values from -0.3 to 0.3
- query_scale: float32 [2048], P('mp'), may hold values from 0.8 to 1.6
- key_base: bfloat16 [2048, 2048], P('mp'), may hold values from -0.125 to 0.125
- key_lower: float32 [2048, 16], P('mp'), may hold values from -0.125 to 0.125
- key_upper: float32 [16, 2048], replicated, may hold values from -0.3 to 0.3
- key_scale: float32 [2048], P('mp'), may hold values from 0.8 to 1.6
- value_base: bfloat16 [2048, 2048], P('mp'), may hold values from -0.125 to 0.125
- value_lower: float32 [2048, 16], P('mp'), may hold values from -0.125 to 0.125
- value_upper: float32 [16, 2048], replicated, may hold values from -0.3 to 0.3
- value_scale: float32 [2048], P('mp'), may hold values from 0.5 to 2
- output_base: bfloat16 [2048, 2048], P('mp'), may hold values from -0.125 to 0.125
- output_lower: float32 [2048, 16], P('mp'), may hold values from -0.125 to 0.125
- output_upper: float32 [16, 2048], replicated, may hold values from -0.3 to 0.3
- output_scale: float32 [2048], P('mp'), may hold values from 2 to 8
- gate_base: bfloat16 [2048, 5632], P('mp'), may hold values from -0.125 to 0.125
- gate_lower: float32 [2048, 16], P('mp'), may hold values from -0.125 to 0.125
- gate_upper: float32 [16, 5632], replicated, may hold values from -0.3 to 0.3
- gate_scale: float32 [5632], P('mp'), may hold values from 0.5 to 2
- lift_base: bfloat16 [2048, 5632], P('mp'), may hold values from -0.125 to 0.125
- lift_lower: float32 [2048, 16], P('mp'), may hold values from -0.125 to 0.125
- lift_upper: float32 [16, 5632], replicated, may hold values from -0.3 to 0.3
- lift_scale: float32 [5632], P('mp'), may hold values from 0.5 to 2
- down_base: bfloat16 [5632, 2048], P('mp'), may hold values from -0.078125 to 0.078125
- down_lower: float32 [5632, 16], P('mp'), may hold values from -0.078125 to 0.078125
- down_upper: float32 [16, 2048], replicated, may hold values from -0.3 to 0.3
- down_scale: float32 [2048], P('mp'), may hold values from 1 to 3
Outputs:
- out_tokens: bfloat16 [8, 2048, 2048], P('dp', None, 'mp')
- in_grad: float32 [8, 2048, 2048], P('dp', None, 'mp')
- query_lower_grad: float32 [2048, 16], P('mp')
- query_upper_grad: float32 [16, 2048], replicated
- query_scale_grad: float32 [2048], P('mp')
- key_lower_grad: float32 [2048, 16], P('mp')
- key_upper_grad: float32 [16, 2048], replicated
- key_scale_grad: float32 [2048], P('mp')
- value_lower_grad: float32 [2048, 16], P('mp')
- value_upper_grad: float32 [16, 2048], replicated
- value_scale_grad: float32 [2048], P('mp')
- output_lower_grad: float32 [2048, 16], P('mp')
- output_upper_grad: float32 [16, 2048], replicated
- output_scale_grad: float32 [2048], P('mp')
- gate_lower_grad: float32 [2048, 16], P('mp')
- gate_upper_grad: float32 [16, 5632], replicated
- gate_scale_grad: float32 [5632], P('mp')
- lift_lower_grad: float32 [2048, 16], P('mp')
- lift_upper_grad: float32 [16, 5632], replicated
- lift_scale_grad: float32 [5632], P('mp')
- down_lower_grad: float32 [5632, 16], P('mp')
- down_upper_grad: float32 [16, 2048], replicated
- down_scale_grad: float32 [2048], P('mp')
The draws below stay inside these ranges and needn't reach their ends.
Inputs may be any that keep to these rules, and one draw needn't show every extreme that they name: `doc_lengths`: each row lists the lengths of one sequence's 5 documents in order, then the length of the padding at its end; each row sums to 2048.
All inputs are finite; a program needn't handle non-finite values.
Results may differ from the reference program's by a relative error of at most 0.035.
Values may be sent and summed in bfloat16 or wider, within the bound.
A program may use at most 320 MiB of HBM per device.

```python
import math
import jax
import jax.numpy as jnp
import numpy as np
from jax import lax

D = 2048
H = 16
HD = 128
FF = 5632
R = 16
SEQ = 2048
NDOC = 5
SEQS = 8


def levels(stream_key, shape, pieces, low, high):
    def one(axis_at, blocks):
        steps = jax.random.uniform(jax.random.fold_in(jax.random.fold_in(stream_key, 6), axis_at), (blocks,), jnp.float32, low / len(pieces), high / len(pieces))
        return jnp.repeat(jnp.exp(steps), shape[axis_at] // blocks).reshape((-1,) + (1,) * (len(shape) - axis_at - 1))

    loudness = one(*pieces[0])
    for cut in pieces[1:]:
        loudness = loudness * one(*cut)
    return loudness


def split_up(count, total, bound, slope):
    weights = [(1 << 20) // math.isqrt(grade ** slope) + 1 for grade in range(2, count + 1)]
    spare, given = total - bound - (count - 1), [1] * (count - 1)
    while spare > 0:
        movable = [i for i in range(count - 1) if given[i] < bound]
        pool, remaining = sum([weights[i] for i in movable]), spare
        for i in movable:
            addition = min(bound - given[i], max(1, remaining * weights[i] // pool), spare)
            given[i] = given[i] + addition
            spare = spare - addition
    return np.array([bound] + given)


def uneven_parts(stream_key, number_of, total, reach, lean):
    if number_of == 2:
        one = jax.random.randint(stream_key, (), max(1, total - reach), min(reach, total - 1) + 1)
        return jnp.stack([one, total - one])
    tallies = jnp.asarray(split_up(number_of, total, reach, lean), jnp.int32)
    couples = (number_of - 1) // 2
    source_of, taker = tallies[1:1 + 2 * couples:2], tallies[2:2 + 2 * couples:2]
    margin = jnp.minimum(source_of - 1, reach - taker)
    passed = jax.random.randint(jax.random.fold_in(stream_key, 1), (couples,), 0, 1 << 20) % (margin + 1)
    tallies = tallies.at[1:1 + 2 * couples:2].set(source_of - passed).at[2:2 + 2 * couples:2].set(taker + passed)
    return tallies[jax.random.permutation(jax.random.fold_in(stream_key, 2), number_of)]


def gaussian(own_key, shape, width, limit, shards=(), kind=jnp.bfloat16):
    array = jax.random.normal(own_key, shape, jnp.float32) * width
    if len(shards) > 0:
        array = levels(own_key, shape, shards, -0.22, 0.18) * array
    return jnp.clip(array, min=-limit, max=limit).astype(kind)


def setup_inputs(seed: int = 0) -> dict:
    key_of = jax.random.split(jax.random.key(seed), 34)
    return {
        "tokens": gaussian(key_of[0], (SEQS, SEQ, D), 1.0, 6.0, ((0, 4), (2, 8))),
        "doc_lengths": jax.vmap(lambda own: uneven_parts(own, NDOC + 1, SEQ, SEQ // 2, 1))(jax.random.split(key_of[1], SEQS)).reshape((SEQS, NDOC + 1)).astype(jnp.int32),
        "out_grad": gaussian(key_of[2], (SEQS, SEQ, D), 1.0, 6.0, ((0, 4), (2, 8))),
        "attn_gain": jnp.clip(1.0 + 0.15 * jax.random.normal(key_of[3], (D,), jnp.float32), 0.25, 1.75),
        "ffn_gain": jnp.clip(1.0 + 0.15 * jax.random.normal(key_of[4], (D,), jnp.float32), 0.25, 1.75),
        "query_base": gaussian(key_of[5], (D, D), D ** -0.5, 0.125, ((0, 8),)),
        "query_lower": gaussian(key_of[6], (D, R), D ** -0.5, 0.125, ((0, 8),), jnp.float32),
        "query_upper": gaussian(key_of[7], (R, D), 0.05, 0.3, (), jnp.float32),
        "query_scale": jnp.clip(jnp.exp(math.log(1.6) - 0.6931472 * jax.random.uniform(key_of[8], (D,), jnp.float32) ** levels(key_of[8], (D,), ((0, 8),), -0.2, 0.2)), 0.8, 1.6),
        "key_base": gaussian(key_of[9], (D, D), D ** -0.5, 0.125, ((0, 8),)),
        "key_lower": gaussian(key_of[10], (D, R), D ** -0.5, 0.125, ((0, 8),), jnp.float32),
        "key_upper": gaussian(key_of[11], (R, D), 0.05, 0.3, (), jnp.float32),
        "key_scale": jnp.clip(jnp.exp(math.log(1.6) - 0.6931472 * jax.random.uniform(key_of[12], (D,), jnp.float32) ** levels(key_of[12], (D,), ((0, 8),), -0.2, 0.2)), 0.8, 1.6),
        "value_base": gaussian(key_of[13], (D, D), D ** -0.5, 0.125, ((0, 8),)),
        "value_lower": gaussian(key_of[14], (D, R), D ** -0.5, 0.125, ((0, 8),), jnp.float32),
        "value_upper": gaussian(key_of[15], (R, D), 0.05, 0.3, (), jnp.float32),
        "value_scale": jnp.clip(jnp.exp(math.log(2.0) - 1.3862944 * jax.random.uniform(key_of[16], (D,), jnp.float32) ** levels(key_of[16], (D,), ((0, 8),), -0.2, 0.2)), 0.5, 2.0),
        "output_base": gaussian(key_of[17], (D, D), D ** -0.5, 0.125, ((0, 8),)),
        "output_lower": gaussian(key_of[18], (D, R), D ** -0.5, 0.125, ((0, 8),), jnp.float32),
        "output_upper": gaussian(key_of[19], (R, D), 0.05, 0.3, (), jnp.float32),
        "output_scale": jnp.clip(jnp.exp(math.log(8.0) - 1.3862944 * jax.random.uniform(key_of[20], (D,), jnp.float32) ** levels(key_of[20], (D,), ((0, 8),), -0.2, 0.2)), 2.0, 8.0),
        "gate_base": gaussian(key_of[21], (D, FF), D ** -0.5, 0.125, ((0, 8),)),
        "gate_lower": gaussian(key_of[22], (D, R), D ** -0.5, 0.125, ((0, 8),), jnp.float32),
        "gate_upper": gaussian(key_of[23], (R, FF), 0.05, 0.3, (), jnp.float32),
        "gate_scale": jnp.clip(jnp.exp(math.log(2.0) - 1.3862944 * jax.random.uniform(key_of[24], (FF,), jnp.float32) ** levels(key_of[24], (FF,), ((0, 8),), -0.2, 0.2)), 0.5, 2.0),
        "lift_base": gaussian(key_of[25], (D, FF), D ** -0.5, 0.125, ((0, 8),)),
        "lift_lower": gaussian(key_of[26], (D, R), D ** -0.5, 0.125, ((0, 8),), jnp.float32),
        "lift_upper": gaussian(key_of[27], (R, FF), 0.05, 0.3, (), jnp.float32),
        "lift_scale": jnp.clip(jnp.exp(math.log(2.0) - 1.3862944 * jax.random.uniform(key_of[28], (FF,), jnp.float32) ** levels(key_of[28], (FF,), ((0, 8),), -0.2, 0.2)), 0.5, 2.0),
        "down_base": gaussian(key_of[29], (FF, D), FF ** -0.5, 0.078125, ((0, 8),)),
        "down_lower": gaussian(key_of[30], (FF, R), FF ** -0.5, 0.078125, ((0, 8),), jnp.float32),
        "down_upper": gaussian(key_of[31], (R, D), 0.05, 0.3, (), jnp.float32),
        "down_scale": jnp.clip(jnp.exp(math.log(3.0) - 1.0986123 * jax.random.uniform(key_of[32], (D,), jnp.float32) ** levels(key_of[32], (D,), ((0, 8),), -0.2, 0.2)), 1.0, 3.0),
    }


EXACT_PRECISION = lax.Precision.HIGHEST
ADAPTER_SCALING = 2.0
EPSILON = 1e-05
ROPE_BASE = 10000.0
NEGATIVE = -1e+30

@jax.custom_vjp
def low(v):
    return lax.optimization_barrier(v.astype(jnp.bfloat16)).astype(jnp.float32)

@jax.custom_vjp
def low_back(v):
    return v

def low_keep(v):
    return (low(v), None)

def low_pass(kept, grad):
    return (grad,)

def back_keep(v):
    return (v, None)

def back_low(kept, grad):
    return (low(grad),)
low.defvjp(low_keep, low_pass)
low_back.defvjp(back_keep, back_low)

def layout(lengths):
    ends = jnp.cumsum(lengths).astype(jnp.int32)
    tokens_at = jnp.arange(SEQ, dtype=jnp.int32)
    after = (tokens_at[:, None] >= ends[None, :NDOC]).astype(jnp.int32)
    segment = lax.optimization_barrier(jnp.sum(after, axis=1)).astype(jnp.int32)
    start_at = lax.optimization_barrier(jnp.sum(after * lengths[None, :NDOC], axis=1)).astype(jnp.int32)
    return (segment, tokens_at - start_at)

def rope_tables(position):
    steps_half = jnp.arange(HD // 2, dtype=jnp.float32)
    frequency = ROPE_BASE ** (-(2.0 * steps_half / HD))
    angles = position.astype(jnp.float32)[:, None] * frequency[None, :]
    cosine_rows = jnp.cos(angles)
    sine_rows = jnp.sin(angles)
    return (jnp.concatenate([cosine_rows, cosine_rows], axis=1), jnp.concatenate([sine_rows, sine_rows], axis=1))

def rotate(vectors, cosine_rows, sine_rows):
    half_width = vectors.shape[-1] // 2
    turned = jnp.concatenate([-vectors[..., half_width:], vectors[..., :half_width]], axis=-1)
    return vectors * cosine_rows[:, None, :] + turned * sine_rows[:, None, :]

def rms_norm(token_rows, gain):
    return token_rows * lax.rsqrt(lax.optimization_barrier(jnp.mean(token_rows * token_rows, axis=-1, keepdims=True)) + EPSILON) * gain

def dora(activation_rows, matrix_operand, lower_factor_matrix, upper_factor_matrix, scale_vec):
    combined_weight = matrix_operand + ADAPTER_SCALING * jnp.dot(lower_factor_matrix, upper_factor_matrix, precision=EXACT_PRECISION)
    norms = jnp.sqrt(lax.optimization_barrier(jnp.sum(combined_weight * combined_weight, axis=0)))
    inner_dimension = low_back(jnp.dot(activation_rows, low(combined_weight), precision=EXACT_PRECISION))
    return inner_dimension * (scale_vec / norms)

def attention(query_rows, key_rows, value_rows, segment):
    block_rows = min(512, SEQ)
    block_count = SEQ // block_rows
    positions = jnp.arange(SEQ, dtype=jnp.int32)
    query_blocks = query_rows.reshape(block_count, block_rows, H, HD)
    segment_blocks = segment.reshape(block_count, block_rows)
    place_blocks = positions.reshape(block_count, block_rows)

    def one_block(inputs):
        query_block, segment_block, place_block = inputs
        raw_scores = jnp.einsum('qhd,khd->hqk', query_block, key_rows, precision=EXACT_PRECISION)
        scores = low_back(raw_scores * HD ** (-0.5))
        allowed = (segment_block[:, None] == segment[None, :]) & (positions[None, :] <= place_block[:, None])
        scores = jnp.where(allowed[None], scores, NEGATIVE)
        row_max = lax.optimization_barrier(jnp.max(scores, axis=-1, keepdims=True))
        exponent = jnp.exp(scores - row_max)
        softmax_rows = exponent / lax.optimization_barrier(jnp.sum(exponent, axis=-1, keepdims=True))
        return jnp.einsum('hqk,khd->qhd', low(softmax_rows), value_rows, precision=EXACT_PRECISION)
    attended = lax.map(jax.checkpoint(one_block), (query_blocks, segment_blocks, place_blocks))
    return attended.reshape(SEQ, H, HD)

def forward(token_rows, segment, position, attn_gain, ffn_gain, bases, trainable):

    def project(activation_rows, weight_id):
        return dora(activation_rows, bases[weight_id], trainable[weight_id][0], trainable[weight_id][1], trainable[weight_id][2])
    cosine_rows, sine_rows = rope_tables(position)
    normed = low(rms_norm(token_rows, attn_gain))
    query_rows = low(rotate(project(normed, 0).reshape(SEQ, H, HD), cosine_rows, sine_rows))
    key_rows = low(rotate(project(normed, 1).reshape(SEQ, H, HD), cosine_rows, sine_rows))
    value_rows = low(project(normed, 2).reshape(SEQ, H, HD))
    attended = low(low_back(attention(query_rows, key_rows, value_rows, segment))).reshape(SEQ, D)
    residual = token_rows + project(attended, 3)
    normed_ffn = low(rms_norm(residual, ffn_gain))
    hidden = low(jax.nn.silu(project(normed_ffn, 4)) * project(normed_ffn, 5))
    return residual + project(hidden, 6)

def reference(tokens, doc_lengths, out_grad, attn_gain, ffn_gain, query_base, query_lower, query_upper, query_scale, key_base, key_lower, key_upper, key_scale, value_base, value_lower, value_upper, value_scale, output_base, output_lower, output_upper, output_scale, gate_base, gate_lower, gate_upper, gate_scale, lift_base, lift_lower, lift_upper, lift_scale, down_base, down_lower, down_upper, down_scale):
    bases = tuple((matrix_operand.astype(jnp.float32) for matrix_operand in (query_base, key_base, value_base, output_base, gate_base, lift_base, down_base)))
    trainable = ((query_lower, query_upper, query_scale), (key_lower, key_upper, key_scale), (value_lower, value_upper, value_scale), (output_lower, output_upper, output_scale), (gate_lower, gate_upper, gate_scale), (lift_lower, lift_upper, lift_scale), (down_lower, down_upper, down_scale))
    zero_grads = jax.tree.map(jnp.zeros_like, trainable)

    def one_sequence(totals, inputs):
        token_low, lengths, grad_low = inputs
        segment, position = layout(lengths)
        valid = (segment < NDOC).astype(jnp.float32)

        def layer(inputs_f, params):
            return forward(inputs_f, segment, position, attn_gain, ffn_gain, bases, params)
        output_rows, pullback = jax.vjp(layer, token_low.astype(jnp.float32), trainable)
        grad_input, grad_params = pullback(grad_low.astype(jnp.float32) * valid[:, None])
        totals = jax.tree.map(lambda first_op, second_op: first_op + second_op, totals, grad_params)
        return (totals, (output_rows.astype(jnp.bfloat16), grad_input))
    totals, (out_tokens, in_grad) = lax.scan(one_sequence, zero_grads, (tokens, doc_lengths, out_grad))
    grad_list = [member for triple in totals for member in triple]
    return (out_tokens, in_grad, grad_list[0], grad_list[1], grad_list[2], grad_list[3], grad_list[4], grad_list[5], grad_list[6], grad_list[7], grad_list[8], grad_list[9], grad_list[10], grad_list[11], grad_list[12], grad_list[13], grad_list[14], grad_list[15], grad_list[16], grad_list[17], grad_list[18], grad_list[19], grad_list[20])
```

```python
import functools

import jax
import jax.numpy as jnp
from jax import lax
from jax.experimental import pallas as pl
from jax.experimental.pallas import tpu as pltpu
from jax.sharding import PartitionSpec as P

HD = 128
R = 16
RP = 128
NDOC = 5
EPSILON = 1e-05
ROPE_BASE = 10000.0
NEGATIVE = -1e30
LOG2E = 1.4426950408889634
BF = jnp.bfloat16
F32 = jnp.float32


def dot_nn(a, b):
    return lax.dot_general(a, b, (((1,), (0,)), ((), ())), preferred_element_type=F32)


def dot_nt(a, b):
    return lax.dot_general(a, b, (((1,), (1,)), ((), ())), preferred_element_type=F32)


def dot_tn(a, b):
    return lax.dot_general(a, b, (((0,), (0,)), ((), ())), preferred_element_type=F32)


def whole(shape):
    rank = len(shape)
    return pl.BlockSpec(tuple(shape), lambda i: (0,) * rank)


def rows(block, width):
    return pl.BlockSpec((block, width), lambda i: (i, 0))


def chunk_rows(count, block, width):
    return pl.BlockSpec((count, block, width), lambda i: (0, i, 0))


def sds(shape, dtype):
    return jax.ShapeDtypeStruct(tuple(shape), dtype)


def estimate(flops, bytes_accessed):
    return pl.CostEstimate(flops=int(flops), bytes_accessed=int(bytes_accessed), transcendentals=0)


def qkv_body(tok_ref, gain_ref, w_ref, l_ref, ratio_ref, cos_ref, sin_ref,
             x_ref, y_ref, q_ref, k_ref, xl_ref, inv_ref):
    count, block, width = tok_ref.shape
    total = jnp.zeros((block, 1), F32)
    for c in range(count):
        part = tok_ref[c].astype(F32)
        total = total + jnp.sum(part * part, axis=1, keepdims=True)
    inv = lax.rsqrt(total / (count * width) + EPSILON)
    inv_ref[...] = inv
    for c in range(count):
        x_ref[:, c * width:(c + 1) * width] = (
            tok_ref[c].astype(F32) * inv * gain_ref[c]
        ).astype(BF)
    y = dot_nn(x_ref[...], w_ref[...]) * ratio_ref[...]
    xl_ref[...] = dot_nn(x_ref[...], l_ref[...]).astype(BF)
    y_ref[...] = y.astype(BF)
    cos, sin = cos_ref[...], sin_ref[...]
    for number, out_ref in ((0, q_ref), (1, k_ref)):
        for h in range(width // HD):
            v = y[:, number * width + h * HD:number * width + (h + 1) * HD]
            out_ref[:, h * HD:(h + 1) * HD] = (
                v * cos - pltpu.roll(v, HD // 2, 1) * sin
            ).astype(BF)


def qkv_forward(tok, gain, w_cat, l_cat, ratio, cos, sin, block=256):
    count, length, width = tok.shape
    depth = count * width
    return pl.pallas_call(
        qkv_body,
        grid=(length // block,),
        in_specs=[
            chunk_rows(count, block, width),
            whole(gain.shape),
            whole(w_cat.shape),
            whole(l_cat.shape),
            whole(ratio.shape),
            rows(block, HD),
            rows(block, HD),
        ],
        out_specs=[
            rows(block, depth),
            rows(block, 3 * width),
            rows(block, width),
            rows(block, width),
            rows(block, RP),
            rows(block, 1),
        ],
        out_shape=[
            sds((length, depth), BF),
            sds((length, 3 * width), BF),
            sds((length, width), BF),
            sds((length, width), BF),
            sds((length, RP), BF),
            sds((length, 1), F32),
        ],
        cost_estimate=estimate(2 * length * depth * (3 * width + RP), 6 * length * depth),
        name="qkv_forward",
    )(tok, gain, w_cat, l_cat, ratio, cos, sin)


def attend_body(lo_ref, start_ref, q_ref, k_ref, v_ref, o_ref, lse_ref, vt_ref, *, block):
    length, width = q_ref.shape
    heads = width // HD
    factor = HD ** (-0.5) * LOG2E
    for h in range(heads):
        vt_ref[h * HD:(h + 1) * HD, :] = v_ref[:, h * HD:(h + 1) * HD].T
    key_iota = lax.broadcasted_iota(jnp.int32, (block, block), 0)
    query_iota = lax.broadcasted_iota(jnp.int32, (1, block), 1)

    def query_step(i, carry):
        base = pl.multiple_of(i * block, block)
        start = start_ref[pl.ds(i, 1), :]
        place = query_iota + base
        queries = [q_ref[pl.ds(base, block), h * HD:(h + 1) * HD] for h in range(heads)]

        def key_step(j, state):
            at = pl.multiple_of(j * block, block)
            key_place = key_iota + at
            allowed = (key_place >= start) & (key_place <= place)
            result = []
            for h in range(heads):
                top, total, acc = state[h]
                keys = k_ref[pl.ds(at, block), h * HD:(h + 1) * HD]
                s = jnp.where(allowed, dot_nt(keys, queries[h]) * factor, NEGATIVE)
                new_top = jnp.maximum(top, jnp.max(s, axis=0, keepdims=True))
                scale = jnp.exp2(top - new_top)
                p = jnp.exp2(s - new_top)
                total = total * scale + jnp.sum(p, axis=0, keepdims=True)
                acc = acc * scale + dot_nn(
                    vt_ref[h * HD:(h + 1) * HD, pl.ds(at, block)], p.astype(BF)
                )
                result.append((new_top, total, acc))
            return tuple(result)

        first = tuple(
            (
                jnp.full((1, block), NEGATIVE, F32),
                jnp.zeros((1, block), F32),
                jnp.zeros((HD, block), F32),
            )
            for _ in range(heads)
        )
        state = lax.fori_loop(lo_ref[i], i + 1, key_step, first)
        for h in range(heads):
            top, total, acc = state[h]
            o_ref[pl.ds(base, block), h * HD:(h + 1) * HD] = (acc / total).T.astype(BF)
            lse_ref[h, pl.ds(i, 1), :] = top + jnp.log2(total)
        return carry

    lax.fori_loop(0, length // block, query_step, 0)


def attend_forward(lo, start, q, k, y, block):
    length, width = q.shape
    count = length // block
    return pl.pallas_call(
        functools.partial(attend_body, block=block),
        grid=(1,),
        in_specs=[
            pl.BlockSpec(memory_space=pltpu.SMEM),
            whole(start.shape),
            whole(q.shape),
            whole(k.shape),
            pl.BlockSpec((length, width), lambda i: (0, 2)),
        ],
        out_specs=[whole(q.shape), whole((width // HD, count, block))],
        out_shape=[sds(q.shape, BF), sds((width // HD, count, block), F32)],
        scratch_shapes=[pltpu.VMEM((width, length), BF)],
        cost_estimate=estimate(2 * length * length * width, 8 * length * width),
        name="attend_forward",
    )(lo, start, q, k, y)


def attend_back_body(lo_ref, start_ref, q_ref, k_ref, v_ref, do_ref, o_ref, lse_ref, cos_ref,
                     sin_ref, ratio_ref, g_ref, kt_ref, dk_ref, dv_ref, *, block):
    length, width = q_ref.shape
    heads = width // HD
    scale = HD ** (-0.5)
    factor = scale * LOG2E
    dk_ref[...] = jnp.zeros_like(dk_ref)
    dv_ref[...] = jnp.zeros_like(dv_ref)
    for h in range(heads):
        kt_ref[h * HD:(h + 1) * HD, :] = k_ref[:, h * HD:(h + 1) * HD].T
    key_iota = lax.broadcasted_iota(jnp.int32, (block, block), 0)
    query_iota = lax.broadcasted_iota(jnp.int32, (1, block), 1)

    def turn_back(grad, base):
        return (
            grad * cos_ref[pl.ds(base, block), :]
            + pltpu.roll(grad, HD // 2, 1) * sin_ref[pl.ds(base, block), :]
        )

    def query_step(i, carry):
        base = pl.multiple_of(i * block, block)
        start = start_ref[pl.ds(i, 1), :]
        place = query_iota + base
        queries, grads, deltas, lses = [], [], [], []
        for h in range(heads):
            cols = slice(h * HD, (h + 1) * HD)
            queries.append(q_ref[pl.ds(base, block), cols])
            grad = do_ref[pl.ds(base, block), cols]
            grads.append(grad)
            product = grad.astype(F32) * o_ref[pl.ds(base, block), cols].astype(F32)
            deltas.append(jnp.sum(product.T, axis=0, keepdims=True))
            lses.append(lse_ref[h, pl.ds(i, 1), :])

        def key_step(j, state):
            at = pl.multiple_of(j * block, block)
            key_place = key_iota + at
            allowed = (key_place >= start) & (key_place <= place)
            result = []
            for h in range(heads):
                cols = slice(h * HD, (h + 1) * HD)
                keys = k_ref[pl.ds(at, block), cols]
                s = dot_nt(keys, queries[h]) * factor
                p = jnp.where(allowed, jnp.exp2(s - lses[h]), 0.0)
                dp = dot_nt(v_ref[pl.ds(at, block), cols], grads[h])
                ds = (p * (dp - deltas[h])).astype(BF)
                dv_ref[pl.ds(at, block), cols] += dot_nn(p.astype(BF), grads[h])
                dk_ref[pl.ds(at, block), cols] += dot_nn(ds, queries[h])
                result.append(state[h] + dot_nn(kt_ref[cols, pl.ds(at, block)], ds))
            return tuple(result)

        first = tuple(jnp.zeros((HD, block), F32) for _ in range(heads))
        state = lax.fori_loop(lo_ref[i], i + 1, key_step, first)
        for h in range(heads):
            cols = slice(h * HD, (h + 1) * HD)
            g_ref[pl.ds(base, block), cols] = (
                turn_back(state[h].T * scale, base) * ratio_ref[:, cols]
            ).astype(BF)
        return carry

    lax.fori_loop(0, length // block, query_step, 0)

    def finish(j, carry):
        base = pl.multiple_of(j * block, block)
        for h in range(heads):
            cols = slice(h * HD, (h + 1) * HD)
            key_cols = slice(width + h * HD, width + (h + 1) * HD)
            value_cols = slice(2 * width + h * HD, 2 * width + (h + 1) * HD)
            g_ref[pl.ds(base, block), key_cols] = (
                turn_back(dk_ref[pl.ds(base, block), cols] * scale, base)
                * ratio_ref[:, key_cols]
            ).astype(BF)
            g_ref[pl.ds(base, block), value_cols] = (
                dv_ref[pl.ds(base, block), cols] * ratio_ref[:, value_cols]
            ).astype(BF)
        return carry

    lax.fori_loop(0, length // block, finish, 0)


def attend_backward(lo, start, q, k, y, grad, attended, lse, cos, sin, ratio, block):
    length, width = q.shape
    return pl.pallas_call(
        functools.partial(attend_back_body, block=block),
        grid=(1,),
        in_specs=[
            pl.BlockSpec(memory_space=pltpu.SMEM),
            whole(start.shape),
            whole(q.shape),
            whole(k.shape),
            pl.BlockSpec((length, width), lambda i: (0, 2)),
            whole(grad.shape),
            whole(attended.shape),
            whole(lse.shape),
            whole(cos.shape),
            whole(sin.shape),
            whole(ratio.shape),
        ],
        out_specs=whole((length, 3 * width)),
        out_shape=sds((length, 3 * width), BF),
        scratch_shapes=[
            pltpu.VMEM((width, length), BF),
            pltpu.VMEM((length, width), F32),
            pltpu.VMEM((length, width), F32),
        ],
        cost_estimate=estimate(5 * length * length * width, 16 * length * width),
        name="attend_backward",
    )(lo, start, q, k, y, grad, attended, lse, cos, sin, ratio)


def ffn_body(x_ref, og_ref, valid_ref, rd_ref, gate_ref, lift_ref, down_ref, rg_ref, rl_ref,
             lgl_ref, ug_ref, ul_ref, ld_ref, ud_ref,
             down_out, back_out, agl_ref, bg_ref, bl_ref, ad_ref, bd_ref, sg_ref, sl_ref,
             gd_ref):
    count, block, width = og_ref.shape

    @pl.when(pl.program_id(0) == 0)
    def _():
        for ref in (agl_ref, bg_ref, bl_ref, ad_ref, bd_ref, sg_ref, sl_ref):
            ref[...] = jnp.zeros_like(ref)

    x = x_ref[...]
    inner_g = dot_nn(x, gate_ref[...])
    inner_u = dot_nn(x, lift_ref[...])
    gate_ratio, lift_ratio = rg_ref[...], rl_ref[...]
    gate_act, lift_act = inner_g * gate_ratio, inner_u * lift_ratio
    sigmoid_g = jax.nn.sigmoid(gate_act)
    silu_g = gate_act * sigmoid_g
    hidden = (silu_g * lift_act).astype(BF)
    down_out[...] = dot_nn(hidden, down_ref[...]).astype(BF)
    valid = valid_ref[...]
    for c in range(count):
        gd_ref[:, c * width:(c + 1) * width] = (
            og_ref[c].astype(F32) * valid * rd_ref[c]
        ).astype(BF)
    grad_down = gd_ref[...]
    grad_hidden = dot_nt(grad_down, down_ref[...])
    d_lift = grad_hidden * silu_g
    d_gate = grad_hidden * lift_act * sigmoid_g * (1.0 + gate_act * (1.0 - sigmoid_g))
    sg_ref[...] += jnp.sum(inner_g * d_gate, axis=0, keepdims=True)
    sl_ref[...] += jnp.sum(inner_u * d_lift, axis=0, keepdims=True)
    grad_g = (d_gate * gate_ratio).astype(BF)
    grad_l = (d_lift * lift_ratio).astype(BF)
    back_out[...] = (dot_nt(grad_g, gate_ref[...]) + dot_nt(grad_l, lift_ref[...])).astype(BF)
    low_x = dot_nn(x, lgl_ref[...]).astype(BF)
    low_g = (dot_nn(grad_g, ug_ref[...]) + dot_nn(grad_l, ul_ref[...])).astype(BF)
    agl_ref[...] += dot_tn(low_g, x)
    bg_ref[...] += dot_tn(low_x, grad_g)
    bl_ref[...] += dot_tn(low_x, grad_l)
    low_h = dot_nn(hidden, ld_ref[...]).astype(BF)
    low_d = dot_nn(grad_down, ud_ref[...]).astype(BF)
    ad_ref[...] += dot_tn(low_d, hidden)
    bd_ref[...] += dot_tn(low_h, grad_down)


def ffn(x, og, valid, rd, gate, lift, down, rg, rl, lgl, ug, ul, ld, ud, block=256):
    length, depth = x.shape
    count, _, width = og.shape
    hidden = gate.shape[1]
    acc_shapes = [
        (RP, depth), (RP, hidden), (RP, hidden), (RP, hidden), (RP, depth),
        (1, hidden), (1, hidden),
    ]
    return pl.pallas_call(
        ffn_body,
        grid=(length // block,),
        in_specs=[
            rows(block, depth),
            chunk_rows(count, block, width),
            rows(block, 1),
            *[whole(a.shape) for a in (rd, gate, lift, down, rg, rl, lgl, ug, ul, ld, ud)],
        ],
        out_specs=[rows(block, depth), rows(block, depth), *[whole(s) for s in acc_shapes]],
        out_shape=[
            sds((length, depth), BF),
            sds((length, depth), BF),
            *[sds(s, F32) for s in acc_shapes],
        ],
        scratch_shapes=[pltpu.VMEM((block, depth), BF)],
        cost_estimate=estimate(14 * length * depth * hidden, 10 * length * depth),
        name="ffn",
    )(x, og, valid, rd, gate, lift, down, rg, rl, lgl, ug, ul, ld, ud)


def out_back_body(g_ref, a_ref, w_ref, u_ref, l_ref, da_ref, aa_ref, bb_ref):
    @pl.when(pl.program_id(0) == 0)
    def _():
        aa_ref[...] = jnp.zeros_like(aa_ref)
        bb_ref[...] = jnp.zeros_like(bb_ref)

    grad, act = g_ref[...], a_ref[...]
    da_ref[...] = dot_nt(grad, w_ref[...]).astype(BF)
    low_g = dot_nn(grad, u_ref[...]).astype(BF)
    low_a = dot_nn(act, l_ref[...]).astype(BF)
    aa_ref[...] += dot_tn(low_g, act)
    bb_ref[...] += dot_tn(low_a, grad)


def out_back(grad, act, w, u, low, block=512):
    length, depth = grad.shape
    width = act.shape[1]
    return pl.pallas_call(
        out_back_body,
        grid=(length // block,),
        in_specs=[
            rows(block, depth), rows(block, width), whole(w.shape), whole(u.shape),
            whole(low.shape),
        ],
        out_specs=[rows(block, width), whole((RP, width)), whole((RP, depth))],
        out_shape=[sds((length, width), BF), sds((RP, width), F32), sds((RP, depth), F32)],
        cost_estimate=estimate(4 * length * depth * width, 3 * length * depth),
        name="out_back",
    )(grad, act, w, u, low)


def qkv_back_body(g_ref, y_ref, x_ref, xl_ref, w_ref, u_ref, inv_ratio_ref,
                  dx_ref, dot_ref, aa_ref, bb_ref, ss_ref):
    @pl.when(pl.program_id(0) == 0)
    def _():
        aa_ref[...] = jnp.zeros_like(aa_ref)
        bb_ref[...] = jnp.zeros_like(bb_ref)
        ss_ref[...] = jnp.zeros_like(ss_ref)

    count, block, width = dx_ref.shape
    grad = g_ref[...]
    product = grad.astype(F32) * y_ref[...].astype(F32) * inv_ratio_ref[...]
    dot_ref[...] = jnp.sum(product, axis=1, keepdims=True)
    ss_ref[...] += jnp.sum(product * inv_ratio_ref[...], axis=0, keepdims=True)
    dx = dot_nt(grad, w_ref[...]).astype(BF)
    for c in range(count):
        dx_ref[c] = dx[:, c * width:(c + 1) * width]
    low_g = dot_nn(grad, u_ref[...]).astype(BF)
    aa_ref[...] += dot_tn(low_g, x_ref[...])
    bb_ref[...] += dot_tn(xl_ref[...], grad)


def qkv_backward(grad, y, x, xl, w_cat, u_cat, inv_ratio, count, block=256):
    length, depth = x.shape
    wide = grad.shape[1]
    width = depth // count
    return pl.pallas_call(
        qkv_back_body,
        grid=(length // block,),
        in_specs=[
            rows(block, wide), rows(block, wide), rows(block, depth), rows(block, RP),
            whole(w_cat.shape), whole(u_cat.shape), whole(inv_ratio.shape),
        ],
        out_specs=[
            chunk_rows(count, block, width), rows(block, 1),
            whole((RP, depth)), whole((RP, wide)), whole((1, wide)),
        ],
        out_shape=[
            sds((count, length, width), BF), sds((length, 1), F32),
            sds((RP, depth), F32), sds((RP, wide), F32), sds((1, wide), F32),
        ],
        cost_estimate=estimate(4 * length * depth * wide, 4 * length * depth),
        name="qkv_backward",
    )(grad, y, x, xl, w_cat, u_cat, inv_ratio)


def split_low(value):
    high = lax.reduce_precision(value, 8, 7)
    return high, value - high


def merge(base, lower, upper):
    lower_high, lower_low = split_low(lower)
    upper_high, upper_low = split_low(2.0 * upper)
    first = jnp.concatenate([lower_high, lower_low, lower_high], axis=1).astype(BF)
    second = jnp.concatenate([upper_high, upper_high, upper_low], axis=0).astype(BF)
    return base.astype(F32) + dot_nn(first, second)


def block_diagonal(blocks):
    height = sum(b.shape[0] for b in blocks)
    at = 0
    result = []
    for b in blocks:
        result.append(jnp.pad(b, ((at, height - at - b.shape[0]), (0, 0))))
        at += b.shape[0]
    return jnp.concatenate(result, axis=1)


def pad_cols(value, at=0):
    return jnp.pad(value, ((0, 0), (at, RP - at - value.shape[1]))).astype(BF)


def tables(lengths, length):
    ends = jnp.cumsum(lengths)
    at = jnp.arange(length, dtype=jnp.int32)
    after = (at[:, None] >= ends[None, :NDOC]).astype(jnp.int32)
    segment = jnp.sum(after, axis=1)
    start = jnp.sum(after * lengths[None, :NDOC], axis=1)
    half = jnp.arange(HD // 2, dtype=F32)
    frequency = ROPE_BASE ** (-(2.0 * half / HD))
    angles = (at - start).astype(F32)[:, None] * frequency[None, :]
    cos, sin = jnp.cos(angles), jnp.sin(angles)
    return (
        start,
        (segment < NDOC).astype(F32)[:, None],
        jnp.concatenate([cos, cos], axis=1),
        jnp.concatenate([sin, -sin], axis=1),
    )


def on_device(
    tokens, doc_lengths, out_grad, attn_gain, ffn_gain,
    query_base, query_lower, query_upper, query_scale,
    key_base, key_lower, key_upper, key_scale,
    value_base, value_lower, value_upper, value_scale,
    output_base, output_lower, output_upper, output_scale,
    gate_base, gate_lower, gate_upper, gate_scale,
    lift_base, lift_lower, lift_upper, lift_scale,
    down_base, down_lower, down_upper, down_scale,
):
    members = lax.axis_size("mp")
    me = lax.axis_index("mp")
    seqs, length, width = tokens.shape
    depth = members * width
    own_tokens = length // members
    hidden = down_base.shape[0]
    block = min(256, length)

    def gather(value):
        return lax.all_gather(value, "mp", axis=0)

    def own_cols(value, size):
        return lax.dynamic_slice_in_dim(value, me * size, size, 1)

    def spread(values):
        pieces = jnp.concatenate(
            [v.reshape(v.shape[0], members, v.shape[1] // members) for v in values], axis=2
        )
        return lax.all_to_all(pieces, "mp", split_axis=1, concat_axis=0, tiled=True)[:, 0]

    pack = jnp.concatenate(
        [
            query_lower, key_lower, value_lower, gate_lower, lift_lower,
            jnp.stack([output_scale, down_scale, attn_gain, ffn_gain], axis=1),
        ],
        axis=1,
    )
    packed = lax.all_gather(pack, "mp", axis=0, tiled=True)
    qkv_base = spread([query_base, key_base, value_base]).reshape(depth, 3 * width)
    gate_cols_base = lax.all_to_all(gate_base, "mp", split_axis=1, concat_axis=0, tiled=True)
    lift_cols_base = lax.all_to_all(lift_base, "mp", split_axis=1, concat_axis=0, tiled=True)
    tok_all = [gather(tokens[s]) for s in range(seqs)]
    og_all = [gather(out_grad[s]) for s in range(seqs)]

    output_w, down_w = merge(output_base, output_lower, output_upper), merge(
        down_base, down_lower, down_upper
    )
    row_stats = lax.psum(
        jnp.concatenate(
            [
                jnp.sum(output_w * output_w, axis=0)[None],
                jnp.sum(down_w * down_w, axis=0)[None],
                dot_tn(output_lower.astype(BF), output_w.astype(BF)),
                dot_tn(down_lower.astype(BF), down_w.astype(BF)),
            ],
            axis=0,
        ),
        "mp",
    )
    output_w, down_w = output_w.astype(BF), down_w.astype(BF)
    norm_o, norm_d = jnp.sqrt(row_stats[0]), jnp.sqrt(row_stats[1])
    cross_o, cross_d = row_stats[2:2 + R], row_stats[2 + R:2 + 2 * R]
    scale_o, scale_d = packed[:, 5 * R], packed[:, 5 * R + 1]
    gain_a, gain_f = packed[:, 5 * R + 2], packed[:, 5 * R + 3]
    ratio_o, ratio_d = scale_o / norm_o, scale_d / norm_d

    lower_qkv, lower_g, lower_l = (
        packed[:, :3 * R], packed[:, 3 * R:4 * R], packed[:, 4 * R:5 * R],
    )
    uppers_qkv = [own_cols(u, width) for u in (query_upper, key_upper, value_upper)]
    upper_qkv = block_diagonal(uppers_qkv)
    upper_g, upper_l = own_cols(gate_upper, hidden), own_cols(lift_upper, hidden)
    qkv_w = merge(qkv_base, lower_qkv, upper_qkv)
    gate_w = merge(gate_cols_base, lower_g, upper_g)
    lift_w = merge(lift_cols_base, lower_l, upper_l)
    norm_qkv = jnp.sqrt(jnp.sum(qkv_w * qkv_w, axis=0))
    norm_g = jnp.sqrt(jnp.sum(gate_w * gate_w, axis=0))
    norm_l = jnp.sqrt(jnp.sum(lift_w * lift_w, axis=0))
    scale_qkv = jnp.concatenate([query_scale, key_scale, value_scale])
    ratio_qkv = (scale_qkv / norm_qkv)[None]
    ratio_g, ratio_l = (gate_scale / norm_g)[None], (lift_scale / norm_l)[None]
    qkv_w, gate_w, lift_w = qkv_w.astype(BF), gate_w.astype(BF), lift_w.astype(BF)
    cross_all = dot_tn(lower_qkv.astype(BF), qkv_w)
    cross_qkv = jnp.concatenate(
        [cross_all[n * R:(n + 1) * R, n * width:(n + 1) * width] for n in range(3)], axis=1
    )
    cross_g, cross_l = dot_tn(lower_g.astype(BF), gate_w), dot_tn(lower_l.astype(BF), lift_w)
    col_stats = gather(
        jnp.concatenate(
            [
                jnp.concatenate([cross_qkv, cross_g, cross_l], axis=1),
                jnp.concatenate(
                    [
                        scale_qkv / norm_qkv ** 3,
                        gate_scale / norm_g ** 3,
                        lift_scale / norm_l ** 3,
                    ]
                )[None],
            ],
            axis=0,
        )
    )

    def col_stat(begin, size):
        part = col_stats[:, :, begin:begin + size]
        return jnp.transpose(part, (1, 0, 2)).reshape(R + 1, members * size)

    low_l_qkv = pad_cols(lower_qkv)
    low_l_gl = pad_cols(packed[:, 3 * R:5 * R])
    low_u_qkv = pad_cols(upper_qkv.T)
    low_u_g, low_u_l = pad_cols(upper_g.T), pad_cols(upper_l.T, R)
    low_l_d, low_u_d = pad_cols(down_lower), pad_cols(down_upper.T)
    low_l_o, low_u_o = pad_cols(output_lower), pad_cols(output_upper.T)
    chunk_gain = gain_a.reshape(members, 1, width)
    chunk_ratio_d = ratio_d.reshape(members, 1, width)
    inv_ratio = 1.0 / ratio_qkv

    def own_rows(value):
        return lax.dynamic_slice_in_dim(value, me * own_tokens, own_tokens, 0)

    def own_of_chunks(value):
        part = lax.dynamic_slice_in_dim(value, me * own_tokens, own_tokens, 1)
        return jnp.transpose(part, (1, 0, 2)).reshape(own_tokens, depth)

    def to_features(value):
        return lax.all_to_all(
            value.astype(BF).reshape(own_tokens, members, width),
            "mp", split_axis=1, concat_axis=0, tiled=True,
        ).reshape(length, width)

    def scatter_tokens(value):
        return lax.psum_scatter(value, "mp", scatter_dimension=0, tiled=True).astype(F32)

    state = [dict() for _ in range(seqs)]

    def attention_stage(s):
        st = state[s]
        start, valid, cos, sin = tables(doc_lengths[s], length)
        st["valid"], st["cos"], st["sin"] = valid, cos, sin
        st["start"] = start.reshape(length // block, block)
        st["lo"] = st["start"][:, 0] // block
        st["x"], st["y"], st["q"], st["k"], st["xl"], st["inv"] = qkv_forward(
            tok_all[s], chunk_gain, qkv_w, low_l_qkv, ratio_qkv, cos, sin
        )
        st["att"], st["lse"] = attend_forward(
            st["lo"], st["start"], st["q"], st["k"], st["y"], block
        )
        st["inner_o"] = scatter_tokens(dot_nn(st["att"], output_w).astype(BF))

    def ffn_stage(s):
        st = state[s]
        residual = own_of_chunks(tok_all[s]).astype(F32) + st["inner_o"] * ratio_o
        inv = lax.rsqrt(jnp.mean(residual * residual, axis=1, keepdims=True) + EPSILON)
        normed = (residual * inv * gain_f).astype(BF)
        st["residual"], st["inv_f"] = residual, inv
        normed_all = lax.all_gather(normed, "mp", axis=0, tiled=True)
        st["ffn"] = ffn(
            normed_all, og_all[s], st["valid"], chunk_ratio_d, gate_w, lift_w, down_w,
            ratio_g, ratio_l, low_l_gl, low_u_g, low_u_l, low_l_d, low_u_d,
        )

    def middle_stage(s):
        st = state[s]
        grad_normed = scatter_tokens(st["ffn"][1])
        grad_top = own_of_chunks(og_all[s]).astype(F32) * own_rows(st["valid"])
        residual, inv = st["residual"], st["inv_f"]
        scaled = gain_f * grad_normed
        dot_f = jnp.sum(residual * scaled, axis=1, keepdims=True)
        grad_residual = grad_top + inv * scaled - residual * (inv ** 3 * dot_f / depth)
        st["g_o"] = jnp.sum(st["inner_o"] * grad_residual, axis=0)
        st["grad_top"] = grad_top
        grad_output = lax.all_gather(
            (grad_residual * ratio_o).astype(BF), "mp", axis=0, tiled=True
        )
        st["grad_residual"] = grad_residual
        grad_att, st["a_o"], st["b_o"] = out_back(
            grad_output, st["att"], output_w, low_u_o, low_l_o
        )
        st["grad_att"] = grad_att

    def late_stage(s):
        st = state[s]
        inner_d = scatter_tokens(st["ffn"][0])
        st["out"] = to_features(st["residual"] + inner_d * ratio_d)
        st["g_d"] = jnp.sum(inner_d * st["grad_top"], axis=0)
        st["feature_residual"] = to_features(st["grad_residual"])

    def attention_back_stage(s):
        st = state[s]
        grads = attend_backward(
            st["lo"], st["start"], st["q"], st["k"], st["y"], st["grad_att"], st["att"],
            st["lse"], st["cos"], st["sin"], ratio_qkv, block,
        )
        dx, st["dot_a"], st["a_qkv"], st["b_qkv"], st["g_qkv"] = qkv_backward(
            grads, st["y"], st["x"], st["xl"], qkv_w, low_u_qkv, inv_ratio, members
        )
        st["dx"] = lax.psum_scatter(dx, "mp", scatter_dimension=0, tiled=False)

    for stage in (attention_stage, ffn_stage, middle_stage, late_stage, attention_back_stage):
        for s in range(seqs):
            stage(s)

    dots = lax.psum(
        jnp.concatenate([state[s]["dot_a"].reshape(1, length) for s in range(seqs)], axis=0), "mp"
    )
    out_rows, in_rows = [], []
    for s in range(seqs):
        st = state[s]
        inv = st["inv"]
        grad = (
            st["feature_residual"].astype(F32)
            + inv * (attn_gain * st["dx"].astype(F32))
            - tokens[s].astype(F32) * (inv * inv * dots[s][:, None] / depth)
        )
        out_rows.append(st["out"])
        in_rows.append(grad)
    out_tokens, in_grad = jnp.stack(out_rows), jnp.stack(in_rows)

    def total(pick):
        result = pick(state[0])
        for s in range(1, seqs):
            result = result + pick(state[s])
        return result

    def place_cols(value, full):
        return lax.dynamic_update_slice_in_dim(
            jnp.zeros((value.shape[0], full), F32), value, me * value.shape[1], 1
        )

    full_hidden = hidden * members
    a_gl = total(lambda st: st["ffn"][2])[:2 * R]
    b_g = total(lambda st: st["ffn"][3])[:R]
    b_l = total(lambda st: st["ffn"][4])[R:2 * R]
    a_d = total(lambda st: st["ffn"][5])[:R]
    b_d = total(lambda st: st["ffn"][6])[:R]
    s_g, s_l = total(lambda st: st["ffn"][7]), total(lambda st: st["ffn"][8])
    a_o, b_o = total(lambda st: st["a_o"])[:R], total(lambda st: st["b_o"])[:R]
    g_o, g_d = total(lambda st: st["g_o"])[None], total(lambda st: st["g_d"])[None]
    a_qkv = total(lambda st: st["a_qkv"])[:3 * R]
    b_all = total(lambda st: st["b_qkv"])
    g_qkv = total(lambda st: st["g_qkv"])
    wide = lax.psum(
        jnp.concatenate(
            [
                place_cols(b_g, full_hidden),
                place_cols(b_l, full_hidden),
                place_cols(a_d, full_hidden),
                place_cols(s_g, full_hidden),
                place_cols(s_l, full_hidden),
            ],
            axis=0,
        ),
        ("dp", "mp"),
    )
    narrow = lax.psum(
        jnp.concatenate([a_gl, b_d, b_o, place_cols(a_o, depth), g_o, g_d], axis=0),
        ("dp", "mp"),
    )
    last = lax.psum(
        jnp.concatenate(
            [a_qkv]
            + [
                place_cols(b_all[n * R:(n + 1) * R, n * width:(n + 1) * width], depth)
                for n in range(3)
            ]
            + [place_cols(g_qkv[:, n * width:(n + 1) * width], depth) for n in range(3)],
            axis=0,
        ),
        ("dp", "mp"),
    )

    results = [out_tokens, in_grad]

    def finish(base, lower, upper, sum_a, sum_b, sum_g, coefficient, cross, norm_own):
        beta = sum_g * coefficient
        scaled = upper * beta[None]
        tilted = scaled.astype(BF)
        own_a = own_cols(sum_a, base.shape[0]).T
        correction = dot_nt(base, tilted) + 2.0 * jnp.dot(
            lower, jnp.dot(upper, scaled.T, precision=lax.Precision.HIGHEST),
            precision=lax.Precision.HIGHEST,
        )
        results.append(2.0 * (own_a - correction))
        results.append(2.0 * (sum_b - cross * beta[None]))
        size = norm_own.shape[0]
        results.append(lax.dynamic_slice_in_dim(sum_g, me * size, size) / norm_own)

    for n, (base, lower, upper) in enumerate(
        (
            (query_base, query_lower, query_upper),
            (key_base, key_lower, key_upper),
            (value_base, value_lower, value_upper),
        )
    ):
        stat = col_stat(n * width, width)
        finish(
            base, lower, upper, last[n * R:(n + 1) * R], last[(3 + n) * R:(4 + n) * R],
            last[6 * R + n], stat[R], stat[:R], norm_qkv[n * width:(n + 1) * width],
        )
    finish(
        output_base, output_lower, output_upper, narrow[4 * R:5 * R], narrow[3 * R:4 * R],
        narrow[5 * R], scale_o / norm_o ** 3, cross_o,
        lax.dynamic_slice_in_dim(norm_o, me * width, width),
    )
    for n, (base, lower, upper, norm) in enumerate(
        ((gate_base, gate_lower, gate_upper, norm_g), (lift_base, lift_lower, lift_upper, norm_l))
    ):
        stat = col_stat(3 * width + n * hidden, hidden)
        finish(
            base, lower, upper, narrow[n * R:(n + 1) * R], wide[n * R:(n + 1) * R],
            wide[3 * R + n], stat[R], stat[:R], norm,
        )
    finish(
        down_base, down_lower, down_upper, wide[2 * R:3 * R], narrow[2 * R:3 * R],
        narrow[5 * R + 1], scale_d / norm_d ** 3, cross_d,
        lax.dynamic_slice_in_dim(norm_d, me * width, width),
    )
    return tuple(results)


def solution(mesh):
    spread, split, rows_spec = P("dp", None, "mp"), P("mp"), P("mp", None)
    weight = (rows_spec, rows_spec, P(), split)
    grads = (rows_spec, P(), split)
    return jax.shard_map(
        on_device,
        mesh=mesh,
        in_specs=(spread, P("dp", None), spread, split, split) + weight * 7,
        out_specs=(spread, spread) + grads * 7,
        check_vma=False,
    )
```

```python
import functools

import jax
import jax.numpy as jnp
from jax import lax
from jax.experimental import pallas as pl
from jax.experimental.pallas import tpu as pltpu
from jax.sharding import PartitionSpec as P

HD = 128
R = 16
RP = 128
NDOC = 5
EPSILON = 1e-05
ROPE_BASE = 10000.0
NEGATIVE = -1e30
LOG2E = 1.4426950408889634
BF = jnp.bfloat16
F32 = jnp.float32


def dot_nn(a, b):
    return lax.dot_general(a, b, (((1,), (0,)), ((), ())), preferred_element_type=F32)


def dot_nt(a, b):
    return lax.dot_general(a, b, (((1,), (1,)), ((), ())), preferred_element_type=F32)


def dot_tn(a, b):
    return lax.dot_general(a, b, (((0,), (0,)), ((), ())), preferred_element_type=F32)


def whole(shape):
    rank = len(shape)
    return pl.BlockSpec(tuple(shape), lambda i: (0,) * rank)


def rows(block, width):
    return pl.BlockSpec((block, width), lambda i: (i, 0))


def chunk_rows(count, block, width):
    return pl.BlockSpec((count, block, width), lambda i: (0, i, 0))


def sds(shape, dtype):
    return jax.ShapeDtypeStruct(tuple(shape), dtype)


def estimate(flops, bytes_accessed):
    return pl.CostEstimate(flops=int(flops), bytes_accessed=int(bytes_accessed), transcendentals=0)


def smem():
    return pl.BlockSpec(memory_space=pltpu.SMEM)


def bit_of(me, k):
    return (me // (1 << k)) % 2


def chunk_of(me, half, place, levels):
    result = 0
    for k in range(levels):
        bit = bit_of(me, k)
        flip = half if k == 0 else (place >> (levels - 1 - k)) & 1
        result = result + ((1 - bit) if flip else bit) * (1 << k)
    return result


def other(me, k):
    return {"mp": me + (1 << k) * (1 - 2 * bit_of(me, k))}


def meet(me, levels):
    barrier = pltpu.get_barrier_semaphore()
    for k in range(levels):
        pl.semaphore_signal(
            barrier, inc=1, device_id=other(me, k), device_id_type=pl.DeviceIdType.MESH
        )
    pl.semaphore_wait(barrier, levels)


def scatter_scratch(count, blocks, block, width):
    levels = count.bit_length() - 1
    shapes = []
    for level in range(levels):
        size = (count >> 1, block, width) if level == 0 else (2, count >> (level + 1), block // 2, width)
        shapes += [
            pltpu.VMEM(size, BF),
            pltpu.VMEM(size, BF),
            pltpu.VMEM((blocks,) + size, BF),
            pltpu.SemaphoreType.DMA((blocks,) if level == 0 else (blocks, 2)),
            pltpu.SemaphoreType.DMA((blocks,) if level == 0 else (blocks, 2)),
        ]
    return shapes


class Scatter:
    def __init__(self, me, count, refs, out_ref):
        self.me, self.levels, self.out_ref = me, count.bit_length() - 1, out_ref
        self.count = count
        self.keep, self.send, self.land, self.sent, self.landed = (
            [refs[5 * level + n] for level in range(self.levels)] for n in range(5)
        )
        self.blocks = self.land[0].shape[0]
        self.block = self.land[0].shape[2]

    def copy(self, level, b, path):
        if level == 0:
            bit, src, at = 0, self.send[0], (b,)
        else:
            bit = level if path == 0 else self.levels - level
            src, at = self.send[level].at[path], (b, path)
        return pltpu.make_async_remote_copy(
            src_ref=src,
            dst_ref=self.land[level].at[at],
            send_sem=self.sent[level].at[at],
            recv_sem=self.landed[level].at[at],
            device_id=other(self.me, bit),
            device_id_type=pl.DeviceIdType.MESH,
        )

    def pass_on(self, level, path, places, place, value):
        upper = place >= places // 2 if path == 0 else place % 2 == 1
        at = place % (places // 2) if path == 0 else place // 2
        ref = self.send[level + 1] if upper else self.keep[level + 1]
        ref[path, at] = value.astype(BF)

    def finish(self, level, b):
        half = self.block // 2
        if level == 0:
            self.copy(0, b, 0).wait()
            places = self.count // 2
            for place in range(places):
                value = self.keep[0][place].astype(F32) + self.land[0][b, place].astype(F32)
                self.pass_on(0, 0, places, place, value[:half])
                self.pass_on(0, 1, places, place, value[half:])
        else:
            for path in range(2):
                self.copy(level, b, path).wait()
                places = self.count >> (level + 1)
                for place in range(places):
                    value = (
                        self.keep[level][path, place].astype(F32)
                        + self.land[level][b, path, place].astype(F32)
                    )
                    if level < self.levels - 1:
                        self.pass_on(level, path, places, place, value)
                    else:
                        at = pl.multiple_of(b * self.block + path * half, half)
                        self.out_ref[pl.ds(at, half), :] = value.astype(self.out_ref.dtype)
        if level < self.levels - 1:
            for path in range(2):
                self.copy(level + 1, b, path).start()

    def advance(self, step):
        for level in range(self.levels - 1, -1, -1):
            b = step - level - 1

            @pl.when((b >= 0) & (b < self.blocks))
            def _():
                self.finish(level, b)

    def chunks(self, width):
        for half in range(2):
            for place in range(self.count // 2):
                at = chunk_of(self.me, half, place, self.levels) * width
                ref = self.send[0] if half else self.keep[0]
                yield ref, place, pl.ds(pl.multiple_of(at, width), width)


def once(shape):
    rank = len(shape)
    return pl.BlockSpec(tuple(shape), lambda i: (0,) * rank, pipeline_mode=pl.Buffered(1))


def upto(last, block, width):
    return pl.BlockSpec((block, width), lambda i: (jnp.minimum(i, last), 0))


def chunk_upto(last, count, block, width):
    return pl.BlockSpec((count, block, width), lambda i: (0, jnp.minimum(i, last), 0))


def arrange_body(*refs):
    out_ref = refs[-1]
    count = out_ref.shape[0]
    at = 0
    for ref in refs[:-1]:
        size = ref.shape[1] // count
        for c in range(count):
            out_ref[c, :, at:at + size] = ref[:, c * size:(c + 1) * size]
        at += size


def arrange(values, count):
    height = values[0].shape[0]
    size = sum(v.shape[1] for v in values) // count
    block = height // 2
    return pl.pallas_call(
        arrange_body,
        grid=(2,),
        in_specs=[rows(block, v.shape[1]) for v in values],
        out_specs=chunk_rows(count, block, size),
        out_shape=sds((count, height, size), BF),
        cost_estimate=estimate(0, 4 * count * height * size),
        name="arrange",
    )(*values)


def merge_body(base_ref, l3_ref, u3_ref, l_ref, *refs):
    w_refs, square_ref, cross_ref = refs[:-2], refs[-2], refs[-1]

    @pl.when(pl.program_id(0) == 0)
    def _():
        square_ref[...] = jnp.zeros_like(square_ref)
        cross_ref[...] = jnp.zeros_like(cross_ref)

    value = base_ref[0].astype(F32) + dot_tn(l3_ref[...], u3_ref[...])
    low = value.astype(BF)
    at = 0
    for ref in w_refs:
        ref[0] = low[:, at:at + ref.shape[2]]
        at += ref.shape[2]
    square_ref[...] += jnp.sum(value * value, axis=0, keepdims=True)
    cross_ref[...] += dot_nn(l_ref[...], low)


def merge(base, lower_t, upper, splits=None):
    count, height, width = base.shape
    splits = splits or [width]
    rank = lower_t.shape[0]
    lower_high, lower_low = split_low(lower_t)
    upper_high, upper_low = split_low(2.0 * upper)
    l3 = jnp.concatenate([lower_high, lower_low, lower_high], axis=0).astype(BF)
    u3 = jnp.concatenate([upper_high, upper_high, upper_low], axis=0).astype(BF)
    return pl.pallas_call(
        merge_body,
        grid=(count,),
        in_specs=[
            pl.BlockSpec((1, height, width), lambda i: (i, 0, 0)),
            pl.BlockSpec((3 * rank, height), lambda i: (0, i)),
            whole(u3.shape),
            pl.BlockSpec((rank, height), lambda i: (0, i)),
        ],
        out_specs=[
            *[pl.BlockSpec((1, height, n), lambda i: (i, 0, 0)) for n in splits],
            whole((1, width)),
            whole((rank, width)),
        ],
        out_shape=[
            *[sds((count, height, n), BF) for n in splits],
            sds((1, width), F32), sds((rank, width), F32),
        ],
        cost_estimate=estimate(
            8 * count * height * width * rank, 4 * count * height * width
        ),
        name="merge",
    )(base, l3, u3, lower_t.astype(BF))


def qkv_body(tok_ref, gain_ref, w_ref, l_ref, ratio_ref, cos_ref, sin_ref,
             x_ref, y_ref, q_ref, k_ref, xl_ref, inv_ref):
    count, block, width = tok_ref.shape
    total = jnp.zeros((block, 1), F32)
    for c in range(count):
        part = tok_ref[c].astype(F32)
        total = total + jnp.sum(part * part, axis=1, keepdims=True)
    inv = lax.rsqrt(total / (count * width) + EPSILON)
    inv_ref[...] = inv
    for c in range(count):
        x_ref[:, c * width:(c + 1) * width] = (
            tok_ref[c].astype(F32) * inv * gain_ref[c]
        ).astype(BF)
    y = dot_nn(x_ref[...], w_ref[...]) * ratio_ref[...]
    xl_ref[...] = dot_nt(x_ref[...], l_ref[...]).astype(BF)
    y_ref[...] = y.astype(BF)
    cos, sin = cos_ref[...], sin_ref[...]
    for number, out_ref in ((0, q_ref), (1, k_ref)):
        for h in range(width // HD):
            v = y[:, number * width + h * HD:number * width + (h + 1) * HD]
            out_ref[:, h * HD:(h + 1) * HD] = (
                v * cos - pltpu.roll(v, HD // 2, 1) * sin
            ).astype(BF)


def qkv_forward(tok, gain, w_cat, l_cat, ratio, cos, sin, block=256):
    count, length, width = tok.shape
    depth = count * width
    return pl.pallas_call(
        qkv_body,
        grid=(length // block,),
        in_specs=[
            chunk_rows(count, block, width),
            whole(gain.shape),
            whole(w_cat.shape),
            whole(l_cat.shape),
            whole(ratio.shape),
            rows(block, HD),
            rows(block, HD),
        ],
        out_specs=[
            rows(block, depth),
            rows(block, 3 * width),
            rows(block, width),
            rows(block, width),
            rows(block, RP),
            rows(block, 1),
        ],
        out_shape=[
            sds((length, depth), BF),
            sds((length, 3 * width), BF),
            sds((length, width), BF),
            sds((length, width), BF),
            sds((length, RP), BF),
            sds((length, 1), F32),
        ],
        cost_estimate=estimate(2 * length * depth * (3 * width + RP), 6 * length * depth),
        name="qkv_forward",
    )(tok, gain, w_cat, l_cat, ratio, cos, sin)


def attend_body(lo_ref, start_ref, q_ref, k_ref, v_ref, o_ref, lse_ref, vt_ref, *, block):
    length, width = q_ref.shape
    heads = width // HD
    factor = HD ** (-0.5) * LOG2E
    for h in range(heads):
        vt_ref[h * HD:(h + 1) * HD, :] = v_ref[:, h * HD:(h + 1) * HD].T
    key_iota = lax.broadcasted_iota(jnp.int32, (block, block), 0)
    query_iota = lax.broadcasted_iota(jnp.int32, (1, block), 1)

    def query_step(i, carry):
        base = pl.multiple_of(i * block, block)
        start = start_ref[pl.ds(i, 1), :]
        place = query_iota + base
        queries = [q_ref[pl.ds(base, block), h * HD:(h + 1) * HD] for h in range(heads)]

        def key_step(j, state):
            at = pl.multiple_of(j * block, block)
            key_place = key_iota + at
            allowed = (key_place >= start) & (key_place <= place)
            result = []
            for h in range(heads):
                top, total, acc = state[h]
                keys = k_ref[pl.ds(at, block), h * HD:(h + 1) * HD]
                s = jnp.where(allowed, dot_nt(keys, queries[h]) * factor, NEGATIVE)
                new_top = jnp.maximum(top, jnp.max(s, axis=0, keepdims=True))
                scale = jnp.exp2(top - new_top)
                p = jnp.exp2(s - new_top)
                total = total * scale + jnp.sum(p, axis=0, keepdims=True)
                acc = acc * scale + dot_nn(
                    vt_ref[h * HD:(h + 1) * HD, pl.ds(at, block)], p.astype(BF)
                )
                result.append((new_top, total, acc))
            return tuple(result)

        first = tuple(
            (
                jnp.full((1, block), NEGATIVE, F32),
                jnp.zeros((1, block), F32),
                jnp.zeros((HD, block), F32),
            )
            for _ in range(heads)
        )
        state = lax.fori_loop(lo_ref[i], i + 1, key_step, first)
        for h in range(heads):
            top, total, acc = state[h]
            o_ref[pl.ds(base, block), h * HD:(h + 1) * HD] = (acc / total).T.astype(BF)
            lse_ref[h, pl.ds(i, 1), :] = top + jnp.log2(total)
        return carry

    lax.fori_loop(0, length // block, query_step, 0)


def attend_forward(lo, start, q, k, y, block):
    length, width = q.shape
    count = length // block
    return pl.pallas_call(
        functools.partial(attend_body, block=block),
        grid=(1,),
        in_specs=[
            pl.BlockSpec(memory_space=pltpu.SMEM),
            whole(start.shape),
            whole(q.shape),
            whole(k.shape),
            pl.BlockSpec((length, width), lambda i: (0, 2)),
        ],
        out_specs=[whole(q.shape), whole((width // HD, count, block))],
        out_shape=[sds(q.shape, BF), sds((width // HD, count, block), F32)],
        scratch_shapes=[pltpu.VMEM((width, length), BF)],
        cost_estimate=estimate(2 * length * length * width, 8 * length * width),
        name="attend_forward",
    )(lo, start, q, k, y)


def attend_back_body(lo_ref, start_ref, q_ref, k_ref, v_ref, do_ref, o_ref, lse_ref, cos_ref,
                     sin_ref, ratio_ref, g_ref, kt_ref, dk_ref, dv_ref, *, block):
    length, width = q_ref.shape
    heads = width // HD
    scale = HD ** (-0.5)
    factor = scale * LOG2E
    dk_ref[...] = jnp.zeros_like(dk_ref)
    dv_ref[...] = jnp.zeros_like(dv_ref)
    for h in range(heads):
        kt_ref[h * HD:(h + 1) * HD, :] = k_ref[:, h * HD:(h + 1) * HD].T
    key_iota = lax.broadcasted_iota(jnp.int32, (block, block), 0)
    query_iota = lax.broadcasted_iota(jnp.int32, (1, block), 1)

    def turn_back(grad, base):
        return (
            grad * cos_ref[pl.ds(base, block), :]
            + pltpu.roll(grad, HD // 2, 1) * sin_ref[pl.ds(base, block), :]
        )

    def query_step(i, carry):
        base = pl.multiple_of(i * block, block)
        start = start_ref[pl.ds(i, 1), :]
        place = query_iota + base
        queries, grads, deltas, lses = [], [], [], []
        for h in range(heads):
            cols = slice(h * HD, (h + 1) * HD)
            queries.append(q_ref[pl.ds(base, block), cols])
            grad = do_ref[pl.ds(base, block), cols]
            grads.append(grad)
            product = grad.astype(F32) * o_ref[pl.ds(base, block), cols].astype(F32)
            deltas.append(jnp.sum(product.T, axis=0, keepdims=True))
            lses.append(lse_ref[h, pl.ds(i, 1), :])

        def key_step(j, state):
            at = pl.multiple_of(j * block, block)
            key_place = key_iota + at
            allowed = (key_place >= start) & (key_place <= place)
            result = []
            for h in range(heads):
                cols = slice(h * HD, (h + 1) * HD)
                keys = k_ref[pl.ds(at, block), cols]
                s = dot_nt(keys, queries[h]) * factor
                p = jnp.where(allowed, jnp.exp2(s - lses[h]), 0.0)
                dp = dot_nt(v_ref[pl.ds(at, block), cols], grads[h])
                ds = (p * (dp - deltas[h])).astype(BF)
                dv_ref[pl.ds(at, block), cols] += dot_nn(p.astype(BF), grads[h])
                dk_ref[pl.ds(at, block), cols] += dot_nn(ds, queries[h])
                result.append(state[h] + dot_nn(kt_ref[cols, pl.ds(at, block)], ds))
            return tuple(result)

        first = tuple(jnp.zeros((HD, block), F32) for _ in range(heads))
        state = lax.fori_loop(lo_ref[i], i + 1, key_step, first)
        for h in range(heads):
            cols = slice(h * HD, (h + 1) * HD)
            g_ref[pl.ds(base, block), cols] = (
                turn_back(state[h].T * scale, base) * ratio_ref[:, cols]
            ).astype(BF)
        return carry

    lax.fori_loop(0, length // block, query_step, 0)

    def finish(j, carry):
        base = pl.multiple_of(j * block, block)
        for h in range(heads):
            cols = slice(h * HD, (h + 1) * HD)
            key_cols = slice(width + h * HD, width + (h + 1) * HD)
            value_cols = slice(2 * width + h * HD, 2 * width + (h + 1) * HD)
            g_ref[pl.ds(base, block), key_cols] = (
                turn_back(dk_ref[pl.ds(base, block), cols] * scale, base)
                * ratio_ref[:, key_cols]
            ).astype(BF)
            g_ref[pl.ds(base, block), value_cols] = (
                dv_ref[pl.ds(base, block), cols] * ratio_ref[:, value_cols]
            ).astype(BF)
        return carry

    lax.fori_loop(0, length // block, finish, 0)


def attend_backward(lo, start, q, k, y, grad, attended, lse, cos, sin, ratio, block):
    length, width = q.shape
    return pl.pallas_call(
        functools.partial(attend_back_body, block=block),
        grid=(1,),
        in_specs=[
            pl.BlockSpec(memory_space=pltpu.SMEM),
            whole(start.shape),
            whole(q.shape),
            whole(k.shape),
            pl.BlockSpec((length, width), lambda i: (0, 2)),
            whole(grad.shape),
            whole(attended.shape),
            whole(lse.shape),
            whole(cos.shape),
            whole(sin.shape),
            whole(ratio.shape),
        ],
        out_specs=whole((length, 3 * width)),
        out_shape=sds((length, 3 * width), BF),
        scratch_shapes=[
            pltpu.VMEM((width, length), BF),
            pltpu.VMEM((length, width), F32),
            pltpu.VMEM((length, width), F32),
        ],
        cost_estimate=estimate(5 * length * length * width, 16 * length * width),
        name="attend_backward",
    )(lo, start, q, k, y, grad, attended, lse, cos, sin, ratio)


def out_body(a_ref, w_ref, out_ref, *scratch):
    width = out_ref.shape[1]
    count = w_ref.shape[1] // width
    step, me = pl.program_id(0), lax.axis_index("mp")
    sums = Scatter(me, count, scratch, out_ref)

    @pl.when(step == 0)
    def _():
        meet(me, sums.levels)

    sums.advance(step)

    @pl.when(step < sums.blocks)
    def _():
        act = a_ref[...]
        for ref, place, cols in sums.chunks(width):
            ref[place] = dot_nn(act, w_ref[:, cols]).astype(BF)
        sums.copy(0, step, 0).start()


def out_forward(act, w, block=256):
    length, width = act.shape
    depth = w.shape[1]
    count, blocks = depth // width, length // block
    levels = count.bit_length() - 1
    return pl.pallas_call(
        out_body,
        grid=(blocks + levels,),
        in_specs=[upto(blocks - 1, block, width), once(w.shape)],
        out_specs=whole((length, width)),
        out_shape=sds((length, width), BF),
        scratch_shapes=scatter_scratch(count, blocks, block, width),
        compiler_params=pltpu.CompilerParams(collective_id=1, has_side_effects=True),
        cost_estimate=estimate(2 * length * depth * width, 40 * length * depth),
        name="out_forward",
    )(act, w)


def ffn_body(res_ref, gain_ref, gd_in_ref, gate_ref, lift_ref, down_ref,
             rg_ref, rl_ref, lgl_ref, ug_ref, ul_ref, ld_ref, ud_ref,
             down_out, back_out, inv_ref, dot_ref,
             agl_ref, bg_ref, bl_ref, ad_ref, bd_ref, sg_ref, sl_ref,
             x_ref, gd_ref, *scratch):
    count, block, width = res_ref.shape
    step, me = pl.program_id(0), lax.axis_index("mp")
    half = len(scratch) // 2
    back_sums = Scatter(me, count, scratch[:half], back_out)
    down_sums = Scatter(me, count, scratch[half:], down_out)

    @pl.when(step == 0)
    def _():
        meet(me, back_sums.levels)
        for ref in (agl_ref, bg_ref, bl_ref, ad_ref, bd_ref, sg_ref, sl_ref):
            ref[...] = jnp.zeros_like(ref)

    back_sums.advance(step)
    down_sums.advance(step)

    @pl.when(step < back_sums.blocks)
    def _():
        total = jnp.zeros((block, 1), F32)
        for c in range(count):
            part = res_ref[c].astype(F32)
            total = total + jnp.sum(part * part, axis=1, keepdims=True)
        inv = lax.rsqrt(total / (count * width) + EPSILON)
        inv_ref[...] = inv
        for c in range(count):
            cols = slice(c * width, (c + 1) * width)
            x_ref[:, cols] = (res_ref[c].astype(F32) * inv * gain_ref[c]).astype(BF)
            gd_ref[:, cols] = gd_in_ref[c]
        x, grad_down = x_ref[...], gd_ref[...]
        inner_g = dot_nn(x, gate_ref[...])
        inner_u = dot_nn(x, lift_ref[...])
        gate_ratio, lift_ratio = rg_ref[...], rl_ref[...]
        gate_act, lift_act = inner_g * gate_ratio, inner_u * lift_ratio
        sigmoid_g = jax.nn.sigmoid(gate_act)
        silu_g = gate_act * sigmoid_g
        hidden = (silu_g * lift_act).astype(BF)
        for ref, place, at in down_sums.chunks(width):
            ref[place] = dot_nn(hidden, down_ref[:, at]).astype(BF)
        down_sums.copy(0, step, 0).start()
        grad_hidden = dot_nt(grad_down, down_ref[...])
        d_lift = grad_hidden * silu_g
        d_gate = grad_hidden * lift_act * sigmoid_g * (1.0 + gate_act * (1.0 - sigmoid_g))
        grad_g = (d_gate * gate_ratio).astype(BF)
        grad_l = (d_lift * lift_ratio).astype(BF)
        for ref, place, at in back_sums.chunks(width):
            ref[place] = (
                dot_nt(grad_g, gate_ref[at, :]) + dot_nt(grad_l, lift_ref[at, :])
            ).astype(BF)
        back_sums.copy(0, step, 0).start()
        product_g, product_l = inner_g * d_gate, inner_u * d_lift
        sg_ref[...] += jnp.sum(product_g, axis=0, keepdims=True)
        sl_ref[...] += jnp.sum(product_l, axis=0, keepdims=True)
        dot_ref[...] = jnp.sum(
            product_g * gate_ratio + product_l * lift_ratio, axis=1, keepdims=True
        )
        low_x = dot_nt(x, lgl_ref[...]).astype(BF)
        low_g = (dot_nt(grad_g, ug_ref[...]) + dot_nt(grad_l, ul_ref[...])).astype(BF)
        agl_ref[...] += dot_tn(low_g, x)
        bg_ref[...] += dot_tn(low_x, grad_g)
        bl_ref[...] += dot_tn(low_x, grad_l)
        low_h = dot_nn(hidden, ld_ref[...]).astype(BF)
        low_d = dot_nt(grad_down, ud_ref[...]).astype(BF)
        ad_ref[...] += dot_tn(low_d, hidden)
        bd_ref[...] += dot_tn(low_h, grad_down)


def ffn(res, gain, gd, gate, lift, down, rg, rl, lgl, ug, ul, ld, ud, block=256):
    count, length, width = res.shape
    depth, hidden = gate.shape
    blocks = length // block
    levels = count.bit_length() - 1
    acc_shapes = [
        (RP, depth), (RP, hidden), (RP, hidden), (RP, hidden), (RP, depth),
        (1, hidden), (1, hidden),
    ]
    return pl.pallas_call(
        ffn_body,
        grid=(blocks + levels,),
        in_specs=[
            chunk_upto(blocks - 1, count, block, width),
            once(gain.shape),
            chunk_upto(blocks - 1, count, block, width),
            *[once(a.shape) for a in (gate, lift, down, rg, rl, lgl, ug, ul, ld, ud)],
        ],
        out_specs=[
            whole((length, width)), whole((length, width)),
            upto(blocks - 1, block, 1), upto(blocks - 1, block, 1),
            *[whole(s) for s in acc_shapes],
        ],
        out_shape=[
            sds((length, width), BF), sds((length, width), BF),
            sds((length, 1), F32), sds((length, 1), F32),
            *[sds(s, F32) for s in acc_shapes],
        ],
        scratch_shapes=[
            pltpu.VMEM((block, depth), BF), pltpu.VMEM((block, depth), BF),
            *scatter_scratch(count, blocks, block, width),
            *scatter_scratch(count, blocks, block, width),
        ],
        compiler_params=pltpu.CompilerParams(collective_id=2, has_side_effects=True),
        cost_estimate=estimate(14 * length * depth * hidden, 40 * length * depth),
        name="ffn",
    )(res, gain, gd, gate, lift, down, rg, rl, lgl, ug, ul, ld, ud)


def out_back_body(g_ref, a_ref, w_ref, u_ref, l_ref, da_ref, aa_ref, bb_ref, grad_ref):
    count, block, width = g_ref.shape

    @pl.when(pl.program_id(0) == 0)
    def _():
        aa_ref[...] = jnp.zeros_like(aa_ref)
        bb_ref[...] = jnp.zeros_like(bb_ref)

    for c in range(count):
        grad_ref[:, c * width:(c + 1) * width] = g_ref[c]
    grad, act = grad_ref[...], a_ref[...]
    da_ref[...] = dot_nt(grad, w_ref[...]).astype(BF)
    low_g = dot_nt(grad, u_ref[...]).astype(BF)
    low_a = dot_nn(act, l_ref[...]).astype(BF)
    aa_ref[...] += dot_tn(low_g, act)
    bb_ref[...] += dot_tn(low_a, grad)


def out_back(grad, act, w, u, low, block=256):
    count, length, width = grad.shape
    depth = count * width
    return pl.pallas_call(
        out_back_body,
        grid=(length // block,),
        in_specs=[
            chunk_rows(count, block, width), rows(block, width), whole(w.shape),
            whole(u.shape), whole(low.shape),
        ],
        out_specs=[rows(block, width), whole((RP, width)), whole((RP, depth))],
        out_shape=[sds((length, width), BF), sds((RP, width), F32), sds((RP, depth), F32)],
        scratch_shapes=[pltpu.VMEM((block, depth), BF)],
        cost_estimate=estimate(4 * length * depth * width, 3 * length * depth),
        name="out_back",
    )(grad, act, w, u, low)


def qkv_back_body(g_ref, y_ref, x_ref, xl_ref, w_ref, u_ref, inv_ratio_ref,
                  dx_ref, dot_ref, aa_ref, bb_ref, ss_ref, *scratch):
    width = dx_ref.shape[1]
    count = w_ref.shape[0] // width
    step, me = pl.program_id(0), lax.axis_index("mp")
    sums = Scatter(me, count, scratch, dx_ref)

    @pl.when(step == 0)
    def _():
        meet(me, sums.levels)
        aa_ref[...] = jnp.zeros_like(aa_ref)
        bb_ref[...] = jnp.zeros_like(bb_ref)
        ss_ref[...] = jnp.zeros_like(ss_ref)

    sums.advance(step)

    @pl.when(step < sums.blocks)
    def _():
        grad = g_ref[...]
        for ref, place, at in sums.chunks(width):
            ref[place] = dot_nt(grad, w_ref[at, :]).astype(BF)
        sums.copy(0, step, 0).start()
        product = grad.astype(F32) * y_ref[...].astype(F32) * inv_ratio_ref[...]
        dot_ref[...] = jnp.sum(product, axis=1, keepdims=True)
        ss_ref[...] += jnp.sum(product * inv_ratio_ref[...], axis=0, keepdims=True)
        low_g = dot_nt(grad, u_ref[...]).astype(BF)
        aa_ref[...] += dot_tn(low_g, x_ref[...])
        bb_ref[...] += dot_tn(xl_ref[...], grad)


def qkv_backward(grad, y, x, xl, w_cat, u_cat, inv_ratio, count, block=256):
    length, depth = x.shape
    wide = grad.shape[1]
    width, blocks = depth // count, length // block
    levels = count.bit_length() - 1
    return pl.pallas_call(
        qkv_back_body,
        grid=(blocks + levels,),
        in_specs=[
            upto(blocks - 1, block, wide), upto(blocks - 1, block, wide),
            upto(blocks - 1, block, depth), upto(blocks - 1, block, RP),
            once(w_cat.shape), once(u_cat.shape), once(inv_ratio.shape),
        ],
        out_specs=[
            whole((length, width)), upto(blocks - 1, block, 1),
            whole((RP, depth)), whole((RP, wide)), whole((1, wide)),
        ],
        out_shape=[
            sds((length, width), BF), sds((length, 1), F32),
            sds((RP, depth), F32), sds((RP, wide), F32), sds((1, wide), F32),
        ],
        scratch_shapes=scatter_scratch(count, blocks, block, width),
        compiler_params=pltpu.CompilerParams(collective_id=3, has_side_effects=True),
        cost_estimate=estimate(4 * length * depth * wide, 40 * length * depth),
        name="qkv_backward",
    )(grad, y, x, xl, w_cat, u_cat, inv_ratio)


def split_low(value):
    high = lax.reduce_precision(value, 8, 7)
    return high, value - high


def block_diagonal(blocks):
    width = sum(b.shape[1] for b in blocks)
    at = 0
    result = []
    for b in blocks:
        result.append(jnp.pad(b, ((0, 0), (at, width - at - b.shape[1]))))
        at += b.shape[1]
    return jnp.concatenate(result, axis=0)


def pad_rows(value, at=0):
    return jnp.pad(value, ((at, RP - at - value.shape[0]), (0, 0))).astype(BF)


def flip(value, bit, axis="mp"):
    size = lax.axis_size(axis)
    return lax.ppermute(value, axis, [(i, i ^ (1 << bit)) for i in range(size)])


def all_sum(value, axis):
    for bit in range(lax.axis_size(axis).bit_length() - 1):
        value = value + flip(value, bit, axis)
    return value


def scatter_cols(value, me):
    members = lax.axis_size("mp")
    part = jnp.transpose(value.reshape(value.shape[0], members, -1), (1, 0, 2))
    for bit in range(members.bit_length() - 1):
        mine = (me >> bit) & 1
        pair = part.reshape(part.shape[0] // 2, 2, *part.shape[1:])
        keep = lax.dynamic_index_in_dim(pair, mine, 1, keepdims=False)
        away = lax.dynamic_index_in_dim(pair, 1 - mine, 1, keepdims=False)
        part = keep + flip(away, bit)
    return part[0]


def tie(value, *others):
    return lax.optimization_barrier((value, *others))[0]


def tables(lengths, length):
    ends = jnp.cumsum(lengths)
    at = jnp.arange(length, dtype=jnp.int32)
    after = (at[:, None] >= ends[None, :NDOC]).astype(jnp.int32)
    segment = jnp.sum(after, axis=1)
    start = jnp.sum(after * lengths[None, :NDOC], axis=1)
    half = jnp.arange(HD // 2, dtype=F32)
    frequency = ROPE_BASE ** (-(2.0 * half / HD))
    angles = (at - start).astype(F32)[:, None] * frequency[None, :]
    cos, sin = jnp.cos(angles), jnp.sin(angles)
    return (
        start,
        (segment < NDOC).astype(F32)[:, None],
        jnp.concatenate([cos, cos], axis=1),
        jnp.concatenate([sin, -sin], axis=1),
    )


def on_device(
    tokens, doc_lengths, out_grad, attn_gain, ffn_gain,
    query_base, query_lower, query_upper, query_scale,
    key_base, key_lower, key_upper, key_scale,
    value_base, value_lower, value_upper, value_scale,
    output_base, output_lower, output_upper, output_scale,
    gate_base, gate_lower, gate_upper, gate_scale,
    lift_base, lift_lower, lift_upper, lift_scale,
    down_base, down_lower, down_upper, down_scale,
):
    members = lax.axis_size("mp")
    me = lax.axis_index("mp")
    seqs, length, width = tokens.shape
    depth = members * width
    hidden = down_base.shape[0]
    block = min(256, length)

    def gather(value):
        return lax.all_gather(value, "mp", axis=0)

    def own_cols(value, size):
        return lax.dynamic_slice_in_dim(value, me * size, size, 1)

    def exchange(value):
        return lax.all_to_all(value, "mp", split_axis=0, concat_axis=0, tiled=True)

    qkv_base = exchange(arrange([query_base, key_base, value_base], members))
    pack = jnp.concatenate(
        [
            query_lower.T, key_lower.T, value_lower.T, gate_lower.T, lift_lower.T,
            jnp.stack([attn_gain, ffn_gain]),
        ],
        axis=0,
    )
    pack = jnp.pad(pack, ((0, 160 - pack.shape[0]), (0, 0)))
    packed = jnp.transpose(gather(pack), (1, 0, 2)).reshape(pack.shape[0], depth)
    tok_all = [gather(tokens[s]) for s in range(seqs)]
    lower_qkv_t, lower_gl_t = packed[:3 * R], packed[3 * R:5 * R]
    gain_a, gain_f = packed[5 * R], packed[5 * R + 1]

    output_w, square_o, cross_o = merge(output_base[None], output_lower.T, output_upper)
    down_w, square_d, cross_d = merge(down_base[None], down_lower.T, down_upper)
    row_stats = scatter_cols(
        jnp.concatenate([square_o, square_d, cross_o, cross_d], axis=0), me
    )
    output_w, down_w = output_w[0], down_w[0]
    norm_o, norm_d = jnp.sqrt(row_stats[0]), jnp.sqrt(row_stats[1])
    cross_o, cross_d = row_stats[2:2 + R], row_stats[2 + R:2 + 2 * R]
    ratio_o, ratio_d = output_scale / norm_o, down_scale / norm_d
    layouts = [tables(doc_lengths[s], length) for s in range(seqs)]
    grad_tops = [out_grad[s].astype(F32) * layouts[s][1] for s in range(seqs)]
    gd_all = [gather((grad_tops[s] * ratio_d).astype(BF)) for s in range(seqs)]

    upper_qkv = block_diagonal([own_cols(u, width) for u in (query_upper, key_upper, value_upper)])
    upper_g, upper_l = own_cols(gate_upper, hidden), own_cols(lift_upper, hidden)
    qkv_w, square_qkv, cross_all = merge(qkv_base, lower_qkv_t, upper_qkv)
    qkv_w = qkv_w.reshape(depth, 3 * width)
    norm_qkv = jnp.sqrt(square_qkv[0])
    scale_qkv = jnp.concatenate([query_scale, key_scale, value_scale])
    ratio_qkv = (scale_qkv / norm_qkv)[None]
    inv_ratio = 1.0 / ratio_qkv

    gl_arranged = arrange([gate_base, lift_base], members)
    gl_base = exchange(gl_arranged)
    gate_w, lift_w, square_gl, cross_gl = merge(
        gl_base, lower_gl_t, block_diagonal([upper_g, upper_l]), [hidden, hidden]
    )
    gate_w, lift_w = gate_w.reshape(depth, hidden), lift_w.reshape(depth, hidden)
    norm_gl = jnp.sqrt(square_gl[0])
    norm_g, norm_l = norm_gl[:hidden], norm_gl[hidden:]
    ratio_g, ratio_l = (gate_scale / norm_g)[None], (lift_scale / norm_l)[None]

    low_l_qkv, low_l_gl = pad_rows(lower_qkv_t), pad_rows(lower_gl_t)
    low_u_qkv, low_u_g, low_u_l = pad_rows(upper_qkv), pad_rows(upper_g), pad_rows(upper_l, R)
    low_l_d, low_u_d = pad_rows(down_lower.T).T, pad_rows(down_upper)
    low_l_o, low_u_o = pad_rows(output_lower.T).T, pad_rows(output_upper)
    chunk_gain_a, chunk_gain_f = (v.reshape(members, 1, width) for v in (gain_a, gain_f))

    state = [dict() for _ in range(seqs)]

    def attention_stage(s):
        st = state[s]
        start, _, st["cos"], st["sin"] = layouts[s]
        st["start"] = start.reshape(length // block, block)
        st["lo"] = st["start"][:, 0] // block
        tok = tie(tok_all[s], gl_arranged) if s == 0 else tok_all[s]
        st["x"], st["y"], st["q"], st["k"], st["xl"], st["inv"] = qkv_forward(
            tok, chunk_gain_a, qkv_w, low_l_qkv, ratio_qkv, st["cos"], st["sin"]
        )
        st["att"], st["lse"] = attend_forward(
            st["lo"], st["start"], st["q"], st["k"], st["y"], block
        )
        act = tie(st["att"], gate_w, lift_w) if s == seqs - 1 else st["att"]
        st["inner_o"] = out_forward(act, output_w).astype(F32)
        st["residual"] = tokens[s].astype(F32) + st["inner_o"] * ratio_o
        st["residual_all"] = gather(st["residual"].astype(BF))

    def ffn_stage(s):
        st = state[s]
        st["inner_d"], back, st["inv_f"], dot_f, *st["ffn"] = ffn(
            st["residual_all"], chunk_gain_f, gd_all[s], gate_w, lift_w, down_w,
            ratio_g, ratio_l, low_l_gl, low_u_g, low_u_l, low_l_d, low_u_d,
        )
        dot_f = all_sum(dot_f.reshape(1, length), "mp").reshape(length, 1)
        inv = st["inv_f"]
        grad_residual = (
            grad_tops[s] + inv * (ffn_gain * back.astype(F32))
            - st["residual"] * (inv * inv * dot_f / depth)
        )
        st["grad_residual"] = grad_residual
        st["grad_output"] = gather((grad_residual * ratio_o).astype(BF))
        inner_d = st["inner_d"].astype(F32)
        st["out"] = (st["residual"] + inner_d * ratio_d).astype(BF)
        st["g_d"] = jnp.sum(inner_d * grad_tops[s], axis=0)
        st["g_o"] = jnp.sum(st["inner_o"] * grad_residual, axis=0)

    def attention_back_stage(s):
        st = state[s]
        grad_att, st["a_o"], st["b_o"] = out_back(
            st["grad_output"], st["att"], output_w, low_u_o, low_l_o
        )
        grads = attend_backward(
            st["lo"], st["start"], st["q"], st["k"], st["y"], grad_att, st["att"],
            st["lse"], st["cos"], st["sin"], ratio_qkv, block,
        )
        dx, dot_a, st["a_qkv"], st["b_qkv"], st["g_qkv"] = qkv_backward(
            grads, st["y"], st["x"], st["xl"], qkv_w, low_u_qkv, inv_ratio, members
        )
        dot_a = all_sum(dot_a.reshape(1, length), "mp").reshape(length, 1)
        inv = st["inv"]
        st["in_grad"] = (
            st["grad_residual"] + inv * (attn_gain * dx.astype(F32))
            - tokens[s].astype(F32) * (inv * inv * dot_a / depth)
        )

    for stage in (attention_stage, ffn_stage, attention_back_stage):
        for s in range(seqs):
            stage(s)

    out_tokens = jnp.stack([st["out"] for st in state])
    in_grad = jnp.stack([st["in_grad"] for st in state])

    def total(pick):
        result = pick(state[0])
        for s in range(1, seqs):
            result = result + pick(state[s])
        return result

    def blocks_of(value, size):
        return jnp.concatenate(
            [value[n * R:(n + 1) * R, n * size:(n + 1) * size] for n in range(value.shape[0] // R)],
            axis=0,
        )

    parts = scatter_cols(
        jnp.concatenate(
            [
                total(lambda st: st["ffn"][0])[:2 * R],
                total(lambda st: st["ffn"][4])[:R],
                total(lambda st: st["b_o"])[:R],
            ],
            axis=0,
        ),
        me,
    )
    early = all_sum(
        jnp.concatenate(
            [
                parts,
                total(lambda st: st["a_o"])[:R],
                total(lambda st: st["g_o"])[None],
                total(lambda st: st["g_d"])[None],
            ],
            axis=0,
        ),
        "dp",
    )
    early_hidden = all_sum(
        jnp.concatenate(
            [
                total(lambda st: st["ffn"][1])[:R],
                total(lambda st: st["ffn"][2])[R:2 * R],
                total(lambda st: st["ffn"][3])[:R],
                total(lambda st: st["ffn"][5]),
                total(lambda st: st["ffn"][6]),
            ],
            axis=0,
        ),
        "dp",
    )
    late = all_sum(
        jnp.concatenate(
            [
                scatter_cols(total(lambda st: st["a_qkv"])[:3 * R], me),
                blocks_of(total(lambda st: st["b_qkv"])[:3 * R], width),
                total(lambda st: st["g_qkv"]).reshape(3, width),
            ],
            axis=0,
        ),
        "dp",
    )

    def column_side(sum_b, sum_g, cross, scale, norm):
        beta = sum_g * scale / norm ** 3
        return jnp.concatenate([2.0 * (sum_b - cross * beta[None]), beta[None]], axis=0), sum_g / norm

    cols, scale_grads = [None] * 7, [None] * 7
    cross_qkv = blocks_of(cross_all, width)
    for n in range(3):
        cols[n], scale_grads[n] = column_side(
            late[(3 + n) * R:(4 + n) * R], late[6 * R + n], cross_qkv[n * R:(n + 1) * R],
            scale_qkv[n * width:(n + 1) * width], norm_qkv[n * width:(n + 1) * width],
        )
    cols[3], scale_grads[3] = column_side(
        early[3 * R:4 * R], early[5 * R], cross_o, output_scale, norm_o
    )
    cols[6], scale_grads[6] = column_side(
        early[2 * R:3 * R], early[5 * R + 1], cross_d, down_scale, norm_d
    )
    for n, scale, norm in ((0, gate_scale, norm_g), (1, lift_scale, norm_l)):
        cols[4 + n], scale_grads[4 + n] = column_side(
            early_hidden[n * R:(n + 1) * R], early_hidden[3 * R + n],
            cross_gl[n * R:(n + 1) * R, n * hidden:(n + 1) * hidden], scale, norm,
        )

    def spread_cols(names):
        full = gather(jnp.concatenate([cols[n] for n in names], axis=0))
        full = jnp.transpose(full, (1, 0, 2)).reshape(full.shape[1], -1)
        for at, n in enumerate(names):
            cols[n] = full[at * (R + 1):(at + 1) * (R + 1)]

    spread_cols((3, 6))
    spread_cols((4, 5))
    spread_cols((0, 1, 2))

    results = [out_tokens, in_grad]
    own_a = [late[:R], late[R:2 * R], late[2 * R:3 * R], early[4 * R:5 * R], early[:R],
             early[R:2 * R], early_hidden[2 * R:3 * R]]
    for n, (base, lower, upper) in enumerate(
        (
            (query_base, query_lower, query_upper),
            (key_base, key_lower, key_upper),
            (value_base, value_lower, value_upper),
            (output_base, output_lower, output_upper),
            (gate_base, gate_lower, gate_upper),
            (lift_base, lift_lower, lift_upper),
            (down_base, down_lower, down_upper),
        )
    ):
        scaled = upper * cols[n][R][None]
        core = jnp.dot(scaled, upper.T, precision=lax.Precision.HIGHEST)
        correction = dot_nt(scaled.astype(BF), base) + 2.0 * jnp.dot(
            core, lower.T, precision=lax.Precision.HIGHEST
        )
        results += [(2.0 * (own_a[n] - correction)).T, cols[n][:R], scale_grads[n]]
    return tuple(results)


def solution(mesh):
    spread, split, rows_spec = P("dp", None, "mp"), P("mp"), P("mp", None)
    weight = (rows_spec, rows_spec, P(), split)
    grads = (rows_spec, P(), split)
    return jax.shard_map(
        on_device,
        mesh=mesh,
        in_specs=(spread, P("dp", None), spread, split, split) + weight * 7,
        out_specs=(spread, spread) + grads * 7,
        check_vma=False,
    )
```

```python
import functools

import jax
import jax.numpy as jnp
from jax import lax
from jax.experimental import pallas as pl
from jax.experimental.pallas import tpu as pltpu
from jax.sharding import PartitionSpec as P


HD = 128
R = 16
RP = 128
NDOC = 5
EPSILON = 1e-05
ROPE_BASE = 10000.0
NEGATIVE = -1e30
LOG2E = 1.4426950408889634
BF = jnp.bfloat16
F32 = jnp.float32


def dot_nn(a, b):
    return lax.dot_general(a, b, (((1,), (0,)), ((), ())), preferred_element_type=F32)


def dot_nt(a, b):
    return lax.dot_general(a, b, (((1,), (1,)), ((), ())), preferred_element_type=F32)


def dot_tn(a, b):
    return lax.dot_general(a, b, (((0,), (0,)), ((), ())), preferred_element_type=F32)


def whole(shape):
    rank = len(shape)
    return pl.BlockSpec(tuple(shape), lambda i: (0,) * rank)


def rows(block, width):
    return pl.BlockSpec((block, width), lambda i: (i, 0))


def chunk_rows(count, block, width):
    return pl.BlockSpec((count, block, width), lambda i: (0, i, 0))


def sds(shape, dtype):
    return jax.ShapeDtypeStruct(tuple(shape), dtype)


def estimate(flops, bytes_accessed):
    return pl.CostEstimate(flops=int(flops), bytes_accessed=int(bytes_accessed), transcendentals=0)


def bit_of(me, k):
    return (me // (1 << k)) % 2


def chunk_of(me, half, place, levels):
    result = 0
    for k in range(levels):
        bit = bit_of(me, k)
        flip = half if k == 0 else (place >> (levels - 1 - k)) & 1
        result = result + ((1 - bit) if flip else bit) * (1 << k)
    return result


def other(me, k):
    return {"mp": me + (1 << k) * (1 - 2 * bit_of(me, k))}


def meet(me, levels):
    barrier = pltpu.get_barrier_semaphore()
    for k in range(levels):
        pl.semaphore_signal(
            barrier, inc=1, device_id=other(me, k), device_id_type=pl.DeviceIdType.MESH
        )
    pl.semaphore_wait(barrier, levels)


def scatter_scratch(count, blocks, block, width):
    levels = count.bit_length() - 1
    shapes = []
    for level in range(levels):
        size = (count >> 1, block, width) if level == 0 else (2, count >> (level + 1), block // 2, width)
        shapes += [
            pltpu.VMEM(size, BF),
            pltpu.VMEM(size, BF),
            pltpu.VMEM((blocks,) + size, BF),
            pltpu.SemaphoreType.DMA((blocks,) if level == 0 else (blocks, 2)),
            pltpu.SemaphoreType.DMA((blocks,) if level == 0 else (blocks, 2)),
        ]
    return shapes


class Scatter:
    def __init__(self, me, count, refs, out_ref):
        self.me, self.levels, self.out_ref = me, count.bit_length() - 1, out_ref
        self.count = count
        self.keep, self.send, self.land, self.sent, self.landed = (
            [refs[5 * level + n] for level in range(self.levels)] for n in range(5)
        )
        self.blocks = self.land[0].shape[0]
        self.block = self.land[0].shape[2]

    def copy(self, level, b, path):
        if level == 0:
            bit, src, at = 0, self.send[0], (b,)
        else:
            bit = level if path == 0 else self.levels - level
            src, at = self.send[level].at[path], (b, path)
        return pltpu.make_async_remote_copy(
            src_ref=src,
            dst_ref=self.land[level].at[at],
            send_sem=self.sent[level].at[at],
            recv_sem=self.landed[level].at[at],
            device_id=other(self.me, bit),
            device_id_type=pl.DeviceIdType.MESH,
        )

    def pass_on(self, level, path, places, place, value):
        upper = place >= places // 2 if path == 0 else place % 2 == 1
        at = place % (places // 2) if path == 0 else place // 2
        ref = self.send[level + 1] if upper else self.keep[level + 1]
        ref[path, at] = value.astype(BF)

    def finish(self, level, b):
        half = self.block // 2
        if level == 0:
            self.copy(0, b, 0).wait()
            places = self.count // 2
            for place in range(places):
                value = self.keep[0][place].astype(F32) + self.land[0][b, place].astype(F32)
                self.pass_on(0, 0, places, place, value[:half])
                self.pass_on(0, 1, places, place, value[half:])
        else:
            for path in range(2):
                self.copy(level, b, path).wait()
                places = self.count >> (level + 1)
                for place in range(places):
                    value = (
                        self.keep[level][path, place].astype(F32)
                        + self.land[level][b, path, place].astype(F32)
                    )
                    if level < self.levels - 1:
                        self.pass_on(level, path, places, place, value)
                    else:
                        at = pl.multiple_of(b * self.block + path * half, half)
                        self.out_ref[pl.ds(at, half), :] = value.astype(self.out_ref.dtype)
        if level < self.levels - 1:
            for path in range(2):
                self.copy(level + 1, b, path).start()

    def advance(self, step):
        for level in range(self.levels - 1, -1, -1):
            b = step - level - 1

            @pl.when((b >= 0) & (b < self.blocks))
            def _():
                self.finish(level, b)

    def chunks(self, width):
        for half in range(2):
            for place in range(self.count // 2):
                at = chunk_of(self.me, half, place, self.levels) * width
                ref = self.send[0] if half else self.keep[0]
                yield ref, place, pl.ds(pl.multiple_of(at, width), width)


def row_scratch(count, blocks, block):
    levels = count.bit_length() - 1
    return [
        pltpu.VMEM((levels, 8, block), F32),
        pltpu.VMEM((blocks, levels, 8, block), F32),
        pltpu.SemaphoreType.DMA((blocks, levels)),
        pltpu.SemaphoreType.DMA((blocks, levels)),
    ]


class RowSum:
    def __init__(self, me, refs, out_ref):
        self.me, self.out_ref = me, out_ref
        self.held, self.land, self.sent, self.landed = refs
        self.levels, _, self.block = self.held.shape
        self.blocks = self.land.shape[0]

    def copy(self, level, b):
        return pltpu.make_async_remote_copy(
            src_ref=self.held.at[level],
            dst_ref=self.land.at[b, level],
            send_sem=self.sent.at[b, level],
            recv_sem=self.landed.at[b, level],
            device_id=other(self.me, level),
            device_id_type=pl.DeviceIdType.MESH,
        )

    def begin(self, b, value):
        self.held[0] = jnp.broadcast_to(value, (self.block, 128)).T[:8]
        self.copy(0, b).start()

    def advance(self, step):
        for level in range(self.levels - 1, -1, -1):
            b = step - level - 1

            @pl.when((b >= 0) & (b < self.blocks))
            def _():
                self.copy(level, b).wait()
                value = self.held[level] + self.land[b, level]
                if level < self.levels - 1:
                    self.held[level + 1] = value
                    self.copy(level + 1, b).start()
                else:
                    at = pl.multiple_of(b * self.block, self.block)
                    column = jnp.broadcast_to(value[:1], (128, self.block)).T
                    self.out_ref[pl.ds(at, self.block), :] = column[:, :1]


def once(shape):
    rank = len(shape)
    return pl.BlockSpec(tuple(shape), lambda i: (0,) * rank, pipeline_mode=pl.Buffered(1))


def upto(last, block, width):
    return pl.BlockSpec((block, width), lambda i: (jnp.minimum(i, last), 0))


def chunk_upto(last, count, block, width):
    return pl.BlockSpec((count, block, width), lambda i: (0, jnp.minimum(i, last), 0))


def arrange_body(*refs):
    out_ref = refs[-1]
    count = out_ref.shape[0]
    at = 0
    for ref in refs[:-1]:
        size = ref.shape[1] // count
        for c in range(count):
            out_ref[c, :, at:at + size] = ref[:, c * size:(c + 1) * size]
        at += size


def arrange(values, count):
    height = values[0].shape[0]
    size = sum(v.shape[1] for v in values) // count
    block = height // 2
    return pl.pallas_call(
        arrange_body,
        grid=(2,),
        in_specs=[rows(block, v.shape[1]) for v in values],
        out_specs=chunk_rows(count, block, size),
        out_shape=sds((count, height, size), BF),
        cost_estimate=estimate(0, 4 * count * height * size),
        name="arrange",
    )(*values)


def merge_body(base_ref, l3_ref, u3_ref, l_ref, *refs):
    splits = (len(refs) - 1) // 2
    w_refs, square_ref, cross_refs = refs[:splits], refs[splits], refs[splits + 1:]

    @pl.when(pl.program_id(0) == 0)
    def _():
        for ref in (square_ref, *cross_refs):
            ref[...] = jnp.zeros_like(ref)

    value = base_ref[0].astype(F32) + dot_tn(l3_ref[...], u3_ref[...])
    low = value.astype(BF)
    at = 0
    for ref, cross_ref in zip(w_refs, cross_refs):
        ref[0] = low[:, at:at + ref.shape[2]]
        at += ref.shape[2]
        cross_ref[...] += dot_nn(l_ref[...], ref[0])
    square_ref[...] += jnp.sum(value * value, axis=0, keepdims=True)


def merge(base, lower_t, upper, splits=None):
    count, height, width = base.shape
    splits = splits or [width]
    rank = lower_t.shape[0]
    lower_high, lower_low = split_low(lower_t)
    upper_high, upper_low = split_low(2.0 * upper)
    l3 = jnp.concatenate([lower_high, lower_low, lower_high], axis=0).astype(BF)
    u3 = jnp.concatenate([upper_high, upper_high, upper_low], axis=0).astype(BF)
    return pl.pallas_call(
        merge_body,
        grid=(count,),
        in_specs=[
            pl.BlockSpec((1, height, width), lambda i: (i, 0, 0)),
            pl.BlockSpec((3 * rank, height), lambda i: (0, i)),
            whole(u3.shape),
            pl.BlockSpec((rank, height), lambda i: (0, i)),
        ],
        out_specs=[
            *[pl.BlockSpec((1, height, n), lambda i: (i, 0, 0)) for n in splits],
            whole((1, width)),
            *[whole((rank, n)) for n in splits],
        ],
        out_shape=[
            *[sds((count, height, n), BF) for n in splits],
            sds((1, width), F32),
            *[sds((rank, n), F32) for n in splits],
        ],
        cost_estimate=estimate(
            8 * count * height * width * rank, 4 * count * height * width
        ),
        name="merge",
    )(base, l3, u3, lower_t.astype(BF))


def qkv_body(tok_ref, gain_ref, w_ref, l_ref, ratio_ref, cos_ref, sin_ref,
             x_ref, y_ref, q_ref, k_ref, xl_ref, inv_ref):
    count, block, width = tok_ref.shape
    total = jnp.zeros((block, 1), F32)
    for c in range(count):
        part = tok_ref[c].astype(F32)
        total = total + jnp.sum(part * part, axis=1, keepdims=True)
    inv = lax.rsqrt(total / (count * width) + EPSILON)
    inv_ref[...] = inv
    for c in range(count):
        x_ref[:, c * width:(c + 1) * width] = (
            tok_ref[c].astype(F32) * inv * gain_ref[c]
        ).astype(BF)
    y = dot_nn(x_ref[...], w_ref[...]) * ratio_ref[...]
    xl_ref[...] = dot_nt(x_ref[...], l_ref[...]).astype(BF)
    y_ref[...] = y.astype(BF)
    cos, sin = cos_ref[...], sin_ref[...]
    for number, out_ref in ((0, q_ref), (1, k_ref)):
        for h in range(width // HD):
            v = y[:, number * width + h * HD:number * width + (h + 1) * HD]
            out_ref[:, h * HD:(h + 1) * HD] = (
                v * cos - pltpu.roll(v, HD // 2, 1) * sin
            ).astype(BF)


def qkv_forward(tok, gain, w_cat, l_cat, ratio, cos, sin, block=256):
    count, length, width = tok.shape
    depth = count * width
    return pl.pallas_call(
        qkv_body,
        grid=(length // block,),
        in_specs=[
            chunk_rows(count, block, width),
            whole(gain.shape),
            whole(w_cat.shape),
            whole(l_cat.shape),
            whole(ratio.shape),
            rows(block, HD),
            rows(block, HD),
        ],
        out_specs=[
            rows(block, depth),
            rows(block, 3 * width),
            rows(block, width),
            rows(block, width),
            rows(block, RP),
            rows(block, 1),
        ],
        out_shape=[
            sds((length, depth), BF),
            sds((length, 3 * width), BF),
            sds((length, width), BF),
            sds((length, width), BF),
            sds((length, RP), BF),
            sds((length, 1), F32),
        ],
        cost_estimate=estimate(2 * length * depth * (3 * width + RP), 6 * length * depth),
        name="qkv_forward",
    )(tok, gain, w_cat, l_cat, ratio, cos, sin)


def attend_body(lo_ref, start_ref, q_ref, k_ref, v_ref, o_ref, lse_ref, vt_ref, *, block):
    length, width = q_ref.shape
    heads = width // HD
    factor = HD ** (-0.5) * LOG2E
    for h in range(heads):
        vt_ref[h * HD:(h + 1) * HD, :] = v_ref[:, h * HD:(h + 1) * HD].T
    key_iota = lax.broadcasted_iota(jnp.int32, (block, block), 0)
    query_iota = lax.broadcasted_iota(jnp.int32, (1, block), 1)

    def query_step(i, carry):
        base = pl.multiple_of(i * block, block)
        start = start_ref[pl.ds(i, 1), :]
        place = query_iota + base
        queries = [q_ref[pl.ds(base, block), h * HD:(h + 1) * HD] for h in range(heads)]

        def key_step(j, state):
            at = pl.multiple_of(j * block, block)
            key_place = key_iota + at
            allowed = (key_place >= start) & (key_place <= place)
            result = []
            for h in range(heads):
                top, total, acc = state[h]
                keys = k_ref[pl.ds(at, block), h * HD:(h + 1) * HD]
                s = jnp.where(allowed, dot_nt(keys, queries[h]) * factor, NEGATIVE)
                new_top = jnp.maximum(top, jnp.max(s, axis=0, keepdims=True))
                scale = jnp.exp2(top - new_top)
                p = jnp.exp2(s - new_top)
                total = total * scale + jnp.sum(p, axis=0, keepdims=True)
                acc = acc * scale + dot_nn(
                    vt_ref[h * HD:(h + 1) * HD, pl.ds(at, block)], p.astype(BF)
                )
                result.append((new_top, total, acc))
            return tuple(result)

        first = tuple(
            (
                jnp.full((1, block), NEGATIVE, F32),
                jnp.zeros((1, block), F32),
                jnp.zeros((HD, block), F32),
            )
            for _ in range(heads)
        )
        state = lax.fori_loop(lo_ref[i], i + 1, key_step, first)
        for h in range(heads):
            top, total, acc = state[h]
            o_ref[pl.ds(base, block), h * HD:(h + 1) * HD] = (acc / total).T.astype(BF)
            lse_ref[h, pl.ds(i, 1), :] = top + jnp.log2(total)
        return carry

    lax.fori_loop(0, length // block, query_step, 0)


def attend_forward(lo, start, q, k, y, block):
    length, width = q.shape
    count = length // block
    return pl.pallas_call(
        functools.partial(attend_body, block=block),
        grid=(1,),
        in_specs=[
            pl.BlockSpec(memory_space=pltpu.SMEM),
            whole(start.shape),
            whole(q.shape),
            whole(k.shape),
            pl.BlockSpec((length, width), lambda i: (0, 2)),
        ],
        out_specs=[whole(q.shape), whole((width // HD, count, block))],
        out_shape=[sds(q.shape, BF), sds((width // HD, count, block), F32)],
        scratch_shapes=[pltpu.VMEM((width, length), BF)],
        cost_estimate=estimate(2 * length * length * width, 8 * length * width),
        name="attend_forward",
    )(lo, start, q, k, y)


def attend_back_body(lo_ref, start_ref, q_ref, k_ref, v_ref, do_ref, o_ref, lse_ref, cos_ref,
                     sin_ref, ratio_ref, g_ref, kt_ref, dk_ref, dv_ref, *, block):
    length, width = q_ref.shape
    heads = width // HD
    scale = HD ** (-0.5)
    factor = scale * LOG2E
    dk_ref[...] = jnp.zeros_like(dk_ref)
    dv_ref[...] = jnp.zeros_like(dv_ref)
    for h in range(heads):
        kt_ref[h * HD:(h + 1) * HD, :] = k_ref[:, h * HD:(h + 1) * HD].T
    key_iota = lax.broadcasted_iota(jnp.int32, (block, block), 0)
    query_iota = lax.broadcasted_iota(jnp.int32, (1, block), 1)

    def turn_back(grad, base):
        return (
            grad * cos_ref[pl.ds(base, block), :]
            + pltpu.roll(grad, HD // 2, 1) * sin_ref[pl.ds(base, block), :]
        )

    def query_step(i, carry):
        base = pl.multiple_of(i * block, block)
        start = start_ref[pl.ds(i, 1), :]
        place = query_iota + base
        queries, grads, deltas, lses = [], [], [], []
        for h in range(heads):
            cols = slice(h * HD, (h + 1) * HD)
            queries.append(q_ref[pl.ds(base, block), cols])
            grad = do_ref[pl.ds(base, block), cols]
            grads.append(grad)
            product = grad.astype(F32) * o_ref[pl.ds(base, block), cols].astype(F32)
            deltas.append(jnp.sum(product.T, axis=0, keepdims=True))
            lses.append(lse_ref[h, pl.ds(i, 1), :])

        def key_step(j, state):
            at = pl.multiple_of(j * block, block)
            key_place = key_iota + at
            allowed = (key_place >= start) & (key_place <= place)
            result = []
            for h in range(heads):
                cols = slice(h * HD, (h + 1) * HD)
                keys = k_ref[pl.ds(at, block), cols]
                s = dot_nt(keys, queries[h]) * factor
                p = jnp.where(allowed, jnp.exp2(s - lses[h]), 0.0)
                dp = dot_nt(v_ref[pl.ds(at, block), cols], grads[h])
                ds = (p * (dp - deltas[h])).astype(BF)
                dv_ref[pl.ds(at, block), cols] += dot_nn(p.astype(BF), grads[h])
                dk_ref[pl.ds(at, block), cols] += dot_nn(ds, queries[h])
                result.append(state[h] + dot_nn(kt_ref[cols, pl.ds(at, block)], ds))
            return tuple(result)

        first = tuple(jnp.zeros((HD, block), F32) for _ in range(heads))
        state = lax.fori_loop(lo_ref[i], i + 1, key_step, first)
        for h in range(heads):
            cols = slice(h * HD, (h + 1) * HD)
            g_ref[pl.ds(base, block), cols] = (
                turn_back(state[h].T * scale, base) * ratio_ref[:, cols]
            ).astype(BF)
        return carry

    lax.fori_loop(0, length // block, query_step, 0)

    def finish(j, carry):
        base = pl.multiple_of(j * block, block)
        for h in range(heads):
            cols = slice(h * HD, (h + 1) * HD)
            key_cols = slice(width + h * HD, width + (h + 1) * HD)
            value_cols = slice(2 * width + h * HD, 2 * width + (h + 1) * HD)
            g_ref[pl.ds(base, block), key_cols] = (
                turn_back(dk_ref[pl.ds(base, block), cols] * scale, base)
                * ratio_ref[:, key_cols]
            ).astype(BF)
            g_ref[pl.ds(base, block), value_cols] = (
                dv_ref[pl.ds(base, block), cols] * ratio_ref[:, value_cols]
            ).astype(BF)
        return carry

    lax.fori_loop(0, length // block, finish, 0)


def attend_backward(lo, start, q, k, y, grad, attended, lse, cos, sin, ratio, block):
    length, width = q.shape
    return pl.pallas_call(
        functools.partial(attend_back_body, block=block),
        grid=(1,),
        in_specs=[
            pl.BlockSpec(memory_space=pltpu.SMEM),
            whole(start.shape),
            whole(q.shape),
            whole(k.shape),
            pl.BlockSpec((length, width), lambda i: (0, 2)),
            whole(grad.shape),
            whole(attended.shape),
            whole(lse.shape),
            whole(cos.shape),
            whole(sin.shape),
            whole(ratio.shape),
        ],
        out_specs=whole((length, 3 * width)),
        out_shape=sds((length, 3 * width), BF),
        scratch_shapes=[
            pltpu.VMEM((width, length), BF),
            pltpu.VMEM((length, width), F32),
            pltpu.VMEM((length, width), F32),
        ],
        cost_estimate=estimate(5 * length * length * width, 16 * length * width),
        name="attend_backward",
    )(lo, start, q, k, y, grad, attended, lse, cos, sin, ratio)


def out_body(a_ref, w_ref, out_ref, *scratch):
    width = out_ref.shape[1]
    count = w_ref.shape[1] // width
    step, me = pl.program_id(0), lax.axis_index("mp")
    sums = Scatter(me, count, scratch, out_ref)

    @pl.when(step == 0)
    def _():
        meet(me, sums.levels)

    sums.advance(step)

    @pl.when(step < sums.blocks)
    def _():
        act = a_ref[...]
        for ref, place, cols in sums.chunks(width):
            ref[place] = dot_nn(act, w_ref[:, cols]).astype(BF)
        sums.copy(0, step, 0).start()


def out_forward(act, w, block=256):
    length, width = act.shape
    depth = w.shape[1]
    count, blocks = depth // width, length // block
    levels = count.bit_length() - 1
    return pl.pallas_call(
        out_body,
        grid=(blocks + levels,),
        in_specs=[upto(blocks - 1, block, width), once(w.shape)],
        out_specs=whole((length, width)),
        out_shape=sds((length, width), BF),
        scratch_shapes=scatter_scratch(count, blocks, block, width),
        compiler_params=pltpu.CompilerParams(collective_id=1, has_side_effects=True),
        cost_estimate=estimate(2 * length * depth * width, 40 * length * depth),
        name="out_forward",
    )(act, w)


def ffn_body(res_ref, gain_ref, gd_in_ref, gate_ref, lift_ref, down_ref,
             rg_ref, rl_ref, lgl_ref, ug_ref, ul_ref, ld_ref, ud_ref,
             down_out, back_out, inv_ref, dot_ref,
             agl_ref, bg_ref, bl_ref, ad_ref, bd_ref, sg_ref, sl_ref,
             x_ref, gd_ref, *scratch):
    count, block, width = res_ref.shape
    step, me = pl.program_id(0), lax.axis_index("mp")
    row_sums = RowSum(me, scratch[:4], dot_ref)
    half = (len(scratch) - 4) // 2
    back_sums = Scatter(me, count, scratch[4:4 + half], back_out)
    down_sums = Scatter(me, count, scratch[4 + half:], down_out)

    @pl.when(step == 0)
    def _():
        meet(me, back_sums.levels)
        for ref in (agl_ref, bg_ref, bl_ref, ad_ref, bd_ref, sg_ref, sl_ref):
            ref[...] = jnp.zeros_like(ref)

    back_sums.advance(step)
    down_sums.advance(step)
    row_sums.advance(step)

    @pl.when(step < back_sums.blocks)
    def _():
        total = jnp.zeros((block, 1), F32)
        for c in range(count):
            part = res_ref[c].astype(F32)
            total = total + jnp.sum(part * part, axis=1, keepdims=True)
        inv = lax.rsqrt(total / (count * width) + EPSILON)
        inv_ref[...] = inv
        for c in range(count):
            cols = slice(c * width, (c + 1) * width)
            x_ref[:, cols] = (res_ref[c].astype(F32) * inv * gain_ref[c]).astype(BF)
            gd_ref[:, cols] = gd_in_ref[c]
        x, grad_down = x_ref[...], gd_ref[...]
        inner_g = dot_nn(x, gate_ref[...])
        inner_u = dot_nn(x, lift_ref[...])
        gate_ratio, lift_ratio = rg_ref[...], rl_ref[...]
        gate_act, lift_act = inner_g * gate_ratio, inner_u * lift_ratio
        sigmoid_g = jax.nn.sigmoid(gate_act)
        silu_g = gate_act * sigmoid_g
        hidden = (silu_g * lift_act).astype(BF)
        for ref, place, at in down_sums.chunks(width):
            ref[place] = dot_nn(hidden, down_ref[:, at]).astype(BF)
        down_sums.copy(0, step, 0).start()
        grad_hidden = dot_nt(grad_down, down_ref[...])
        d_lift = grad_hidden * silu_g
        d_gate = grad_hidden * lift_act * sigmoid_g * (1.0 + gate_act * (1.0 - sigmoid_g))
        grad_g = (d_gate * gate_ratio).astype(BF)
        grad_l = (d_lift * lift_ratio).astype(BF)
        for ref, place, at in back_sums.chunks(width):
            ref[place] = (
                dot_nt(grad_g, gate_ref[at, :]) + dot_nt(grad_l, lift_ref[at, :])
            ).astype(BF)
        back_sums.copy(0, step, 0).start()
        product_g, product_l = inner_g * d_gate, inner_u * d_lift
        sg_ref[...] += jnp.sum(product_g, axis=0, keepdims=True)
        sl_ref[...] += jnp.sum(product_l, axis=0, keepdims=True)
        row_sums.begin(
            step,
            jnp.sum(product_g * gate_ratio + product_l * lift_ratio, axis=1, keepdims=True),
        )
        low_x = dot_nt(x, lgl_ref[...]).astype(BF)
        low_g = (dot_nt(grad_g, ug_ref[...]) + dot_nt(grad_l, ul_ref[...])).astype(BF)
        agl_ref[...] += dot_tn(low_g, x)
        bg_ref[...] += dot_tn(low_x, grad_g)
        bl_ref[...] += dot_tn(low_x, grad_l)
        low_h = dot_nn(hidden, ld_ref[...]).astype(BF)
        low_d = dot_nt(grad_down, ud_ref[...]).astype(BF)
        ad_ref[...] += dot_tn(low_d, hidden)
        bd_ref[...] += dot_tn(low_h, grad_down)


def ffn(res, gain, gd, gate, lift, down, rg, rl, lgl, ug, ul, ld, ud, block=256):
    count, length, width = res.shape
    depth, hidden = gate.shape
    blocks = length // block
    levels = count.bit_length() - 1
    acc_shapes = [
        (RP, depth), (RP, hidden), (RP, hidden), (RP, hidden), (RP, depth),
        (1, hidden), (1, hidden),
    ]
    return pl.pallas_call(
        ffn_body,
        grid=(blocks + levels,),
        in_specs=[
            chunk_upto(blocks - 1, count, block, width),
            once(gain.shape),
            chunk_upto(blocks - 1, count, block, width),
            *[once(a.shape) for a in (gate, lift, down, rg, rl, lgl, ug, ul, ld, ud)],
        ],
        out_specs=[
            whole((length, width)), whole((length, width)),
            upto(blocks - 1, block, 1), whole((length, 1)),
            *[whole(s) for s in acc_shapes],
        ],
        out_shape=[
            sds((length, width), BF), sds((length, width), BF),
            sds((length, 1), F32), sds((length, 1), F32),
            *[sds(s, F32) for s in acc_shapes],
        ],
        scratch_shapes=[
            pltpu.VMEM((block, depth), BF), pltpu.VMEM((block, depth), BF),
            *row_scratch(count, blocks, block),
            *scatter_scratch(count, blocks, block, width),
            *scatter_scratch(count, blocks, block, width),
        ],
        compiler_params=pltpu.CompilerParams(collective_id=2, has_side_effects=True),
        cost_estimate=estimate(14 * length * depth * hidden, 40 * length * depth),
        name="ffn",
    )(res, gain, gd, gate, lift, down, rg, rl, lgl, ug, ul, ld, ud)


def out_back_body(g_ref, a_ref, w_ref, u_ref, l_ref, da_ref, aa_ref, bb_ref, grad_ref):
    count, _, width = g_ref.shape

    @pl.when(pl.program_id(0) == 0)
    def _():
        aa_ref[...] = jnp.zeros_like(aa_ref)
        bb_ref[...] = jnp.zeros_like(bb_ref)

    for c in range(count):
        grad_ref[:, c * width:(c + 1) * width] = g_ref[c]
    grad, act = grad_ref[...], a_ref[...]
    da_ref[...] = dot_nt(grad, w_ref[...]).astype(BF)
    low_g = dot_nt(grad, u_ref[...]).astype(BF)
    low_a = dot_nn(act, l_ref[...]).astype(BF)
    aa_ref[...] += dot_tn(low_g, act)
    bb_ref[...] += dot_tn(low_a, grad)


def out_back(grad, act, w, u, low, block=256):
    count, length, width = grad.shape
    depth = count * width
    return pl.pallas_call(
        out_back_body,
        grid=(length // block,),
        in_specs=[
            chunk_rows(count, block, width), rows(block, width), whole(w.shape),
            whole(u.shape), whole(low.shape),
        ],
        out_specs=[rows(block, width), whole((RP, width)), whole((RP, depth))],
        out_shape=[sds((length, width), BF), sds((RP, width), F32), sds((RP, depth), F32)],
        scratch_shapes=[pltpu.VMEM((block, depth), BF)],
        cost_estimate=estimate(4 * length * depth * width, 3 * length * depth),
        name="out_back",
    )(grad, act, w, u, low)


def qkv_back_body(g_ref, y_ref, x_ref, xl_ref, w_ref, u_ref, inv_ratio_ref,
                  dx_ref, dot_ref, aa_ref, bb_ref, ss_ref, *scratch):
    width = dx_ref.shape[1]
    count = w_ref.shape[0] // width
    step, me = pl.program_id(0), lax.axis_index("mp")
    row_sums = RowSum(me, scratch[:4], dot_ref)
    sums = Scatter(me, count, scratch[4:], dx_ref)

    @pl.when(step == 0)
    def _():
        meet(me, sums.levels)
        aa_ref[...] = jnp.zeros_like(aa_ref)
        bb_ref[...] = jnp.zeros_like(bb_ref)
        ss_ref[...] = jnp.zeros_like(ss_ref)

    sums.advance(step)
    row_sums.advance(step)

    @pl.when(step < sums.blocks)
    def _():
        grad = g_ref[...]
        for ref, place, at in sums.chunks(width):
            ref[place] = dot_nt(grad, w_ref[at, :]).astype(BF)
        sums.copy(0, step, 0).start()
        product = grad.astype(F32) * y_ref[...].astype(F32) * inv_ratio_ref[...]
        row_sums.begin(step, jnp.sum(product, axis=1, keepdims=True))
        ss_ref[...] += jnp.sum(product * inv_ratio_ref[...], axis=0, keepdims=True)
        low_g = dot_nt(grad, u_ref[...]).astype(BF)
        aa_ref[...] += dot_tn(low_g, x_ref[...])
        bb_ref[...] += dot_tn(xl_ref[...], grad)


def qkv_backward(grad, y, x, xl, w_cat, u_cat, inv_ratio, count, block=256):
    length, depth = x.shape
    wide = grad.shape[1]
    width, blocks = depth // count, length // block
    levels = count.bit_length() - 1
    return pl.pallas_call(
        qkv_back_body,
        grid=(blocks + levels,),
        in_specs=[
            upto(blocks - 1, block, wide), upto(blocks - 1, block, wide),
            upto(blocks - 1, block, depth), upto(blocks - 1, block, RP),
            once(w_cat.shape), once(u_cat.shape), once(inv_ratio.shape),
        ],
        out_specs=[
            whole((length, width)), whole((length, 1)),
            whole((RP, depth)), whole((RP, wide)), whole((1, wide)),
        ],
        out_shape=[
            sds((length, width), BF), sds((length, 1), F32),
            sds((RP, depth), F32), sds((RP, wide), F32), sds((1, wide), F32),
        ],
        scratch_shapes=[
            *row_scratch(count, blocks, block), *scatter_scratch(count, blocks, block, width)
        ],
        compiler_params=pltpu.CompilerParams(collective_id=3, has_side_effects=True),
        cost_estimate=estimate(4 * length * depth * wide, 40 * length * depth),
        name="qkv_backward",
    )(grad, y, x, xl, w_cat, u_cat, inv_ratio)


def far(z, k):
    return {"dp": z + (1 << k) * (1 - 2 * bit_of(z, k))}


def reduce_body(part_ref, *refs, levels, depths, ranks, weights):
    groups, count = len(ranks), len(weights)

    def take(number):
        nonlocal refs
        taken, refs = refs[:number], refs[number:]
        return taken

    own_refs, cross_refs, coef_refs, inv_refs = (take(groups) for _ in range(4))
    base_refs, upper_refs, lower_refs = (take(count) for _ in range(3))
    scale_outs, upper_outs, lower_outs = take(groups), take(count), take(count)
    keep, send, land = (take(levels) for _ in range(3))
    sums, held, come, full, beta_refs = (take(groups) for _ in range(5))
    bases = take(count)
    sent, landed, far_sent, far_landed, full_sent, full_landed, base_sems = refs
    me, z = lax.axis_index("mp"), lax.axis_index("dp")
    loads = [
        pltpu.make_async_copy(base_refs[n], bases[n], base_sems.at[n]) for n in range(count)
    ]
    for load in loads:
        load.start()
    barrier = pltpu.get_barrier_semaphore()
    for target in [other(me, k) for k in range(levels)] + [far(z, k) for k in range(depths)]:
        pl.semaphore_signal(
            barrier, inc=1, device_id=target, device_id_type=pl.DeviceIdType.MESH
        )
    pl.semaphore_wait(barrier, levels + depths)

    def swap(src, dst, sent_at, landed_at, target):
        return pltpu.make_async_remote_copy(
            src_ref=src, dst_ref=dst, send_sem=sent_at, recv_sem=landed_at,
            device_id=target, device_id_type=pl.DeviceIdType.MESH,
        )

    places = part_ref.shape[0] // 2
    for place in range(places):
        keep[0][place] = part_ref[chunk_of(me, 0, place, levels)]
        send[0][place] = part_ref[chunk_of(me, 1, place, levels)].astype(BF)
    rank = part_ref.shape[1]
    for level in range(levels):
        copy = swap(send[level], land[level], sent.at[level], landed.at[level], other(me, level))
        copy.start()
        copy.wait()
        for place in range(places):
            value = keep[level][place] + land[level][place].astype(F32)
            if level == levels - 1:
                held[0][0, :rank] = value.astype(BF)
            elif place >= places // 2:
                send[level + 1][place - places // 2] = value.astype(BF)
            else:
                keep[level + 1][place] = value
        places //= 2
    held[0][0, rank:] = own_refs[0][...].astype(BF)
    for n in range(1, groups):
        held[n][0] = own_refs[n][...].astype(BF)
    for k in range(depths):
        copies = [
            swap(held[n].at[k], come[n].at[k], far_sent.at[k, n], far_landed.at[k, n], far(z, k))
            for n in range(groups)
        ]
        for copy in copies:
            copy.start()
        for n, copy in enumerate(copies):
            copy.wait()
            value = held[n][k].astype(F32) + come[n][k].astype(F32)
            if k == depths - 1:
                sums[n][...] = value
            else:
                held[n][k + 1] = value.astype(BF)
    for n, (number, upper_at, square_at) in enumerate(ranks):
        square = sums[n][square_at:square_at + 8]
        scale_outs[n][...] = square * inv_refs[n][...]
        betas = square * coef_refs[n][...]
        for i in range(number):
            at = upper_at + i * R
            full[n][me, i * R:(i + 1) * R] = (
                2.0 * (
                    sums[n][at:at + R] - cross_refs[n][i * R:(i + 1) * R] * betas[i:i + 1]
                )
            ).astype(BF)
        full[n][me, number * R:] = jnp.concatenate([betas, jnp.zeros_like(betas)], 0).astype(BF)
    known, serial = [()], 0
    for bit in range(levels - 1, -1, -1):
        copies = []
        for flips in known:
            at = 0
            for k in range(levels):
                mine = bit_of(me, k)
                at = at + ((1 - mine) if k in flips else mine) * (1 << k)
            for n in range(groups):
                copies.append(
                    swap(
                        full[n].at[at], full[n].at[at], full_sent.at[serial, n],
                        full_landed.at[serial, n], other(me, bit),
                    )
                )
            serial += 1
        for copy in copies:
            copy.start()
        for copy in copies:
            copy.wait()
        known = known + [flips + (bit,) for flips in known]
    for load in loads:
        load.wait()
    for n, (group, i, (own_group, own_at)) in enumerate(weights):
        number = ranks[group][0]
        chunks, _, size = full[group].shape
        beta_ref = beta_refs[group]
        for c in range(chunks):
            cols = slice(c * size, (c + 1) * size)
            upper_outs[n][:, cols] = full[group][c, i * R:(i + 1) * R].astype(F32)
            row = full[group][c, number * R:].astype(F32)[i:i + 1]
            beta_ref[:, cols] = jnp.broadcast_to(row, (R, size))
        upper = upper_refs[n][...]
        tilted = (upper * beta_ref[...]).astype(BF)
        core = dot_nt(tilted, upper.astype(BF))
        correction = dot_nt(tilted, bases[n][...]) + 2.0 * dot_nn(
            core.astype(BF), lower_refs[n][...].astype(BF)
        )
        lower_outs[n][...] = 2.0 * (sums[own_group][own_at:own_at + R] - correction)


def reduce_sums(part, groups, weights):
    members = lax.axis_size("mp")
    rank, width = part.shape[0], part.shape[1] // members
    part = jnp.transpose(part.reshape(rank, members, width), (1, 0, 2))
    levels = members.bit_length() - 1
    depths = lax.axis_size("dp").bit_length() - 1
    owns, crosses, coefs, invs, ranks = zip(*groups)
    places, bases, uppers, lowers = zip(*weights)
    shapes = [(rank + owns[0].shape[0], width)] + [v.shape for v in owns[1:]]
    fulls = [(members, r[0] * R + 16, v[1]) for r, v in zip(ranks, shapes)]
    vmem, dma = pl.BlockSpec(memory_space=pltpu.VMEM), pltpu.SemaphoreType.DMA

    def halves(dtype):
        return [pltpu.VMEM((members >> (k + 1), rank, width), dtype) for k in range(levels)]

    steps = [pltpu.VMEM((depths,) + tuple(v), BF) for v in shapes]
    number = len(groups)
    return pl.pallas_call(
        functools.partial(
            reduce_body, levels=levels, depths=depths, ranks=ranks, weights=places
        ),
        in_specs=[
            *[vmem] * (1 + 4 * number),
            *[pl.BlockSpec(memory_space=pl.ANY)] * len(bases),
            *[vmem] * (2 * len(bases)),
        ],
        out_specs=[vmem] * (number + 2 * len(bases)),
        out_shape=[
            *[sds((8, v[1]), F32) for v in shapes],
            *[sds(v.shape, F32) for v in uppers],
            *[sds(v.shape, F32) for v in lowers],
        ],
        scratch_shapes=[
            *halves(F32), *halves(BF), *halves(BF),
            *[pltpu.VMEM(v, F32) for v in shapes], *steps, *steps,
            *[pltpu.VMEM(v, BF) for v in fulls],
            *[pltpu.VMEM((R, members * v[1]), F32) for v in shapes],
            *[pltpu.VMEM(v.shape, BF) for v in bases],
            dma((levels,)), dma((levels,)),
            dma((depths, number)), dma((depths, number)),
            dma((members - 1, number)), dma((members - 1, number)),
            dma((len(bases),)),
        ],
        compiler_params=pltpu.CompilerParams(collective_id=4, has_side_effects=True),
        cost_estimate=estimate(0, 60_000_000),
        name="reduce_sums",
    )(part, *owns, *crosses, *coefs, *invs, *bases, *uppers, *lowers)


def split_low(value):
    high = lax.reduce_precision(value, 8, 7)
    return high, value - high


def block_diagonal(blocks):
    width = sum(b.shape[1] for b in blocks)
    at = 0
    result = []
    for b in blocks:
        result.append(jnp.pad(b, ((0, 0), (at, width - at - b.shape[1]))))
        at += b.shape[1]
    return jnp.concatenate(result, axis=0)


def pad_rows(value, at=0):
    return jnp.pad(value, ((at, RP - at - value.shape[0]), (0, 0))).astype(BF)


def flip(value, bit, axis="mp"):
    size = lax.axis_size(axis)
    return lax.ppermute(value, axis, [(i, i ^ (1 << bit)) for i in range(size)])


def gather_small(value, me):
    part = value[None]
    for bit in range(lax.axis_size("mp").bit_length() - 1):
        came = flip(part, bit)
        upper = ((me >> bit) & 1) == 1
        part = jnp.concatenate(
            [jnp.where(upper, came, part), jnp.where(upper, part, came)], axis=0
        )
    return part


def scatter_cols(value, me):
    members = lax.axis_size("mp")
    part = jnp.transpose(value.reshape(value.shape[0], members, -1), (1, 0, 2))
    for bit in range(members.bit_length() - 1):
        mine = (me >> bit) & 1
        pair = part.reshape(part.shape[0] // 2, 2, *part.shape[1:])
        keep = lax.dynamic_index_in_dim(pair, mine, 1, keepdims=False)
        away = lax.dynamic_index_in_dim(pair, 1 - mine, 1, keepdims=False)
        part = keep + flip(away, bit)
    return part[0]


def tie(value, *others):
    return lax.optimization_barrier((value, *others))[0]


def tables(lengths, length):
    ends = jnp.cumsum(lengths)
    at = jnp.arange(length, dtype=jnp.int32)
    after = (at[:, None] >= ends[None, :NDOC]).astype(jnp.int32)
    segment = jnp.sum(after, axis=1)
    start = jnp.sum(after * lengths[None, :NDOC], axis=1)
    half = jnp.arange(HD // 2, dtype=F32)
    frequency = ROPE_BASE ** (-(2.0 * half / HD))
    angles = (at - start).astype(F32)[:, None] * frequency[None, :]
    cos, sin = jnp.cos(angles), jnp.sin(angles)
    return (
        start,
        (segment < NDOC).astype(F32)[:, None],
        jnp.concatenate([cos, cos], axis=1),
        jnp.concatenate([sin, -sin], axis=1),
    )


def on_device(
    tokens, doc_lengths, out_grad, attn_gain, ffn_gain,
    query_base, query_lower, query_upper, query_scale,
    key_base, key_lower, key_upper, key_scale,
    value_base, value_lower, value_upper, value_scale,
    output_base, output_lower, output_upper, output_scale,
    gate_base, gate_lower, gate_upper, gate_scale,
    lift_base, lift_lower, lift_upper, lift_scale,
    down_base, down_lower, down_upper, down_scale,
):
    members = lax.axis_size("mp")
    me = lax.axis_index("mp")
    seqs, length, width = tokens.shape
    depth = members * width
    hidden = down_base.shape[0]
    block = min(256, length)

    def gather(value):
        return lax.all_gather(value, "mp", axis=0)

    def own_cols(value, size):
        return lax.dynamic_slice_in_dim(value, me * size, size, 1)

    def exchange(value):
        return lax.all_to_all(value, "mp", split_axis=0, concat_axis=0, tiled=True)

    qkv_arranged = arrange([query_base, key_base, value_base], members)
    qkv_base = exchange(qkv_arranged)
    pack = jnp.concatenate(
        [
            tie(query_lower, qkv_arranged).T, key_lower.T, value_lower.T,
            gate_lower.T, lift_lower.T,
            jnp.stack([attn_gain, ffn_gain]),
        ],
        axis=0,
    )
    pack = jnp.pad(pack, ((0, 88 - pack.shape[0]), (0, 0)))
    packed = jnp.transpose(gather_small(pack, me), (1, 0, 2)).reshape(pack.shape[0], depth)
    tok_all = [gather(tokens[s]) for s in range(seqs)]
    lower_qkv_t, lower_gl_t = packed[:3 * R], packed[3 * R:5 * R]
    gain_a, gain_f = packed[5 * R], packed[5 * R + 1]

    output_w, square_o, cross_o = merge(
        tie(output_base, qkv_arranged)[None], output_lower.T, output_upper)
    down_w, square_d, cross_d = merge(
        tie(down_base, qkv_arranged)[None], down_lower.T, down_upper)
    row_stats = scatter_cols(
        jnp.concatenate([square_o, square_d, cross_o, cross_d], axis=0), me
    )
    output_w, down_w = output_w[0], down_w[0]
    norm_o, norm_d = jnp.sqrt(row_stats[0]), jnp.sqrt(row_stats[1])
    cross_o, cross_d = row_stats[2:2 + R], row_stats[2 + R:2 + 2 * R]
    ratio_o, ratio_d = output_scale / norm_o, down_scale / norm_d
    layouts = [tables(doc_lengths[s], length) for s in range(seqs)]
    grad_tops = [out_grad[s].astype(F32) * layouts[s][1] for s in range(seqs)]
    gd_low = [(grad_tops[s] * ratio_d).astype(BF) for s in range(seqs)]
    gd_all = [gather(gd_low[s]) for s in range(seqs)]

    upper_qkv = block_diagonal([own_cols(u, width) for u in (query_upper, key_upper, value_upper)])
    upper_g, upper_l = own_cols(gate_upper, hidden), own_cols(lift_upper, hidden)
    qkv_w, square_qkv, cross_all = merge(qkv_base, lower_qkv_t, upper_qkv)
    qkv_w = qkv_w.reshape(depth, 3 * width)
    norm_qkv = jnp.sqrt(square_qkv[0])
    scale_qkv = jnp.concatenate([query_scale, key_scale, value_scale])
    ratio_qkv = (scale_qkv / norm_qkv)[None]
    inv_ratio = 1.0 / ratio_qkv

    gl_arranged = arrange([gate_base, lift_base], members)
    gl_base = exchange(tie(gl_arranged, tok_all[0]))
    gate_w, lift_w, square_gl, cross_g, cross_l = merge(
        gl_base, lower_gl_t, block_diagonal([upper_g, upper_l]), [hidden, hidden]
    )
    gate_w, lift_w = gate_w.reshape(depth, hidden), lift_w.reshape(depth, hidden)
    norm_gl = jnp.sqrt(square_gl[0])
    norm_g, norm_l = norm_gl[:hidden], norm_gl[hidden:]
    ratio_g, ratio_l = (gate_scale / norm_g)[None], (lift_scale / norm_l)[None]

    low_l_qkv, low_l_gl = pad_rows(lower_qkv_t), pad_rows(lower_gl_t)
    low_u_qkv, low_u_g, low_u_l = pad_rows(upper_qkv), pad_rows(upper_g), pad_rows(upper_l, R)
    low_l_d, low_u_d = pad_rows(down_lower.T).T, pad_rows(down_upper)
    low_l_o, low_u_o = pad_rows(output_lower.T).T, pad_rows(output_upper)
    chunk_gain_a, chunk_gain_f = (v.reshape(members, 1, width) for v in (gain_a, gain_f))

    state = [dict() for _ in range(seqs)]

    def attention_stage(s):
        st = state[s]
        start, _, st["cos"], st["sin"] = layouts[s]
        st["start"] = start.reshape(length // block, block)
        st["lo"] = st["start"][:, 0] // block
        if s == 0:
            tok = tie(tok_all[s], gl_arranged, *gd_low)
        else:
            tok = tie(tok_all[s], state[s - 1]["residual_low"])
        st["x"], st["y"], st["q"], st["k"], st["xl"], st["inv"] = qkv_forward(
            tok, chunk_gain_a, qkv_w, low_l_qkv, ratio_qkv, st["cos"], st["sin"]
        )
        st["att"], st["lse"] = attend_forward(
            st["lo"], st["start"], st["q"], st["k"], st["y"], block
        )
        act = tie(st["att"], gate_w, lift_w) if s == seqs - 1 else st["att"]
        st["inner_o"] = out_forward(act, output_w).astype(F32)
        st["residual"] = tokens[s].astype(F32) + st["inner_o"] * ratio_o
        st["residual_low"] = st["residual"].astype(BF)
        st["residual_all"] = gather(st["residual_low"])

    def ffn_stage(s):
        st = state[s]
        if s + 1 < seqs:
            res = tie(st["residual_all"], state[s + 1]["residual_low"])
        else:
            res = tie(st["residual_all"], state[s - 1]["grad_output_low"])
        st["inner_d"], back, st["inv_f"], dot_f, *st["ffn"] = ffn(
            res, chunk_gain_f, gd_all[s], gate_w, lift_w, down_w,
            ratio_g, ratio_l, low_l_gl, low_u_g, low_u_l, low_l_d, low_u_d,
        )
        inv = st["inv_f"]
        grad_residual = (
            grad_tops[s] + inv * (ffn_gain * back.astype(F32))
            - st["residual"] * (inv * inv * dot_f / depth)
        )
        st["grad_residual"] = grad_residual
        st["grad_output_low"] = (grad_residual * ratio_o).astype(BF)
        st["grad_output"] = gather(st["grad_output_low"])
        inner_d = st["inner_d"].astype(F32)
        st["out"] = (st["residual"] + inner_d * ratio_d).astype(BF)
        st["g_d"] = jnp.sum(inner_d * grad_tops[s], axis=0)
        st["g_o"] = jnp.sum(st["inner_o"] * grad_residual, axis=0)

    def attention_back_stage(s):
        st = state[s]
        grad = st["grad_output"]
        if s + 1 < seqs:
            grad = tie(grad, state[s + 1]["grad_output_low"])
        else:
            grad = tie(grad, state[s - 1]["dx"])
        grad_att, st["a_o"], st["b_o"] = out_back(
            grad, st["att"], output_w, low_u_o, low_l_o
        )
        grads = attend_backward(
            st["lo"], st["start"], st["q"], st["k"], st["y"], grad_att, st["att"],
            st["lse"], st["cos"], st["sin"], ratio_qkv, block,
        )
        st["dx"], dot_a, st["a_qkv"], st["b_qkv"], st["g_qkv"] = qkv_backward(
            grads, st["y"], st["x"], st["xl"], qkv_w, low_u_qkv, inv_ratio, members
        )
        inv = st["inv"]
        st["in_grad"] = (
            st["grad_residual"] + inv * (attn_gain * st["dx"].astype(F32))
            - tokens[s].astype(F32) * (inv * inv * dot_a / depth)
        )

    for stage in (attention_stage, ffn_stage, attention_back_stage):
        for s in range(seqs):
            stage(s)

    out_tokens = jnp.stack([st["out"] for st in state])
    in_grad = jnp.stack([st["in_grad"] for st in state])

    def total(pick):
        result = pick(state[0])
        for s in range(1, seqs):
            result = result + pick(state[s])
        return result

    def blocks_of(value, size):
        return jnp.concatenate(
            [value[n * R:(n + 1) * R, n * size:(n + 1) * size] for n in range(value.shape[0] // R)],
            axis=0,
        )

    def stacked(values, height):
        value = jnp.concatenate(values, axis=0)
        return jnp.pad(value, ((0, height - value.shape[0]), (0, 0)))

    coef_qkv = (scale_qkv / norm_qkv ** 3).reshape(3, width)
    coef_o, coef_d = output_scale / norm_o ** 3, down_scale / norm_d ** 3
    coef_g, coef_l = gate_scale / norm_g ** 3, lift_scale / norm_l ** 3
    norm_rows = norm_qkv.reshape(3, width)
    groups = [
        (
            stacked(
                [
                    blocks_of(total(lambda st: st["b_qkv"])[:3 * R], width),
                    total(lambda st: st["a_o"])[:R],
                    total(lambda st: st["g_o"])[None],
                    total(lambda st: st["g_d"])[None],
                    total(lambda st: st["g_qkv"]).reshape(3, width),
                ],
                4 * R + 8,
            ),
            jnp.concatenate([cross_o, cross_d, blocks_of(cross_all, width)], axis=0),
            stacked([coef_o[None], coef_d[None], coef_qkv], 8),
            stacked([1.0 / norm_o[None], 1.0 / norm_d[None], 1.0 / norm_rows], 8),
            (5, 5 * R, 11 * R),
        ),
        (
            stacked(
                [
                    total(lambda st: st["ffn"][1])[:R],
                    total(lambda st: st["ffn"][2])[R:2 * R],
                    total(lambda st: st["ffn"][3])[:R],
                    total(lambda st: st["ffn"][5]),
                    total(lambda st: st["ffn"][6]),
                ],
                3 * R + 8,
            ),
            jnp.concatenate([cross_g[:R], cross_l[R:2 * R]], axis=0),
            stacked([coef_g[None], coef_l[None]], 8),
            stacked([1.0 / norm_g[None], 1.0 / norm_l[None]], 8),
            (2, 0, 3 * R),
        ),
    ]
    weights = [
        ((0, 2, (0, 0)), query_base, query_upper, query_lower.T),
        ((0, 3, (0, R)), key_base, key_upper, key_lower.T),
        ((0, 4, (0, 2 * R)), value_base, value_upper, value_lower.T),
        ((0, 0, (0, 10 * R)), output_base, output_upper, output_lower.T),
        ((1, 0, (0, 3 * R)), gate_base, gate_upper, gate_lower.T),
        ((1, 1, (0, 4 * R)), lift_base, lift_upper, lift_lower.T),
        ((0, 1, (1, 2 * R)), down_base, down_upper, down_lower.T),
    ]
    part = jnp.concatenate(
        [
            total(lambda st: st["a_qkv"])[:3 * R],
            total(lambda st: st["ffn"][0])[:2 * R],
            total(lambda st: st["b_o"])[:R],
            total(lambda st: st["ffn"][4])[:R],
        ],
        axis=0,
    )
    finished = reduce_sums(part, groups, weights)
    results = [out_tokens, in_grad]
    for n, ((group, i, _), _, _, _) in enumerate(weights):
        results += [finished[2 + len(weights) + n].T, finished[2 + n], finished[group][i]]
    return tuple(results)


def solution(mesh):
    spread, split, rows_spec = P("dp", None, "mp"), P("mp"), P("mp", None)
    weight = (rows_spec, rows_spec, P(), split)
    grads = (rows_spec, P(), split)

    return jax.shard_map(
        on_device,
        mesh=mesh,
        in_specs=(spread, P("dp", None), spread, split, split) + weight * 7,
        out_specs=(spread, spread) + grads * 7,
        check_vma=False,
    )
```

```python
import functools

import jax
import jax.numpy as jnp
from jax import lax
from jax.experimental import pallas as pl
from jax.experimental.pallas import tpu as pltpu
from jax.sharding import PartitionSpec as P


HD = 128
R = 16
RP = 128
NDOC = 5
EPSILON = 1e-05
ROPE_BASE = 10000.0
NEGATIVE = -1e30
LOG2E = 1.4426950408889634
BF = jnp.bfloat16
F32 = jnp.float32


def dot_nn(a, b):
    return lax.dot_general(a, b, (((1,), (0,)), ((), ())), preferred_element_type=F32)


def dot_nt(a, b):
    return lax.dot_general(a, b, (((1,), (1,)), ((), ())), preferred_element_type=F32)


def dot_tn(a, b):
    return lax.dot_general(a, b, (((0,), (0,)), ((), ())), preferred_element_type=F32)


def whole(shape):
    rank = len(shape)
    return pl.BlockSpec(tuple(shape), lambda i: (0,) * rank)


def rows(block, width):
    return pl.BlockSpec((block, width), lambda i: (i, 0))


def chunk_rows(count, block, width):
    return pl.BlockSpec((count, block, width), lambda i: (0, i, 0))


def sds(shape, dtype):
    return jax.ShapeDtypeStruct(tuple(shape), dtype)


def estimate(flops, bytes_accessed):
    return pl.CostEstimate(flops=int(flops), bytes_accessed=int(bytes_accessed), transcendentals=0)


def smem():
    return pl.BlockSpec(memory_space=pltpu.SMEM)


def bit_of(me, k):
    return (me // (1 << k)) % 2


def chunk_of(me, half, place, levels):
    result = 0
    for k in range(levels):
        bit = bit_of(me, k)
        flip = half if k == 0 else (place >> (levels - 1 - k)) & 1
        result = result + ((1 - bit) if flip else bit) * (1 << k)
    return result


def other(me, k):
    return {"mp": me + (1 << k) * (1 - 2 * bit_of(me, k))}


def meet(me, levels):
    barrier = pltpu.get_barrier_semaphore()
    for k in range(levels):
        pl.semaphore_signal(
            barrier, inc=1, device_id=other(me, k), device_id_type=pl.DeviceIdType.MESH
        )
    pl.semaphore_wait(barrier, levels)


def scatter_scratch(count, blocks, block, width):
    levels = count.bit_length() - 1
    shapes = []
    for level in range(levels):
        size = (count >> 1, block, width) if level == 0 else (2, count >> (level + 1), block // 2, width)
        shapes += [
            pltpu.VMEM(size, BF),
            pltpu.VMEM(size, BF),
            pltpu.VMEM((blocks,) + size, BF),
            pltpu.SemaphoreType.DMA((blocks,) if level == 0 else (blocks, 2)),
            pltpu.SemaphoreType.DMA((blocks,) if level == 0 else (blocks, 2)),
        ]
    return shapes


class Scatter:
    def __init__(self, me, count, refs, out_ref):
        self.me, self.levels, self.out_ref = me, count.bit_length() - 1, out_ref
        self.count = count
        self.keep, self.send, self.land, self.sent, self.landed = (
            [refs[5 * level + n] for level in range(self.levels)] for n in range(5)
        )
        self.blocks = self.land[0].shape[0]
        self.block = self.land[0].shape[2]

    def copy(self, level, b, path):
        if level == 0:
            bit, src, at = 0, self.send[0], (b,)
        else:
            bit = level if path == 0 else self.levels - level
            src, at = self.send[level].at[path], (b, path)
        return pltpu.make_async_remote_copy(
            src_ref=src,
            dst_ref=self.land[level].at[at],
            send_sem=self.sent[level].at[at],
            recv_sem=self.landed[level].at[at],
            device_id=other(self.me, bit),
            device_id_type=pl.DeviceIdType.MESH,
        )

    def pass_on(self, level, path, places, place, value):
        upper = place >= places // 2 if path == 0 else place % 2 == 1
        at = place % (places // 2) if path == 0 else place // 2
        ref = self.send[level + 1] if upper else self.keep[level + 1]
        ref[path, at] = value.astype(BF)

    def finish(self, level, b):
        half = self.block // 2
        if level == 0:
            self.copy(0, b, 0).wait()
            places = self.count // 2
            for place in range(places):
                value = self.keep[0][place].astype(F32) + self.land[0][b, place].astype(F32)
                self.pass_on(0, 0, places, place, value[:half])
                self.pass_on(0, 1, places, place, value[half:])
        else:
            for path in range(2):
                self.copy(level, b, path).wait()
                places = self.count >> (level + 1)
                for place in range(places):
                    value = (
                        self.keep[level][path, place].astype(F32)
                        + self.land[level][b, path, place].astype(F32)
                    )
                    if level < self.levels - 1:
                        self.pass_on(level, path, places, place, value)
                    else:
                        at = pl.multiple_of(b * self.block + path * half, half)
                        self.out_ref[pl.ds(at, half), :] = value.astype(self.out_ref.dtype)
        if level < self.levels - 1:
            for path in range(2):
                self.copy(level + 1, b, path).start()

    def advance(self, step):
        for level in range(self.levels - 1, -1, -1):
            b = step - level - 1

            @pl.when((b >= 0) & (b < self.blocks))
            def _():
                self.finish(level, b)

    def chunks(self, width):
        for half in range(2):
            for place in range(self.count // 2):
                at = chunk_of(self.me, half, place, self.levels) * width
                ref = self.send[0] if half else self.keep[0]
                yield ref, place, pl.ds(pl.multiple_of(at, width), width)


def row_scratch(count, blocks, block):
    levels = count.bit_length() - 1
    return [
        pltpu.VMEM((levels, 8, block), F32),
        pltpu.VMEM((blocks, levels, 8, block), F32),
        pltpu.SemaphoreType.DMA((blocks, levels)),
        pltpu.SemaphoreType.DMA((blocks, levels)),
    ]


class RowSum:
    def __init__(self, me, refs, out_ref):
        self.me, self.out_ref = me, out_ref
        self.held, self.land, self.sent, self.landed = refs
        self.levels, _, self.block = self.held.shape
        self.blocks = self.land.shape[0]

    def copy(self, level, b):
        return pltpu.make_async_remote_copy(
            src_ref=self.held.at[level],
            dst_ref=self.land.at[b, level],
            send_sem=self.sent.at[b, level],
            recv_sem=self.landed.at[b, level],
            device_id=other(self.me, level),
            device_id_type=pl.DeviceIdType.MESH,
        )

    def begin(self, b, value):
        self.held[0] = jnp.broadcast_to(value, (self.block, 128)).T[:8]
        self.copy(0, b).start()

    def advance(self, step):
        for level in range(self.levels - 1, -1, -1):
            b = step - level - 1

            @pl.when((b >= 0) & (b < self.blocks))
            def _():
                self.copy(level, b).wait()
                value = self.held[level] + self.land[b, level]
                if level < self.levels - 1:
                    self.held[level + 1] = value
                    self.copy(level + 1, b).start()
                else:
                    at = pl.multiple_of(b * self.block, self.block)
                    column = jnp.broadcast_to(value[:1], (128, self.block)).T
                    self.out_ref[pl.ds(at, self.block), :] = column[:, :1]


def once(shape):
    rank = len(shape)
    return pl.BlockSpec(tuple(shape), lambda i: (0,) * rank, pipeline_mode=pl.Buffered(1))


def upto(last, block, width):
    return pl.BlockSpec((block, width), lambda i: (jnp.minimum(i, last), 0))


def chunk_upto(last, count, block, width):
    return pl.BlockSpec((count, block, width), lambda i: (0, jnp.minimum(i, last), 0))


def arrange_body(*refs):
    out_ref = refs[-1]
    count = out_ref.shape[0]
    at = 0
    for ref in refs[:-1]:
        size = ref.shape[1] // count
        for c in range(count):
            out_ref[c, :, at:at + size] = ref[:, c * size:(c + 1) * size]
        at += size


def arrange(values, count):
    height = values[0].shape[0]
    size = sum(v.shape[1] for v in values) // count
    block = max(16, height // 2)
    return pl.pallas_call(
        arrange_body,
        grid=(height // block,),
        in_specs=[rows(block, v.shape[1]) for v in values],
        out_specs=chunk_rows(count, block, size),
        out_shape=sds((count, height, size), BF),
        cost_estimate=estimate(0, 4 * count * height * size),
        name="arrange",
    )(*values)


def merge_body(place_ref, *refs, pieces):
    base_refs, (l3_ref, u3_ref, l_ref), refs = refs[:pieces], refs[pieces:pieces + 3], refs[pieces + 3:]
    splits = (len(refs) - 1) // 2
    w_refs, square_ref, cross_refs = refs[:splits], refs[splits], refs[splits + 1:]

    @pl.when(pl.program_id(0) == 0)
    def _():
        for ref in (square_ref, *cross_refs):
            ref[...] = jnp.zeros_like(ref)

    parts, place = (pieces + 1) // 2, place_ref[0]
    base = []
    for part in range(parts):
        piece = base_refs[parts - 1 + part][0]
        for at in range(1, parts):
            piece = jnp.where(place == at, base_refs[parts - 1 + part - at][0], piece)
        base.append(piece)
    value = jnp.concatenate(base, axis=0).astype(F32) + dot_tn(l3_ref[...], u3_ref[...])
    low = value.astype(BF)
    at = 0
    for ref, cross_ref in zip(w_refs, cross_refs):
        ref[0] = low[:, at:at + ref.shape[2]]
        at += ref.shape[2]
        cross_ref[...] += dot_nn(l_ref[...], ref[0])
    square_ref[...] += jnp.sum(value * value, axis=0, keepdims=True)


def merge(pieces, lower_t, upper, splits=None):
    count, share, width = pieces[0].shape
    height = share * ((len(pieces) + 1) // 2)
    splits = splits or [width]
    rank = lower_t.shape[0]
    lower_high, lower_low = split_low(lower_t)
    upper_high, upper_low = split_low(2.0 * upper)
    l3 = jnp.concatenate([lower_high, lower_low, lower_high], axis=0).astype(BF)
    u3 = jnp.concatenate([upper_high, upper_high, upper_low], axis=0).astype(BF)
    place = jnp.full((1,), lax.axis_index("dp"), jnp.int32)
    return pl.pallas_call(
        functools.partial(merge_body, pieces=len(pieces)),
        grid=(count,),
        in_specs=[
            smem(),
            *[pl.BlockSpec((1, share, width), lambda i: (i, 0, 0))] * len(pieces),
            pl.BlockSpec((3 * rank, height), lambda i: (0, i)),
            whole(u3.shape),
            pl.BlockSpec((rank, height), lambda i: (0, i)),
        ],
        out_specs=[
            *[pl.BlockSpec((1, height, n), lambda i: (i, 0, 0)) for n in splits],
            whole((1, width)),
            *[whole((rank, n)) for n in splits],
        ],
        out_shape=[
            *[sds((count, height, n), BF) for n in splits],
            sds((1, width), F32),
            *[sds((rank, n), F32) for n in splits],
        ],
        cost_estimate=estimate(
            8 * count * height * width * rank, 4 * count * height * width
        ),
        name="merge",
    )(place, *pieces, l3, u3, lower_t.astype(BF))


def qkv_body(tok_ref, gain_ref, w_ref, l_ref, ratio_ref, cos_ref, sin_ref,
             x_ref, y_ref, q_ref, k_ref, xl_ref, inv_ref):
    count, block, width = tok_ref.shape
    total = jnp.zeros((block, 1), F32)
    for c in range(count):
        part = tok_ref[c].astype(F32)
        total = total + jnp.sum(part * part, axis=1, keepdims=True)
    inv = lax.rsqrt(total / (count * width) + EPSILON)
    inv_ref[...] = inv
    for c in range(count):
        x_ref[:, c * width:(c + 1) * width] = (
            tok_ref[c].astype(F32) * inv * gain_ref[c]
        ).astype(BF)
    y = dot_nn(x_ref[...], w_ref[...]) * ratio_ref[...]
    xl_ref[...] = dot_nt(x_ref[...], l_ref[...]).astype(BF)
    y_ref[...] = y.astype(BF)
    cos, sin = cos_ref[...], sin_ref[...]
    for number, out_ref in ((0, q_ref), (1, k_ref)):
        for h in range(width // HD):
            v = y[:, number * width + h * HD:number * width + (h + 1) * HD]
            out_ref[:, h * HD:(h + 1) * HD] = (
                v * cos - pltpu.roll(v, HD // 2, 1) * sin
            ).astype(BF)


def qkv_forward(tok, gain, w_cat, l_cat, ratio, cos, sin, block=256):
    count, length, width = tok.shape
    depth = count * width
    return pl.pallas_call(
        qkv_body,
        grid=(length // block,),
        in_specs=[
            chunk_rows(count, block, width),
            whole(gain.shape),
            whole(w_cat.shape),
            whole(l_cat.shape),
            whole(ratio.shape),
            rows(block, HD),
            rows(block, HD),
        ],
        out_specs=[
            rows(block, depth),
            rows(block, 3 * width),
            rows(block, width),
            rows(block, width),
            rows(block, RP),
            rows(block, 1),
        ],
        out_shape=[
            sds((length, depth), BF),
            sds((length, 3 * width), BF),
            sds((length, width), BF),
            sds((length, width), BF),
            sds((length, RP), BF),
            sds((length, 1), F32),
        ],
        cost_estimate=estimate(2 * length * depth * (3 * width + RP), 6 * length * depth),
        name="qkv_forward",
    )(tok, gain, w_cat, l_cat, ratio, cos, sin)


def attend_body(lo_ref, start_ref, q_ref, k_ref, v_ref, o_ref, lse_ref, vt_ref, *, block):
    length, width = q_ref.shape
    heads = width // HD
    factor = HD ** (-0.5) * LOG2E
    for h in range(heads):
        vt_ref[h * HD:(h + 1) * HD, :] = v_ref[:, h * HD:(h + 1) * HD].T
    key_iota = lax.broadcasted_iota(jnp.int32, (block, block), 0)
    query_iota = lax.broadcasted_iota(jnp.int32, (1, block), 1)

    def query_step(i, carry):
        base = pl.multiple_of(i * block, block)
        start = start_ref[pl.ds(i, 1), :]
        place = query_iota + base
        queries = [q_ref[pl.ds(base, block), h * HD:(h + 1) * HD] for h in range(heads)]

        def key_step(j, state):
            at = pl.multiple_of(j * block, block)
            key_place = key_iota + at
            allowed = (key_place >= start) & (key_place <= place)
            result = []
            for h in range(heads):
                top, total, acc = state[h]
                keys = k_ref[pl.ds(at, block), h * HD:(h + 1) * HD]
                s = jnp.where(allowed, dot_nt(keys, queries[h]) * factor, NEGATIVE)
                new_top = jnp.maximum(top, jnp.max(s, axis=0, keepdims=True))
                scale = jnp.exp2(top - new_top)
                p = jnp.exp2(s - new_top)
                total = total * scale + jnp.sum(p, axis=0, keepdims=True)
                acc = acc * scale + dot_nn(
                    vt_ref[h * HD:(h + 1) * HD, pl.ds(at, block)], p.astype(BF)
                )
                result.append((new_top, total, acc))
            return tuple(result)

        first = tuple(
            (
                jnp.full((1, block), NEGATIVE, F32),
                jnp.zeros((1, block), F32),
                jnp.zeros((HD, block), F32),
            )
            for _ in range(heads)
        )
        state = lax.fori_loop(lo_ref[i], i + 1, key_step, first)
        for h in range(heads):
            top, total, acc = state[h]
            o_ref[pl.ds(base, block), h * HD:(h + 1) * HD] = (acc / total).T.astype(BF)
            lse_ref[h, pl.ds(i, 1), :] = top + jnp.log2(total)
        return carry

    lax.fori_loop(0, length // block, query_step, 0)


def attend_forward(lo, start, q, k, y, block):
    length, width = q.shape
    count = length // block
    return pl.pallas_call(
        functools.partial(attend_body, block=block),
        grid=(1,),
        in_specs=[
            pl.BlockSpec(memory_space=pltpu.SMEM),
            whole(start.shape),
            whole(q.shape),
            whole(k.shape),
            pl.BlockSpec((length, width), lambda i: (0, 2)),
        ],
        out_specs=[whole(q.shape), whole((width // HD, count, block))],
        out_shape=[sds(q.shape, BF), sds((width // HD, count, block), F32)],
        scratch_shapes=[pltpu.VMEM((width, length), BF)],
        cost_estimate=estimate(2 * length * length * width, 8 * length * width),
        name="attend_forward",
    )(lo, start, q, k, y)


def attend_back_body(lo_ref, start_ref, q_ref, k_ref, v_ref, do_ref, o_ref, lse_ref, cos_ref,
                     sin_ref, ratio_ref, g_ref, kt_ref, dk_ref, dv_ref, *, block):
    length, width = q_ref.shape
    heads = width // HD
    scale = HD ** (-0.5)
    factor = scale * LOG2E
    dk_ref[...] = jnp.zeros_like(dk_ref)
    dv_ref[...] = jnp.zeros_like(dv_ref)
    for h in range(heads):
        kt_ref[h * HD:(h + 1) * HD, :] = k_ref[:, h * HD:(h + 1) * HD].T
    key_iota = lax.broadcasted_iota(jnp.int32, (block, block), 0)
    query_iota = lax.broadcasted_iota(jnp.int32, (1, block), 1)

    def turn_back(grad, base):
        return (
            grad * cos_ref[pl.ds(base, block), :]
            + pltpu.roll(grad, HD // 2, 1) * sin_ref[pl.ds(base, block), :]
        )

    def query_step(i, carry):
        base = pl.multiple_of(i * block, block)
        start = start_ref[pl.ds(i, 1), :]
        place = query_iota + base
        queries, grads, deltas, lses = [], [], [], []
        for h in range(heads):
            cols = slice(h * HD, (h + 1) * HD)
            queries.append(q_ref[pl.ds(base, block), cols])
            grad = do_ref[pl.ds(base, block), cols]
            grads.append(grad)
            product = grad.astype(F32) * o_ref[pl.ds(base, block), cols].astype(F32)
            deltas.append(jnp.sum(product.T, axis=0, keepdims=True))
            lses.append(lse_ref[h, pl.ds(i, 1), :])

        def key_step(j, state):
            at = pl.multiple_of(j * block, block)
            key_place = key_iota + at
            allowed = (key_place >= start) & (key_place <= place)
            result = []
            for h in range(heads):
                cols = slice(h * HD, (h + 1) * HD)
                keys = k_ref[pl.ds(at, block), cols]
                s = dot_nt(keys, queries[h]) * factor
                p = jnp.where(allowed, jnp.exp2(s - lses[h]), 0.0)
                dp = dot_nt(v_ref[pl.ds(at, block), cols], grads[h])
                ds = (p * (dp - deltas[h])).astype(BF)
                dv_ref[pl.ds(at, block), cols] += dot_nn(p.astype(BF), grads[h])
                dk_ref[pl.ds(at, block), cols] += dot_nn(ds, queries[h])
                result.append(state[h] + dot_nn(kt_ref[cols, pl.ds(at, block)], ds))
            return tuple(result)

        first = tuple(jnp.zeros((HD, block), F32) for _ in range(heads))
        state = lax.fori_loop(lo_ref[i], i + 1, key_step, first)
        for h in range(heads):
            cols = slice(h * HD, (h + 1) * HD)
            g_ref[pl.ds(base, block), cols] = (
                turn_back(state[h].T * scale, base) * ratio_ref[:, cols]
            ).astype(BF)
        return carry

    lax.fori_loop(0, length // block, query_step, 0)

    def finish(j, carry):
        base = pl.multiple_of(j * block, block)
        for h in range(heads):
            cols = slice(h * HD, (h + 1) * HD)
            key_cols = slice(width + h * HD, width + (h + 1) * HD)
            value_cols = slice(2 * width + h * HD, 2 * width + (h + 1) * HD)
            g_ref[pl.ds(base, block), key_cols] = (
                turn_back(dk_ref[pl.ds(base, block), cols] * scale, base)
                * ratio_ref[:, key_cols]
            ).astype(BF)
            g_ref[pl.ds(base, block), value_cols] = (
                dv_ref[pl.ds(base, block), cols] * ratio_ref[:, value_cols]
            ).astype(BF)
        return carry

    lax.fori_loop(0, length // block, finish, 0)


def attend_backward(lo, start, q, k, y, grad, attended, lse, cos, sin, ratio, block):
    length, width = q.shape
    return pl.pallas_call(
        functools.partial(attend_back_body, block=block),
        grid=(1,),
        in_specs=[
            pl.BlockSpec(memory_space=pltpu.SMEM),
            whole(start.shape),
            whole(q.shape),
            whole(k.shape),
            pl.BlockSpec((length, width), lambda i: (0, 2)),
            whole(grad.shape),
            whole(attended.shape),
            whole(lse.shape),
            whole(cos.shape),
            whole(sin.shape),
            whole(ratio.shape),
        ],
        out_specs=whole((length, 3 * width)),
        out_shape=sds((length, 3 * width), BF),
        scratch_shapes=[
            pltpu.VMEM((width, length), BF),
            pltpu.VMEM((length, width), F32),
            pltpu.VMEM((length, width), F32),
        ],
        cost_estimate=estimate(5 * length * length * width, 16 * length * width),
        name="attend_backward",
    )(lo, start, q, k, y, grad, attended, lse, cos, sin, ratio)


def out_body(a_ref, w_ref, out_ref, *scratch):
    width = out_ref.shape[1]
    count = w_ref.shape[1] // width
    step, me = pl.program_id(0), lax.axis_index("mp")
    sums = Scatter(me, count, scratch, out_ref)

    @pl.when(step == 0)
    def _():
        meet(me, sums.levels)

    sums.advance(step)

    @pl.when(step < sums.blocks)
    def _():
        act = a_ref[...]
        for ref, place, cols in sums.chunks(width):
            ref[place] = dot_nn(act, w_ref[:, cols]).astype(BF)
        sums.copy(0, step, 0).start()


def out_forward(act, w, block=256):
    length, width = act.shape
    depth = w.shape[1]
    count, blocks = depth // width, length // block
    levels = count.bit_length() - 1
    return pl.pallas_call(
        out_body,
        grid=(blocks + levels,),
        in_specs=[upto(blocks - 1, block, width), once(w.shape)],
        out_specs=whole((length, width)),
        out_shape=sds((length, width), BF),
        scratch_shapes=scatter_scratch(count, blocks, block, width),
        compiler_params=pltpu.CompilerParams(collective_id=1, has_side_effects=True),
        cost_estimate=estimate(2 * length * depth * width, 40 * length * depth),
        name="out_forward",
    )(act, w)


def ffn_body(res_ref, gain_ref, gd_in_ref, gate_ref, lift_ref, down_ref,
             rg_ref, rl_ref, lgl_ref, ug_ref, ul_ref, ld_ref, ud_ref,
             down_out, back_out, inv_ref, dot_ref,
             agl_ref, bg_ref, bl_ref, ad_ref, bd_ref, sg_ref, sl_ref,
             x_ref, gd_ref, *scratch):
    count, block, width = res_ref.shape
    step, me = pl.program_id(0), lax.axis_index("mp")
    row_sums = RowSum(me, scratch[:4], dot_ref)
    back_sums = Scatter(me, count, scratch[4:], back_out)

    @pl.when(step == 0)
    def _():
        meet(me, back_sums.levels)
        for ref in (agl_ref, bg_ref, bl_ref, ad_ref, bd_ref, sg_ref, sl_ref):
            ref[...] = jnp.zeros_like(ref)

    back_sums.advance(step)
    row_sums.advance(step)

    @pl.when(step < back_sums.blocks)
    def _():
        total = jnp.zeros((block, 1), F32)
        for c in range(count):
            part = res_ref[c].astype(F32)
            total = total + jnp.sum(part * part, axis=1, keepdims=True)
        inv = lax.rsqrt(total / (count * width) + EPSILON)
        inv_ref[...] = inv
        for c in range(count):
            cols = slice(c * width, (c + 1) * width)
            x_ref[:, cols] = (res_ref[c].astype(F32) * inv * gain_ref[c]).astype(BF)
            gd_ref[:, cols] = gd_in_ref[c]
        x, grad_down = x_ref[...], gd_ref[...]
        inner_g = dot_nn(x, gate_ref[...])
        inner_u = dot_nn(x, lift_ref[...])
        gate_ratio, lift_ratio = rg_ref[...], rl_ref[...]
        gate_act, lift_act = inner_g * gate_ratio, inner_u * lift_ratio
        sigmoid_g = jax.nn.sigmoid(gate_act)
        silu_g = gate_act * sigmoid_g
        hidden = (silu_g * lift_act).astype(BF)
        grad_hidden = dot_nt(grad_down, down_ref[...])
        d_lift = grad_hidden * silu_g
        d_gate = grad_hidden * lift_act * sigmoid_g * (1.0 + gate_act * (1.0 - sigmoid_g))
        grad_g = (d_gate * gate_ratio).astype(BF)
        grad_l = (d_lift * lift_ratio).astype(BF)
        for ref, place, at in back_sums.chunks(width):
            ref[place] = (
                dot_nt(grad_g, gate_ref[at, :]) + dot_nt(grad_l, lift_ref[at, :])
            ).astype(BF)
        back_sums.copy(0, step, 0).start()
        for c in range(count):
            cols = slice(c * width, (c + 1) * width)
            down_out[c] = dot_nn(hidden, down_ref[:, cols]).astype(BF)
        product_g, product_l = inner_g * d_gate, inner_u * d_lift
        sg_ref[...] += jnp.sum(product_g, axis=0, keepdims=True)
        sl_ref[...] += jnp.sum(product_l, axis=0, keepdims=True)
        row_sums.begin(
            step,
            jnp.sum(product_g * gate_ratio + product_l * lift_ratio, axis=1, keepdims=True),
        )
        low_x = dot_nt(x, lgl_ref[...]).astype(BF)
        low_g = (dot_nt(grad_g, ug_ref[...]) + dot_nt(grad_l, ul_ref[...])).astype(BF)
        agl_ref[...] += dot_tn(low_g, x)
        bg_ref[...] += dot_tn(low_x, grad_g)
        bl_ref[...] += dot_tn(low_x, grad_l)
        low_h = dot_nn(hidden, ld_ref[...]).astype(BF)
        low_d = dot_nt(grad_down, ud_ref[...]).astype(BF)
        ad_ref[...] += dot_tn(low_d, hidden)
        bd_ref[...] += dot_tn(low_h, grad_down)


def ffn(res, gain, gd, gate, lift, down, rg, rl, lgl, ug, ul, ld, ud, block=256):
    count, length, width = res.shape
    depth, hidden = gate.shape
    blocks = length // block
    levels = count.bit_length() - 1
    acc_shapes = [
        (RP, depth), (RP, hidden), (RP, hidden), (RP, hidden), (RP, depth),
        (1, hidden), (1, hidden),
    ]
    return pl.pallas_call(
        ffn_body,
        grid=(blocks + levels,),
        in_specs=[
            chunk_upto(blocks - 1, count, block, width),
            once(gain.shape),
            chunk_upto(blocks - 1, count, block, width),
            *[once(a.shape) for a in (gate, lift, down, rg, rl, lgl, ug, ul, ld, ud)],
        ],
        out_specs=[
            chunk_upto(blocks - 1, count, block, width), whole((length, width)),
            upto(blocks - 1, block, 1), whole((length, 1)),
            *[whole(s) for s in acc_shapes],
        ],
        out_shape=[
            sds((count, length, width), BF), sds((length, width), BF),
            sds((length, 1), F32), sds((length, 1), F32),
            *[sds(s, F32) for s in acc_shapes],
        ],
        scratch_shapes=[
            pltpu.VMEM((block, depth), BF), pltpu.VMEM((block, depth), BF),
            *row_scratch(count, blocks, block),
            *scatter_scratch(count, blocks, block, width),
        ],
        compiler_params=pltpu.CompilerParams(collective_id=2, has_side_effects=True),
        cost_estimate=estimate(14 * length * depth * hidden, 40 * length * depth),
        name="ffn",
    )(res, gain, gd, gate, lift, down, rg, rl, lgl, ug, ul, ld, ud)


def out_back_body(g_ref, a_ref, w_ref, u_ref, l_ref, da_ref, aa_ref, bb_ref, grad_ref):
    count, _, width = g_ref.shape

    @pl.when(pl.program_id(0) == 0)
    def _():
        aa_ref[...] = jnp.zeros_like(aa_ref)
        bb_ref[...] = jnp.zeros_like(bb_ref)

    for c in range(count):
        grad_ref[:, c * width:(c + 1) * width] = g_ref[c]
    grad, act = grad_ref[...], a_ref[...]
    da_ref[...] = dot_nt(grad, w_ref[...]).astype(BF)
    low_g = dot_nt(grad, u_ref[...]).astype(BF)
    low_a = dot_nn(act, l_ref[...]).astype(BF)
    aa_ref[...] += dot_tn(low_g, act)
    bb_ref[...] += dot_tn(low_a, grad)


def out_back(grad, act, w, u, low, block=256):
    count, length, width = grad.shape
    depth = count * width
    return pl.pallas_call(
        out_back_body,
        grid=(length // block,),
        in_specs=[
            chunk_rows(count, block, width), rows(block, width), whole(w.shape),
            whole(u.shape), whole(low.shape),
        ],
        out_specs=[rows(block, width), whole((RP, width)), whole((RP, depth))],
        out_shape=[sds((length, width), BF), sds((RP, width), F32), sds((RP, depth), F32)],
        scratch_shapes=[pltpu.VMEM((block, depth), BF)],
        cost_estimate=estimate(4 * length * depth * width, 3 * length * depth),
        name="out_back",
    )(grad, act, w, u, low)


def qkv_back_body(g_ref, y_ref, x_ref, xl_ref, w_ref, u_ref, inv_ratio_ref,
                  dx_ref, dot_ref, aa_ref, bb_ref, ss_ref, *scratch):
    width = dx_ref.shape[1]
    count = w_ref.shape[0] // width
    step, me = pl.program_id(0), lax.axis_index("mp")
    row_sums = RowSum(me, scratch[:4], dot_ref)
    sums = Scatter(me, count, scratch[4:], dx_ref)

    @pl.when(step == 0)
    def _():
        meet(me, sums.levels)
        aa_ref[...] = jnp.zeros_like(aa_ref)
        bb_ref[...] = jnp.zeros_like(bb_ref)
        ss_ref[...] = jnp.zeros_like(ss_ref)

    sums.advance(step)
    row_sums.advance(step)

    @pl.when(step < sums.blocks)
    def _():
        grad = g_ref[...]
        for ref, place, at in sums.chunks(width):
            ref[place] = dot_nt(grad, w_ref[at, :]).astype(BF)
        sums.copy(0, step, 0).start()
        product = grad.astype(F32) * y_ref[...].astype(F32) * inv_ratio_ref[...]
        row_sums.begin(step, jnp.sum(product, axis=1, keepdims=True))
        ss_ref[...] += jnp.sum(product * inv_ratio_ref[...], axis=0, keepdims=True)
        low_g = dot_nt(grad, u_ref[...]).astype(BF)
        aa_ref[...] += dot_tn(low_g, x_ref[...])
        bb_ref[...] += dot_tn(xl_ref[...], grad)


def qkv_backward(grad, y, x, xl, w_cat, u_cat, inv_ratio, count, block=256):
    length, depth = x.shape
    wide = grad.shape[1]
    width, blocks = depth // count, length // block
    levels = count.bit_length() - 1
    return pl.pallas_call(
        qkv_back_body,
        grid=(blocks + levels,),
        in_specs=[
            upto(blocks - 1, block, wide), upto(blocks - 1, block, wide),
            upto(blocks - 1, block, depth), upto(blocks - 1, block, RP),
            once(w_cat.shape), once(u_cat.shape), once(inv_ratio.shape),
        ],
        out_specs=[
            whole((length, width)), whole((length, 1)),
            whole((RP, depth)), whole((RP, wide)), whole((1, wide)),
        ],
        out_shape=[
            sds((length, width), BF), sds((length, 1), F32),
            sds((RP, depth), F32), sds((RP, wide), F32), sds((1, wide), F32),
        ],
        scratch_shapes=[
            *row_scratch(count, blocks, block), *scatter_scratch(count, blocks, block, width)
        ],
        compiler_params=pltpu.CompilerParams(collective_id=3, has_side_effects=True),
        cost_estimate=estimate(4 * length * depth * wide, 40 * length * depth),
        name="qkv_backward",
    )(grad, y, x, xl, w_cat, u_cat, inv_ratio)


def far(z, k):
    return {"dp": z + (1 << k) * (1 - 2 * bit_of(z, k))}


def reduce_body(part_ref, *refs, levels, depths, ranks, weights):
    groups, count = len(ranks), len(weights)

    def take(number):
        nonlocal refs
        taken, refs = refs[:number], refs[number:]
        return taken

    own_refs, cross_refs, coef_refs, inv_refs = (take(groups) for _ in range(4))
    base_refs, upper_refs, lower_refs = (take(count) for _ in range(3))
    scale_outs, upper_outs, lower_outs = take(groups), take(count), take(count)
    keep, send, land = (take(levels) for _ in range(3))
    sums, held, come, full, beta_refs = (take(groups) for _ in range(5))
    bases = take(count)
    sent, landed, far_sent, far_landed, full_sent, full_landed, base_sems = refs
    me, z = lax.axis_index("mp"), lax.axis_index("dp")
    loads = [
        pltpu.make_async_copy(base_refs[n], bases[n], base_sems.at[n]) for n in range(count)
    ]
    for load in loads:
        load.start()
    barrier = pltpu.get_barrier_semaphore()
    for target in [other(me, k) for k in range(levels)] + [far(z, k) for k in range(depths)]:
        pl.semaphore_signal(
            barrier, inc=1, device_id=target, device_id_type=pl.DeviceIdType.MESH
        )
    pl.semaphore_wait(barrier, levels + depths)

    def swap(src, dst, sent_at, landed_at, target):
        return pltpu.make_async_remote_copy(
            src_ref=src, dst_ref=dst, send_sem=sent_at, recv_sem=landed_at,
            device_id=target, device_id_type=pl.DeviceIdType.MESH,
        )

    places = part_ref.shape[0] // 2
    for place in range(places):
        keep[0][place] = part_ref[chunk_of(me, 0, place, levels)]
        send[0][place] = part_ref[chunk_of(me, 1, place, levels)].astype(BF)
    rank = part_ref.shape[1]
    for level in range(levels):
        copy = swap(send[level], land[level], sent.at[level], landed.at[level], other(me, level))
        copy.start()
        copy.wait()
        for place in range(places):
            value = keep[level][place] + land[level][place].astype(F32)
            if level == levels - 1:
                held[0][0, :rank] = value.astype(BF)
            elif place >= places // 2:
                send[level + 1][place - places // 2] = value.astype(BF)
            else:
                keep[level + 1][place] = value
        places //= 2
    held[0][0, rank:] = own_refs[0][...].astype(BF)
    for n in range(1, groups):
        held[n][0] = own_refs[n][...].astype(BF)
    for k in range(depths):
        copies = [
            swap(held[n].at[k], come[n].at[k], far_sent.at[k, n], far_landed.at[k, n], far(z, k))
            for n in range(groups)
        ]
        for copy in copies:
            copy.start()
        for n, copy in enumerate(copies):
            copy.wait()
            value = held[n][k].astype(F32) + come[n][k].astype(F32)
            if k == depths - 1:
                sums[n][...] = value
            else:
                held[n][k + 1] = value.astype(BF)
    for n, (number, upper_at, square_at) in enumerate(ranks):
        square = sums[n][square_at:square_at + 8]
        scale_outs[n][...] = square * inv_refs[n][...]
        betas = square * coef_refs[n][...]
        for i in range(number):
            at = upper_at + i * R
            full[n][me, i * R:(i + 1) * R] = (
                2.0 * (
                    sums[n][at:at + R] - cross_refs[n][i * R:(i + 1) * R] * betas[i:i + 1]
                )
            ).astype(BF)
        full[n][me, number * R:] = jnp.concatenate([betas, jnp.zeros_like(betas)], 0).astype(BF)
    known, serial = [()], 0
    for bit in range(levels - 1, -1, -1):
        copies = []
        for flips in known:
            at = 0
            for k in range(levels):
                mine = bit_of(me, k)
                at = at + ((1 - mine) if k in flips else mine) * (1 << k)
            for n in range(groups):
                copies.append(
                    swap(
                        full[n].at[at], full[n].at[at], full_sent.at[serial, n],
                        full_landed.at[serial, n], other(me, bit),
                    )
                )
            serial += 1
        for copy in copies:
            copy.start()
        for copy in copies:
            copy.wait()
        known = known + [flips + (bit,) for flips in known]
    for load in loads:
        load.wait()
    for n, (group, i, (own_group, own_at)) in enumerate(weights):
        number = ranks[group][0]
        chunks, _, size = full[group].shape
        beta_ref = beta_refs[group]
        for c in range(chunks):
            cols = slice(c * size, (c + 1) * size)
            upper_outs[n][:, cols] = full[group][c, i * R:(i + 1) * R].astype(F32)
            row = full[group][c, number * R:].astype(F32)[i:i + 1]
            beta_ref[:, cols] = jnp.broadcast_to(row, (R, size))
        upper = upper_refs[n][...]
        tilted = (upper * beta_ref[...]).astype(BF)
        core = dot_nt(tilted, upper.astype(BF))
        correction = dot_nt(tilted, bases[n][...]) + 2.0 * dot_nn(
            core.astype(BF), lower_refs[n][...].astype(BF)
        )
        lower_outs[n][...] = 2.0 * (sums[own_group][own_at:own_at + R] - correction)


def reduce_sums(part, groups, weights):
    members = lax.axis_size("mp")
    rank, width = part.shape[0], part.shape[1] // members
    part = jnp.transpose(part.reshape(rank, members, width), (1, 0, 2))
    levels = members.bit_length() - 1
    depths = lax.axis_size("dp").bit_length() - 1
    owns, crosses, coefs, invs, ranks = zip(*groups)
    places, bases, uppers, lowers = zip(*weights)
    shapes = [(rank + owns[0].shape[0], width)] + [v.shape for v in owns[1:]]
    fulls = [(members, r[0] * R + 16, v[1]) for r, v in zip(ranks, shapes)]
    vmem, dma = pl.BlockSpec(memory_space=pltpu.VMEM), pltpu.SemaphoreType.DMA

    def halves(dtype):
        return [pltpu.VMEM((members >> (k + 1), rank, width), dtype) for k in range(levels)]

    steps = [pltpu.VMEM((depths,) + tuple(v), BF) for v in shapes]
    number = len(groups)
    return pl.pallas_call(
        functools.partial(
            reduce_body, levels=levels, depths=depths, ranks=ranks, weights=places
        ),
        in_specs=[
            *[vmem] * (1 + 4 * number),
            *[pl.BlockSpec(memory_space=pl.ANY)] * len(bases),
            *[vmem] * (2 * len(bases)),
        ],
        out_specs=[vmem] * (number + 2 * len(bases)),
        out_shape=[
            *[sds((8, v[1]), F32) for v in shapes],
            *[sds(v.shape, F32) for v in uppers],
            *[sds(v.shape, F32) for v in lowers],
        ],
        scratch_shapes=[
            *halves(F32), *halves(BF), *halves(BF),
            *[pltpu.VMEM(v, F32) for v in shapes], *steps, *steps,
            *[pltpu.VMEM(v, BF) for v in fulls],
            *[pltpu.VMEM((R, members * v[1]), F32) for v in shapes],
            *[pltpu.VMEM(v.shape, BF) for v in bases],
            dma((levels,)), dma((levels,)),
            dma((depths, number)), dma((depths, number)),
            dma((members - 1, number)), dma((members - 1, number)),
            dma((len(bases),)),
        ],
        compiler_params=pltpu.CompilerParams(collective_id=4, has_side_effects=True),
        cost_estimate=estimate(0, 60_000_000),
        name="reduce_sums",
    )(part, *owns, *crosses, *coefs, *invs, *bases, *uppers, *lowers)


def split_low(value):
    high = lax.reduce_precision(value, 8, 7)
    return high, value - high


def block_diagonal(blocks):
    width = sum(b.shape[1] for b in blocks)
    at = 0
    result = []
    for b in blocks:
        result.append(jnp.pad(b, ((0, 0), (at, width - at - b.shape[1]))))
        at += b.shape[1]
    return jnp.concatenate(result, axis=0)


def pad_rows(value, at=0):
    return jnp.pad(value, ((at, RP - at - value.shape[0]), (0, 0))).astype(BF)


def flip(value, bit, axis="mp"):
    size = lax.axis_size(axis)
    return lax.ppermute(value, axis, [(i, i ^ (1 << bit)) for i in range(size)])


def gather_small(value, me):
    levels = lax.axis_size("mp").bit_length() - 1
    part = value.reshape((1,) * levels + value.shape)
    for bit in range(levels - 1, -1, -1):
        came = flip(part, bit)
        upper = ((me >> bit) & 1) == 1
        part = jnp.concatenate(
            [jnp.where(upper, came, part), jnp.where(upper, part, came)], axis=levels - 1 - bit
        )
    return part.reshape((1 << levels,) + value.shape)


def scatter_cols(value, me):
    members = lax.axis_size("mp")
    part = jnp.transpose(value.reshape(value.shape[0], members, -1), (1, 0, 2))
    for bit in range(members.bit_length() - 1):
        mine = (me >> bit) & 1
        pair = part.reshape(part.shape[0] // 2, 2, *part.shape[1:])
        keep = lax.dynamic_index_in_dim(pair, mine, 1, keepdims=False)
        away = lax.dynamic_index_in_dim(pair, 1 - mine, 1, keepdims=False)
        part = keep + flip(away, bit)
    return part[0]


def tie(value, *others):
    return lax.optimization_barrier((value, *others))[0]


def tables(lengths, length):
    ends = jnp.cumsum(lengths)
    at = jnp.arange(length, dtype=jnp.int32)
    after = (at[:, None] >= ends[None, :NDOC]).astype(jnp.int32)
    segment = jnp.sum(after, axis=1)
    start = jnp.sum(after * lengths[None, :NDOC], axis=1)
    half = jnp.arange(HD // 2, dtype=F32)
    frequency = ROPE_BASE ** (-(2.0 * half / HD))
    angles = (at - start).astype(F32)[:, None] * frequency[None, :]
    cos, sin = jnp.cos(angles), jnp.sin(angles)
    return (
        start,
        (segment < NDOC).astype(F32)[:, None],
        jnp.concatenate([cos, cos], axis=1),
        jnp.concatenate([sin, -sin], axis=1),
    )


def on_device(
    tokens, doc_lengths, out_grad, attn_gain, ffn_gain,
    query_base, query_lower, query_upper, query_scale,
    key_base, key_lower, key_upper, key_scale,
    value_base, value_lower, value_upper, value_scale,
    output_base, output_lower, output_upper, output_scale,
    gate_base, gate_lower, gate_upper, gate_scale,
    lift_base, lift_lower, lift_upper, lift_scale,
    down_base, down_lower, down_upper, down_scale,
):
    members = lax.axis_size("mp")
    me = lax.axis_index("mp")
    seqs, length, width = tokens.shape
    depth = members * width
    hidden = down_base.shape[0]
    block = min(256, length)

    def gather(value):
        return lax.all_gather(value, "mp", axis=0)

    def own_cols(value, size):
        return lax.dynamic_slice_in_dim(value, me * size, size, 1)

    def exchange(value):
        return lax.all_to_all(value, "mp", split_axis=0, concat_axis=0, tiled=True)

    qkv_arranged = arrange([query_base, key_base, value_base], members)
    qkv_base = exchange(qkv_arranged)
    pack = jnp.concatenate(
        [
            tie(query_lower, qkv_arranged).T, key_lower.T, value_lower.T,
            gate_lower.T, lift_lower.T,
            jnp.stack([attn_gain, ffn_gain]),
        ],
        axis=0,
    )
    pack = jnp.pad(pack, ((0, 88 - pack.shape[0]), (0, 0)))
    packed = jnp.transpose(gather_small(pack, me), (1, 0, 2)).reshape(pack.shape[0], depth)
    tok_all = [gather(tokens[s]) for s in range(seqs)]
    lower_qkv_t, lower_gl_t = packed[:3 * R], packed[3 * R:5 * R]
    gain_a, gain_f = packed[5 * R], packed[5 * R + 1]

    output_w, square_o, cross_o = merge(
        [tie(output_base, qkv_arranged)[None]], output_lower.T, output_upper)
    down_w, square_d, cross_d = merge(
        [tie(down_base, qkv_arranged)[None]], down_lower.T, down_upper)
    row_stats = scatter_cols(
        jnp.concatenate([square_o, square_d, cross_o, cross_d], axis=0), me
    )
    output_w, down_w = output_w[0], down_w[0]
    norm_o, norm_d = jnp.sqrt(row_stats[0]), jnp.sqrt(row_stats[1])
    cross_o, cross_d = row_stats[2:2 + R], row_stats[2 + R:2 + 2 * R]
    ratio_o, ratio_d = output_scale / norm_o, down_scale / norm_d
    layouts = [tables(doc_lengths[s], length) for s in range(seqs)]
    grad_tops = [out_grad[s].astype(F32) * layouts[s][1] for s in range(seqs)]
    gd_low = [(grad_tops[s] * ratio_d).astype(BF) for s in range(seqs)]
    gd_all = [gather(gd_low[s]) for s in range(seqs)]

    upper_qkv = block_diagonal([own_cols(u, width) for u in (query_upper, key_upper, value_upper)])
    upper_g, upper_l = own_cols(gate_upper, hidden), own_cols(lift_upper, hidden)
    qkv_w, square_qkv, cross_all = merge([qkv_base], lower_qkv_t, upper_qkv)
    qkv_w = qkv_w.reshape(depth, 3 * width)
    norm_qkv = jnp.sqrt(square_qkv[0])
    scale_qkv = jnp.concatenate([query_scale, key_scale, value_scale])
    ratio_qkv = (scale_qkv / norm_qkv)[None]
    inv_ratio = 1.0 / ratio_qkv

    copies, z = lax.axis_size("dp"), lax.axis_index("dp")
    share = width // copies
    gl_arranged = arrange(
        [
            lax.dynamic_slice_in_dim(tie(v, qkv_arranged), z * share, share, 0)
            for v in (gate_base, lift_base)
        ],
        members,
    )
    gl_own = exchange(tie(gl_arranged, qkv_base))
    from_low, from_high = [gl_own], [gl_own]
    for _ in range(1, copies):
        from_low.append(lax.ppermute(from_low[-1], "dp", [(i, i + 1) for i in range(copies - 1)]))
        from_high.append(lax.ppermute(from_high[-1], "dp", [(i + 1, i) for i in range(copies - 1)]))
    gl_pieces = from_low[:0:-1] + from_high
    gate_w, lift_w, square_gl, cross_g, cross_l = merge(
        gl_pieces, lower_gl_t, block_diagonal([upper_g, upper_l]), [hidden, hidden]
    )
    gate_w, lift_w = gate_w.reshape(depth, hidden), lift_w.reshape(depth, hidden)
    norm_gl = jnp.sqrt(square_gl[0])
    norm_g, norm_l = norm_gl[:hidden], norm_gl[hidden:]
    ratio_g, ratio_l = (gate_scale / norm_g)[None], (lift_scale / norm_l)[None]

    low_l_qkv, low_l_gl = pad_rows(lower_qkv_t), pad_rows(lower_gl_t)
    low_u_qkv, low_u_g, low_u_l = pad_rows(upper_qkv), pad_rows(upper_g), pad_rows(upper_l, R)
    low_l_d, low_u_d = pad_rows(down_lower.T).T, pad_rows(down_upper)
    low_l_o, low_u_o = pad_rows(output_lower.T).T, pad_rows(output_upper)
    chunk_gain_a, chunk_gain_f = (v.reshape(members, 1, width) for v in (gain_a, gain_f))

    state = [dict() for _ in range(seqs)]

    def attention_stage(s):
        st = state[s]
        start, _, st["cos"], st["sin"] = layouts[s]
        st["start"] = start.reshape(length // block, block)
        st["lo"] = st["start"][:, 0] // block
        if s == 0:
            tok = tie(tok_all[s], gl_arranged, *gd_low)
        else:
            tok = tie(tok_all[s], state[s - 1]["residual_low"])
        st["x"], st["y"], st["q"], st["k"], st["xl"], st["inv"] = qkv_forward(
            tok, chunk_gain_a, qkv_w, low_l_qkv, ratio_qkv, st["cos"], st["sin"]
        )
        st["att"], st["lse"] = attend_forward(
            st["lo"], st["start"], st["q"], st["k"], st["y"], block
        )
        act = tie(st["att"], gate_w, lift_w) if s == seqs - 1 else st["att"]
        st["inner_o"] = out_forward(act, output_w).astype(F32)
        st["residual"] = tokens[s].astype(F32) + st["inner_o"] * ratio_o
        st["residual_low"] = st["residual"].astype(BF)
        st["residual_all"] = gather(st["residual_low"])

    def ffn_stage(s):
        st = state[s]
        if s + 1 < seqs:
            res = tie(st["residual_all"], state[s + 1]["residual_low"])
        else:
            res = tie(st["residual_all"], state[s - 1]["grad_output_low"])
        st["down"], back, st["inv_f"], dot_f, *st["ffn"] = ffn(
            res, chunk_gain_f, gd_all[s], gate_w, lift_w, down_w,
            ratio_g, ratio_l, low_l_gl, low_u_g, low_u_l, low_l_d, low_u_d,
        )
        inv = st["inv_f"]
        grad_residual = (
            grad_tops[s] + inv * (ffn_gain * back.astype(F32))
            - st["residual"] * (inv * inv * dot_f / depth)
        )
        st["grad_residual"] = grad_residual
        st["grad_output_low"] = (grad_residual * ratio_o).astype(BF)
        st["grad_output"] = gather(st["grad_output_low"])
        st["g_o"] = jnp.sum(st["inner_o"] * grad_residual, axis=0)

    def attention_back_stage(s):
        st = state[s]
        grad = st["grad_output"]
        if s + 1 < seqs:
            grad = tie(grad, state[s + 1]["grad_output_low"])
        else:
            grad = tie(grad, state[s - 1]["dx"])
        grad_att, st["a_o"], st["b_o"] = out_back(
            grad, st["att"], output_w, low_u_o, low_l_o
        )
        st["grad_att"] = grad_att
        grads = attend_backward(
            st["lo"], st["start"], st["q"], st["k"], st["y"], grad_att, st["att"],
            st["lse"], st["cos"], st["sin"], ratio_qkv, block,
        )
        st["grads"] = grads
        st["dx"], dot_a, st["a_qkv"], st["b_qkv"], st["g_qkv"] = qkv_backward(
            grads, st["y"], st["x"], st["xl"], qkv_w, low_u_qkv, inv_ratio, members
        )
        inv = st["inv"]
        st["in_grad"] = (
            st["grad_residual"] + inv * (attn_gain * st["dx"].astype(F32))
            - tokens[s].astype(F32) * (inv * inv * dot_a / depth)
        )

    def late_stage(s):
        st = state[s]
        down = tie(st["down"], state[0]["grad_att"] if s == 0 else state[0]["grads"])
        inner_d = lax.psum_scatter(down, "mp", scatter_dimension=0, tiled=False)
        inner_d = inner_d.astype(F32)
        st["out"] = (st["residual"] + inner_d * ratio_d).astype(BF)
        st["g_d"] = jnp.sum(inner_d * grad_tops[s], axis=0)

    for stage in (attention_stage, ffn_stage, attention_back_stage, late_stage):
        for s in range(seqs):
            stage(s)

    out_tokens = jnp.stack([st["out"] for st in state])
    in_grad = jnp.stack([st["in_grad"] for st in state])

    def total(pick):
        result = pick(state[0])
        for s in range(1, seqs):
            result = result + pick(state[s])
        return result

    def blocks_of(value, size):
        return jnp.concatenate(
            [value[n * R:(n + 1) * R, n * size:(n + 1) * size] for n in range(value.shape[0] // R)],
            axis=0,
        )

    def stacked(values, height):
        value = jnp.concatenate(values, axis=0)
        return jnp.pad(value, ((0, height - value.shape[0]), (0, 0)))

    coef_qkv = (scale_qkv / norm_qkv ** 3).reshape(3, width)
    coef_o, coef_d = output_scale / norm_o ** 3, down_scale / norm_d ** 3
    coef_g, coef_l = gate_scale / norm_g ** 3, lift_scale / norm_l ** 3
    norm_rows = norm_qkv.reshape(3, width)
    groups = [
        (
            stacked(
                [
                    blocks_of(total(lambda st: st["b_qkv"])[:3 * R], width),
                    total(lambda st: st["a_o"])[:R],
                    total(lambda st: st["g_o"])[None],
                    total(lambda st: st["g_d"])[None],
                    total(lambda st: st["g_qkv"]).reshape(3, width),
                ],
                4 * R + 8,
            ),
            jnp.concatenate([cross_o, cross_d, blocks_of(cross_all, width)], axis=0),
            stacked([coef_o[None], coef_d[None], coef_qkv], 8),
            stacked([1.0 / norm_o[None], 1.0 / norm_d[None], 1.0 / norm_rows], 8),
            (5, 5 * R, 11 * R),
        ),
        (
            stacked(
                [
                    total(lambda st: st["ffn"][1])[:R],
                    total(lambda st: st["ffn"][2])[R:2 * R],
                    total(lambda st: st["ffn"][3])[:R],
                    total(lambda st: st["ffn"][5]),
                    total(lambda st: st["ffn"][6]),
                ],
                3 * R + 8,
            ),
            jnp.concatenate([cross_g[:R], cross_l[R:2 * R]], axis=0),
            stacked([coef_g[None], coef_l[None]], 8),
            stacked([1.0 / norm_g[None], 1.0 / norm_l[None]], 8),
            (2, 0, 3 * R),
        ),
    ]
    weights = [
        ((0, 2, (0, 0)), query_base, query_upper, query_lower.T),
        ((0, 3, (0, R)), key_base, key_upper, key_lower.T),
        ((0, 4, (0, 2 * R)), value_base, value_upper, value_lower.T),
        ((0, 0, (0, 10 * R)), output_base, output_upper, output_lower.T),
        ((1, 0, (0, 3 * R)), gate_base, gate_upper, gate_lower.T),
        ((1, 1, (0, 4 * R)), lift_base, lift_upper, lift_lower.T),
        ((0, 1, (1, 2 * R)), down_base, down_upper, down_lower.T),
    ]
    part = jnp.concatenate(
        [
            total(lambda st: st["a_qkv"])[:3 * R],
            total(lambda st: st["ffn"][0])[:2 * R],
            total(lambda st: st["b_o"])[:R],
            total(lambda st: st["ffn"][4])[:R],
        ],
        axis=0,
    )
    finished = reduce_sums(part, groups, weights)
    results = [out_tokens, in_grad]
    for n, ((group, i, _), _, _, _) in enumerate(weights):
        results += [finished[2 + len(weights) + n].T, finished[2 + n], finished[group][i]]
    return tuple(results)


def solution(mesh):
    spread, split, rows_spec = P("dp", None, "mp"), P("mp"), P("mp", None)
    weight = (rows_spec, rows_spec, P(), split)
    grads = (rows_spec, P(), split)

    return jax.shard_map(
        on_device,
        mesh=mesh,
        in_specs=(spread, P("dp", None), spread, split, split) + weight * 7,
        out_specs=(spread, spread) + grads * 7,
        check_vma=False,
    )
```
